32 devices in a mesh: head: 2 (over core), batch: 8 (over z, x), group: 2 (over y).
Axes of the slice: x: 2, y: 2, z: 4, core: 2. Of those that a mesh axis runs over, the one named last changes fastest.
Arguments:
- inputs: bfloat16 [16, 512, 2048], P(('batch', 'group'), 'head'), may hold values from -6 to 6
- rms_gain: float32 [2048], replicated, may hold values from 0.5 to 1.5
- w_query: bfloat16 [2048, 2048], P('batch', 'head'), may hold values from -0.125 to 0.125
- w_key: bfloat16 [2048, 2048], P('batch', 'head'), may hold values from -0.125 to 0.125
- w_value: bfloat16 [2048, 4096], P('batch', 'head'), may hold values from -0.125 to 0.125
- w_gate: bfloat16 [2048, 4096], P('batch', 'head'), may hold values from -0.125 to 0.125
- w_out: bfloat16 [4096, 2048], P('head', 'batch'), may hold values from -0.125 to 0.125
- ln_gain: float32 [2048], replicated, may hold values from 0.5 to 1.5
- w_up: bfloat16 [2048, 4096], P('batch', 'head'), may hold values from -0.125 to 0.125
- w_down: bfloat16 [4096, 2048], P('head', 'batch'), may hold values from -0.09375 to 0.09375
- cotangent: bfloat16 [16, 512, 2048], P(('batch', 'group'), 'head'), may hold values from -6 to 6
- domain_of: int32 [16], replicated, may hold values from 0 to 3, as said below
- domain_weight: int32 [4], replicated, may hold values from 1 to 8, as said below
Outputs:
- output: bfloat16 [16, 512, 2048], P(('batch', 'group'), 'head')
- d_inputs: bfloat16 [16, 512, 2048], P(('batch', 'group'), 'head')
- d_rms_gain: float32 [2048], replicated
- d_w_query: float32 [2048, 2048], P('batch', 'head')
- d_w_key: float32 [2048, 2048], P('batch', 'head')
- d_w_value: float32 [2048, 4096], P('batch', 'head')
- d_w_gate: float32 [2048, 4096], P('batch', 'head')
- d_w_out: float32 [4096, 2048], P('head', 'batch')
- d_ln_gain: float32 [2048], replicated
- d_w_up: float32 [2048, 4096], P('batch', 'head')
- d_w_down: float32 [4096, 2048], P('head', 'batch')
The draws below stay inside these ranges and needn't reach their ends.
Inputs may be any that keep to these rules, and one draw needn't show every extreme that they name: `domain_of`: every domain group has at least one sequence. `domain_weight`: some domain has weight 1 and another weight 8.
All inputs are finite; a program needn't handle non-finite values.
Results may differ from the reference program's by a relative error of at most 0.019.
Values may be sent and summed in bfloat16 or wider, within the bound.
A program may use at most 256 MiB of HBM per device.

```python
import jax
import jax.numpy as jnp
from jax import lax

D = 2048
HEADS = 8
KEY = 256
VAL = 512
FF = 4096
LEN = 512
DOMAINS = 4
QK = 2048
VD = 4096
SEQS = 16


def draw_domain_of(key, part):
    key_low = jax.random.fold_in(key, 11)
    key_high = jax.random.fold_in(key, 12)
    key_shuffle = jax.random.fold_in(key, 13)
    chosen_domain = jnp.minimum(jax.random.randint(key_low, (SEQS,), 0, DOMAINS), jax.random.randint(key_high, (SEQS,), 0, DOMAINS))
    shuffled = jax.random.permutation(key_shuffle, SEQS)
    placed = chosen_domain.at[shuffled[:DOMAINS]].set(jnp.arange(DOMAINS, dtype=jnp.int32))
    return placed.astype(jnp.int32)


def draw_domain_weight(key, part):
    base = jax.random.randint(jax.random.fold_in(key, 21), (DOMAINS,), 1, 9)
    order = jax.random.permutation(jax.random.fold_in(key, 22), DOMAINS)
    base = base.at[order[0]].set(8)
    base = base.at[order[1]].set(1)
    return base.astype(jnp.int32)


def block_levels(stream_key, dims, pieces, smallest, largest):
    gain, own = 1.0, jax.random.fold_in(stream_key, 6)
    for axis_at, parts in pieces:
        steps = jnp.exp(jax.random.uniform(jax.random.fold_in(own, axis_at), (parts,), jnp.float32, smallest / len(pieces), largest / len(pieces)))
        gain = gain * jnp.repeat(steps, dims[axis_at] // parts).reshape([-1 if axis == axis_at else 1 for axis in range(len(dims))])
    return gain


def normal_values(key, dims, spread, limit, split=(), held_as=jnp.bfloat16):
    drawn = spread * jax.random.normal(key, dims, jnp.float32)
    if split:
        drawn = drawn * block_levels(key, dims, split, -0.22, 0.18)
    return jnp.clip(drawn, -limit, limit).astype(held_as)


def setup_inputs(seed: int = 0) -> dict:
    splits = jax.random.split(jax.random.key(seed), 14)
    inputs = normal_values(splits[0], (SEQS, LEN, D), 1.0, 6.0, ((0, 16), (1, 2)))
    rms_gain = jnp.clip(1.0 + 0.1 * jax.random.normal(splits[1], (D,), jnp.float32), 0.5, 1.5)
    w_query = normal_values(splits[2], (D, QK), D ** -0.5, 0.125, ((0, 8), (1, 2)))
    w_key = normal_values(splits[3], (D, QK), D ** -0.5, 0.125, ((0, 8), (1, 2)))
    w_value = normal_values(splits[4], (D, VD), D ** -0.5, 0.125, ((0, 8), (1, 2)))
    w_gate = normal_values(splits[5], (D, VD), D ** -0.5, 0.125, ((0, 8), (1, 2)))
    w_out = normal_values(splits[6], (VD, D), D ** -0.5, 0.125, ((0, 2), (1, 8)))
    ln_gain = jnp.clip(1.0 + 0.1 * jax.random.normal(splits[7], (D,), jnp.float32), 0.5, 1.5)
    w_up = normal_values(splits[8], (D, FF), D ** -0.5, 0.125, ((0, 8), (1, 2)))
    w_down = normal_values(splits[9], (FF, D), FF ** -0.5, 0.09375, ((0, 2), (1, 8)))
    cotangent = normal_values(splits[10], (SEQS, LEN, D), 1.0, 6.0, ((0, 16), (1, 2)))
    domain_of = draw_domain_of(jax.random.fold_in(splits[13], 71), 0)
    domain_weight = draw_domain_weight(jax.random.fold_in(splits[13], 71), 0)
    return {"inputs": inputs, "rms_gain": rms_gain, "w_query": w_query, "w_key": w_key, "w_value": w_value, "w_gate": w_gate, "w_out": w_out, "ln_gain": ln_gain, "w_up": w_up, "w_down": w_down, "cotangent": cotangent, "domain_of": domain_of, "domain_weight": domain_weight}


@jax.custom_vjp
def low(v):
    return lax.optimization_barrier(v.astype(jnp.bfloat16)).astype(jnp.float32)

@jax.custom_vjp
def low_back(v):
    return v

def low_keep(v):
    return (low(v), None)

def low_pass(kept, grad):
    return (grad,)

def back_keep(v):
    return (v, None)

def back_low(kept, grad):
    return (low(grad),)
low.defvjp(low_keep, low_pass)
low_back.defvjp(back_keep, back_low)

def matmul(left, right):
    return jnp.dot(left, right, precision=lax.Precision.HIGHEST, preferred_element_type=jnp.float32)

def rotate_half(block):
    half = block.shape[-1] // 2
    return jnp.concatenate([-block[..., half:], block[..., :half]], axis=-1)

def rotary_tables(length, width):
    ramp = jnp.linspace(jnp.float32(0.0), jnp.float32(1.0), width // 2).astype(jnp.float32)
    freqs = jnp.exp(-ramp * jnp.log(jnp.float32(10000.0))).astype(jnp.float32)
    places = jnp.arange(length, dtype=jnp.int32).astype(jnp.float32)
    angles = places[:, None] * freqs[None, :]
    angles = jnp.concatenate([angles, angles], axis=1)
    return (jnp.cos(angles), jnp.sin(angles))

def decay_mask(length, head_ids):
    exponent = (jnp.float32(-5.0) - head_ids.astype(jnp.float32)) * jnp.log(jnp.float32(2.0))
    log_keep = jnp.log1p(-jnp.exp(exponent))
    places = jnp.arange(length, dtype=jnp.int32)
    offset = places[:, None] - places[None, :]
    steps = jnp.maximum(offset, 0).astype(jnp.float32)
    zeros = jnp.zeros((head_ids.shape[0], length, length), jnp.float32)
    return jnp.where(offset[None] >= 0, jnp.exp(steps[None] * log_keep[:, None, None]), zeros)

def sequence_factor(domain_of, domain_weight):
    same = (domain_of[:, None] == domain_of[None, :]).astype(jnp.float32)
    counts = lax.optimization_barrier(jnp.sum(same, axis=1))
    domain_ids = jnp.arange(domain_weight.shape[0], dtype=jnp.int32)
    onehot = (domain_of[:, None] == domain_ids[None, :]).astype(jnp.float32)
    weight_seq = lax.optimization_barrier(jnp.sum(onehot * domain_weight.astype(jnp.float32)[None, :], axis=1))
    total = jnp.sum(weight_seq / counts)
    return jnp.float32(domain_of.shape[0]) * weight_seq / (counts * total)

def forward(inputs, rms_gain, w_query, w_key, w_value, w_gate, w_out, ln_gain, w_up, w_down):
    seq_count, length, width = inputs.shape
    flat = inputs.reshape(seq_count * length, width)
    scale = lax.rsqrt(lax.optimization_barrier(jnp.mean(flat * flat, axis=1, keepdims=True)) + 1e-06)
    normed = low(flat * scale * rms_gain)
    queries = low_back(matmul(normed, w_query))
    keys = low_back(matmul(normed, w_key))
    values = low(low_back(matmul(normed, w_value)))
    gates = low_back(matmul(normed, w_gate))
    cosine_table, sine_table = rotary_tables(length, KEY)

    def rotary(block):
        block = block.reshape(seq_count, length, HEADS, KEY)
        return block * cosine_table[None, :, None, :] + rotate_half(block) * sine_table[None, :, None, :]
    q_rot = low(rotary(queries))
    k_rot = low(rotary(keys))
    v_heads = values.reshape(seq_count, length, HEADS, VAL)
    decays = decay_mask(length, jnp.arange(HEADS, dtype=jnp.int32))

    def per_sequence(trio):
        scores = jnp.einsum('nhk,mhk->hnm', trio[0], trio[1], precision=lax.Precision.HIGHEST)
        weighted = low(low_back(scores) * decays)
        return jnp.einsum('hnm,mhv->nhv', weighted, trio[2], precision=lax.Precision.HIGHEST)
    retained = lax.map(jax.checkpoint(per_sequence), (q_rot, k_rot, v_heads))
    retained = low_back(retained)
    centered = retained - lax.optimization_barrier(jnp.mean(retained, axis=-1, keepdims=True))
    variance = lax.optimization_barrier(jnp.mean(centered * centered, axis=-1, keepdims=True))
    normalized = (centered * lax.rsqrt(variance + 1e-05)).reshape(seq_count * length, VD)
    mixed = low(normalized * jax.nn.silu(gates))
    attention = low_back(matmul(mixed, w_out))
    hidden = flat + attention
    mean_row = lax.optimization_barrier(jnp.mean(hidden, axis=1, keepdims=True))
    shifted = hidden - mean_row
    var_row = lax.optimization_barrier(jnp.mean(shifted * shifted, axis=1, keepdims=True))
    ln_out = low(shifted * lax.rsqrt(var_row + 1e-05) * ln_gain)
    pre_act = low_back(matmul(ln_out, w_up))
    lifted = low(jax.nn.gelu(pre_act, approximate=True))
    ffn_out = low_back(matmul(lifted, w_down))
    return (hidden + ffn_out).reshape(seq_count, length, width)

def reference(inputs, rms_gain, w_query, w_key, w_value, w_gate, w_out, ln_gain, w_up, w_down, cotangent, domain_of, domain_weight):
    params = (inputs.astype(jnp.float32), rms_gain.astype(jnp.float32), w_query.astype(jnp.float32), w_key.astype(jnp.float32), w_value.astype(jnp.float32), w_gate.astype(jnp.float32), w_out.astype(jnp.float32), ln_gain.astype(jnp.float32), w_up.astype(jnp.float32), w_down.astype(jnp.float32))
    output, pullback = jax.vjp(forward, *params)
    factor = sequence_factor(domain_of, domain_weight)
    grads = pullback(cotangent.astype(jnp.float32) * factor[:, None, None])
    return (output.astype(jnp.bfloat16), grads[0].astype(jnp.bfloat16), grads[1], grads[2], grads[3], grads[4], grads[5], grads[6], grads[7], grads[8], grads[9])
```

```python
import functools

import jax
import jax.numpy as jnp
from jax import lax
from jax.experimental import pallas as pl
from jax.experimental.pallas import tpu as pltpu
from jax.sharding import PartitionSpec as P


KEY = 256
VAL = 512
BF = jnp.bfloat16
F32 = jnp.float32


def rotary_tables(places, width):
    ramp = jnp.linspace(jnp.float32(0.0), jnp.float32(1.0), width // 2).astype(F32)
    freqs = jnp.exp(-ramp * jnp.log(jnp.float32(10000.0)))
    angles = places.astype(F32)[:, None] * freqs[None, :]
    angles = jnp.concatenate([angles, angles], axis=1)
    return jnp.cos(angles), jnp.sin(angles)


def decay_mask(places, head_id):
    exponent = (jnp.float32(-5.0) - head_id.astype(F32)) * jnp.log(jnp.float32(2.0))
    log_keep = jnp.log1p(-jnp.exp(exponent))
    offset = places[:, None] - places[None, :]
    steps = jnp.maximum(offset, 0).astype(F32)
    return jnp.where(offset >= 0, jnp.exp(steps * log_keep), jnp.float32(0.0))


def sequence_factor(domain_of, domain_weight):
    same = (domain_of[:, None] == domain_of[None, :]).astype(F32)
    counts = jnp.sum(same, axis=1)
    domain_ids = jnp.arange(domain_weight.shape[0], dtype=jnp.int32)
    onehot = (domain_of[:, None] == domain_ids[None, :]).astype(F32)
    weight_seq = jnp.sum(onehot * domain_weight.astype(F32)[None, :], axis=1)
    total = jnp.sum(weight_seq / counts)
    return jnp.float32(domain_of.shape[0]) * weight_seq / (counts * total)


def rotate_half(block):
    half = block.shape[-1] // 2
    return jnp.concatenate([-block[..., half:], block[..., :half]], axis=-1)


def group_norm(block):
    centered = block - jnp.mean(block, axis=-1, keepdims=True)
    variance = jnp.mean(centered * centered, axis=-1, keepdims=True)
    return centered * lax.rsqrt(variance + 1e-05)


def gate_mix(retained, gates):
    return group_norm(retained) * jax.nn.silu(gates)


def gelu_tanh(pre_act):
    return jax.nn.gelu(pre_act, approximate=True)


def mm(left, right, left_dim, right_dim, out=F32):
    return lax.dot_general(
        left, right, (((left_dim,), (right_dim,)), ((), ())), preferred_element_type=F32
    ).astype(out)


def after(value, *others):
    return lax.optimization_barrier((value,) + others)[0]


def swap_batch(value, bits):
    size = lax.axis_size("batch")
    return lax.ppermute(value, "batch", [(i, i ^ bits) for i in range(size)])


def swap_group(value):
    return lax.ppermute(value, "group", [(0, 1), (1, 0)])


def swap_core(value):
    return lax.ppermute(value, "head", [(0, 1), (1, 0)])


def spread(rows):
    half = rows.shape[0] // 2
    pair = swap_batch(rows, 2)
    side = swap_group(rows)
    far_a = swap_group(pair[:half])
    far_b = swap_batch(side[half:], 2)
    far = jnp.concatenate([far_a, far_b], axis=0)
    pieces = []
    for piece in (rows, pair, side, far):
        pieces += [piece, swap_core(piece)]
    return jnp.concatenate(pieces, axis=0)


def collect(partial):
    width = partial.shape[1]
    blocks = partial.reshape(4, 2, -1, width)
    half = blocks.shape[2] // 2
    other = swap_core(blocks[:, 1])
    mine = blocks[:, 0].astype(F32) + other.astype(F32)
    a, b = mine[:, :half], mine[:, half:]
    a_low, b_low = a.astype(BF), b.astype(BF)
    got_a = swap_batch(jnp.stack([a_low[1], a_low[3]]), 2).astype(F32)
    got_b = swap_group(jnp.stack([b_low[2], b_low[3]])).astype(F32)
    end_a = swap_group((a[2] + got_a[1]).astype(BF)).astype(F32)
    end_b = swap_batch((b[1] + got_b[1]).astype(BF), 2).astype(F32)
    return jnp.concatenate([a[0] + got_a[0] + end_a, b[0] + got_b[0] + end_b], axis=0)


TEAM = ("head", "batch", "group")


def peers(lines):
    b = lax.axis_index("batch")
    table = {
        "head": {"head": 1 - lax.axis_index("head")},
        "batch": {"batch": b ^ 2},
        "group": {"group": 1 - lax.axis_index("group")},
        "x": {"batch": b ^ 1},
    }
    for k in range(1, lines):
        table["line", k] = {"batch": b ^ (2 * k)}
    return table


def along(lines):
    return tuple(("line", k) for k in range(1, lines))


class Wires:
    def __init__(self, send, recv, lines=1):
        self.send, self.recv, self.made, self.peers = send, recv, {}, peers(lines)

    def enter(self, names):
        barrier = pltpu.get_barrier_semaphore()
        for name in names:
            pl.semaphore_signal(barrier, inc=1, device_id=self.peers[name], device_id_type=pl.DeviceIdType.MESH)
        pl.semaphore_wait(barrier, len(names))

    def start(self, name, source, target, peer):
        n = len(self.made)
        copy = pltpu.make_async_remote_copy(
            src_ref=source,
            dst_ref=target,
            send_sem=self.send.at[n],
            recv_sem=self.recv.at[n],
            device_id=self.peers[peer],
            device_id_type=pl.DeviceIdType.MESH,
        )
        copy.start()
        self.made[name] = copy

    def arrived(self, *names):
        for name in names:
            self.made[name].wait_recv()

    def finish(self):
        for copy in self.made.values():
            copy.wait_send()


class Moves:
    def __init__(self, sems):
        self.sems, self.made = sems, []

    def start(self, source, target):
        copy = pltpu.make_async_copy(source, target, self.sems.at[len(self.made)])
        copy.start()
        self.made.append(copy)

    def finish(self):
        for copy in self.made:
            copy.wait()


TILE = 16


def tiles(rows, body):
    def step(i, _):
        body(pl.ds(pl.multiple_of(i * TILE, TILE), TILE))
        return 0

    lax.fori_loop(0, rows // TILE, step, 0)


def exchange(part, whole, rc, sums, ra, rb, ea, eb, sa, sb, wires, pointwise, hooks=()):
    rows = part.shape[2]
    half = rows // 2
    top, low = pl.ds(0, half), pl.ds(half, half)
    hook = dict(enumerate(hooks)).get
    for s in (3, 1, 2, 0):
        wires.start(("core", s), part.at[s, 1], rc.at[s], "head")

    def add(s, first):
        def body(r):
            rr = pl.ds(r.start + first, TILE)
            total = part[s, 0, rr, :].astype(F32) + rc[s, rr, :].astype(F32)
            sums[s, rr, :] = total.astype(BF)

        tiles(half, body)

    wires.arrived(("core", 3))
    add(3, 0)
    wires.start("a3", sums.at[3, top], ra.at[0], "batch")
    add(3, half)
    wires.start("b3", sums.at[3, low], rb.at[0], "group")
    wires.arrived(("core", 1))
    add(1, 0)
    wires.start("a1", sums.at[1, top], ra.at[1], "batch")
    wires.arrived(("core", 2))
    add(2, half)
    wires.start("b2", sums.at[2, low], rb.at[1], "group")
    add(2, 0)
    add(1, half)

    def second_a(r):
        sa[r, :] = (sums[2, r, :].astype(F32) + ra[0, r, :].astype(F32)).astype(BF)

    def second_b(r):
        rr = pl.ds(r.start + half, TILE)
        sb[r, :] = (sums[1, rr, :].astype(F32) + rb[0, r, :].astype(F32)).astype(BF)

    wires.arrived("a3")
    tiles(half, second_a)
    wires.start("a2", sa, ea, "group")
    wires.arrived("b3")
    tiles(half, second_b)
    wires.start("b1", sb, eb, "batch")
    if hook(0):
        hook(0)()

    def last(first, near, end):
        def body(r):
            rr = pl.ds(r.start + first, TILE)
            total = part[0, 0, rr, :].astype(F32) + rc[0, rr, :].astype(F32)
            total = total + near[1, r, :].astype(F32) + end[r, :].astype(F32)
            pointwise(rr, total)

        tiles(half, body)

    wires.arrived(("core", 0), "a1", "a2")
    last(0, ra, ea)
    if whole is not None:
        wires.start("za", whole.at[0, 0, top], whole.at[1, 0, top], "batch")
    if hook(1):
        hook(1)()
    wires.arrived("b2", "b1")
    last(half, rb, eb)
    if whole is None:
        return
    wires.start("yb", whole.at[0, 0, low], whole.at[2, 0, low], "group")
    wires.start("zb", whole.at[0, 0, low], whole.at[1, 0, low], "batch")
    wires.start("ya", whole.at[0, 0, top], whole.at[2, 0, top], "group")
    wires.start("own", whole.at[0, 0], whole.at[0, 1], "head")
    if hook(2):
        hook(2)()
    wires.arrived("za")
    wires.start("fa", whole.at[1, 0, top], whole.at[3, 0, top], "group")
    wires.start("cza", whole.at[1, 0, top], whole.at[1, 1, top], "head")
    wires.arrived("yb")
    wires.start("fb", whole.at[2, 0, low], whole.at[3, 0, low], "batch")
    wires.start("cyb", whole.at[2, 0, low], whole.at[2, 1, low], "head")
    wires.arrived("zb")
    wires.start("czb", whole.at[1, 0, low], whole.at[1, 1, low], "head")
    wires.arrived("ya")
    wires.start("cya", whole.at[2, 0, top], whole.at[2, 1, top], "head")
    wires.arrived("fa")
    wires.start("cfa", whole.at[3, 0, top], whole.at[3, 1, top], "head")
    wires.arrived("fb")
    wires.start("cfb", whole.at[3, 0, low], whole.at[3, 1, low], "head")
    wires.arrived("own", "cza", "cyb", "czb", "cya", "cfa", "cfb")


def gather_kernel(*refs, lines, pieces):
    n = len(pieces)
    mine, others = refs[:n], refs[n : 2 * n]
    x, gain = refs[2 * n : 2 * n + 2]
    weights = refs[2 * n + 2 : 3 * n + 2]
    whole, normed, send, recv, local = refs[3 * n + 2 :]
    b = lax.axis_index("batch")
    wires, moves = Wires(send, recv, lines), Moves(local)
    wires.enter(("head", "group", "x") + along(lines))
    order = [k for k in (2, 3, 1) if k < lines] + list(range(4, lines))
    cuts = [(i, pl.ds(c, w)) for i, cols in enumerate(pieces) for c, w in cols]

    def piece(i, cut):
        for k in order:
            source = others[i] if k % 2 else mine[i]
            wires.start((i, cut.start, k), source.at[:, cut], weights[i].at[b, :, cut], ("line", k))

    def own_piece(i, cut):
        wires.start((i, cut.start, "x", 0), mine[i].at[:, cut], weights[i].at[b, :, cut], "x")

    def relay(i, cut):
        for k in order:
            wires.arrived((i, cut.start, k))
            block = weights[i].at[b ^ (2 * k), :, cut]
            wires.start((i, cut.start, "x", k), block, block, "x")

    own_piece(*cuts[0])
    for i in range(n):
        moves.start(mine[i], weights[i].at[b])

    def body(r):
        row = x[r, :].astype(F32)
        scale = lax.rsqrt(jnp.mean(row * row, axis=1, keepdims=True) + 1e-06)
        normed[r, :] = (row * scale * gain[...]).astype(BF)

    tiles(x.shape[0], body)
    wires.start("z", normed, whole.at[1, 0], ("line", 1))
    wires.start("y", normed, whole.at[2, 0], "group")
    wires.start("own", normed, whole.at[0, 1], "head")
    moves.start(normed, whole.at[0, 0])
    for at, cut in enumerate(cuts):
        piece(*cut)
        if at:
            own_piece(*cut)
    wires.arrived("z")
    wires.start("far", whole.at[1, 0], whole.at[3, 0], "group")
    wires.start("cz", whole.at[1, 0], whole.at[1, 1], "head")
    relay(*cuts[0])
    wires.arrived("y")
    wires.start("cy", whole.at[2, 0], whole.at[2, 1], "head")
    relay(*cuts[1])
    wires.arrived("far")
    wires.start("cfar", whole.at[3, 0], whole.at[3, 1], "head")
    for cut in cuts[2:]:
        relay(*cut)
    wires.arrived("own", "cz", "cy", "cfar")
    for i, cut in cuts:
        wires.arrived(*[(i, cut.start, "x", k) for k in range(lines)])
    moves.finish()
    wires.finish()


def gather_first(own, other, x, gain, batch):
    rows, width = x.shape
    lines = batch // 2
    pieces = [[(c, 512) for c in range(0, o.shape[1], 512)] for o in own]
    count = sum(len(p) for p in pieces) * 2 * lines + 8
    result = pl.pallas_call(
        functools.partial(gather_kernel, lines=lines, pieces=pieces),
        out_shape=tuple(jax.ShapeDtypeStruct((batch,) + o.shape, BF) for o in own)
        + (jax.ShapeDtypeStruct((4, 2, rows, width), BF),),
        in_specs=[vmem()] * (2 * len(own) + 2),
        out_specs=tuple([pl.BlockSpec(memory_space=pl.ANY)] * (len(own) + 1)),
        scratch_shapes=[
            pltpu.VMEM((rows, width), BF),
            pltpu.SemaphoreType.DMA((count,)),
            pltpu.SemaphoreType.DMA((count,)),
            pltpu.SemaphoreType.DMA((len(own) + 1,)),
        ],
        compiler_params=pltpu.CompilerParams(collective_id=2, has_side_effects=True, vmem_limit_bytes=16 * 2**20),
        cost_estimate=pl.CostEstimate(flops=10 * rows * width, bytes_accessed=300000000, transcendentals=0),
        name="gather_first",
    )(*own, *other, x, gain[None])
    return [w.reshape(-1, w.shape[2]) for w in result[:-1]], result[-1].reshape(8 * rows, width)


def forward_kernel(*refs, lines, widths):
    part, x, gain = refs[:3]
    got = refs[3 : 3 + lines]
    whole, hidden = refs[3 + lines : 5 + lines]
    n = len(widths)
    weights = refs[5 + lines : 5 + lines + n]
    rc, sums, ra, rb, ea, eb, sa, sb, send, recv, local = refs[5 + lines + n :]
    b = lax.axis_index("batch")
    wires, moves = Wires(send, recv, 2), Moves(local)
    wires.enter(TEAM + ("x",))

    def pointwise(r, total):
        row = x[r, :].astype(F32) + total
        hidden[r, :] = row
        shifted = row - jnp.mean(row, axis=1, keepdims=True)
        var_row = jnp.mean(shifted * shifted, axis=1, keepdims=True)
        whole[0, 0, r, :] = (shifted * lax.rsqrt(var_row + 1e-05) * gain[...]).astype(BF)

    for k in range(lines):
        first = 0
        for i, width in enumerate(widths):
            source = got[k].at[:, pl.ds(first, width)]
            block = weights[i].at[b ^ (2 * k)]
            wires.start(("x", k, i), source, block, "x")
            moves.start(source, block)
            first += width
    exchange(part, whole, rc, sums, ra, rb, ea, eb, sa, sb, wires, pointwise)
    wires.arrived(*[("x", k, i) for k in range(lines) for i in range(n)])
    moves.finish()
    wires.finish()


def backward_kernel(
    part,
    hidden,
    cotangent,
    factor,
    gain,
    grads,
    whole,
    d_hidden,
    d_gain,
    lines_out,
    rc,
    sums,
    ra,
    rb,
    ea,
    eb,
    sa,
    sb,
    rx,
    send,
    recv,
    *,
    lines,
):
    wires = Wires(send, recv, 2)
    wires.enter(TEAM + ("x",))
    x = lax.axis_index("batch") % 2
    for z in range(lines):
        wires.start(("x", z), grads.at[2 * z + 1 - x], rx.at[z], "x")
    d_gain[...] = jnp.zeros_like(d_gain)

    def pointwise(r, total):
        row = hidden[r, :]
        shifted = row - jnp.mean(row, axis=1, keepdims=True)
        var_row = jnp.mean(shifted * shifted, axis=1, keepdims=True)
        rstd = lax.rsqrt(var_row + 1e-05)
        unit = shifted * rstd
        terms = total * unit
        d_gain[...] += terms[:8] + terms[8:]
        d_unit = total * gain[...]
        mean_d = jnp.mean(d_unit, axis=1, keepdims=True)
        mean_du = jnp.mean(d_unit * unit, axis=1, keepdims=True)
        grad = cotangent[r, :].astype(F32) * factor[0, 0] + rstd * (d_unit - mean_d - unit * mean_du)
        d_hidden[r, :] = grad
        whole[0, 0, r, :] = grad.astype(BF)

    def join():
        for z in range(lines):
            wires.arrived(("x", z))

            def body(r):
                total = grads[2 * z + x, r, :].astype(F32) + rx[z, r, :].astype(F32)
                lines_out[z, r, :] = total.astype(BF)

            tiles(rx.shape[1], body)

    exchange(part, whole, rc, sums, ra, rb, ea, eb, sa, sb, wires, pointwise, (None, None, join))
    wires.finish()


def last_kernel(
    part,
    x,
    d_hidden,
    gain,
    ln_gains,
    grads,
    d_inputs,
    gains,
    slices,
    rc,
    sums,
    ra,
    rb,
    ea,
    eb,
    sa,
    sb,
    rx,
    lined,
    rz,
    held,
    came,
    send,
    recv,
    *,
    lines,
    cuts,
):
    wires = Wires(send, recv, lines)
    b = lax.axis_index("batch")
    y = lax.axis_index("group")
    xbit, z = b % 2, b // 2
    p = z % 2
    rows = rx.shape[1]
    wires.enter(("head", "group", "x") + along(lines))
    order = [k for k in (2, 3, 1) if k < lines] + list(range(4, lines))
    for at, cut in enumerate(cuts):
        for line in range(lines):
            wires.start(("x", at, line), grads.at[2 * line + 1 - xbit, :, cut], rx.at[line, :, cut], "x")

    held[0] = jnp.zeros_like(held[0])

    def pointwise(r, total):
        row = x[r, :].astype(F32)
        scale = lax.rsqrt(jnp.mean(row * row, axis=1, keepdims=True) + 1e-06)
        unit = row * scale
        terms = total * unit
        held[0, :8] += terms[:8] + terms[8:]
        d_unit = total * gain[...]
        mean_du = jnp.mean(d_unit * unit, axis=1, keepdims=True)
        d_inputs[r, :] = (d_hidden[r, :] + scale * (d_unit - unit * mean_du)).astype(BF)

    def stage_x(at):
        cut = cuts[at]
        for line in range(lines):
            wires.arrived(("x", at, line))

            def body(r):
                total = grads[2 * line + xbit, r, cut].astype(F32) + rx[line, r, cut].astype(F32)
                lined[line, r, cut] = total.astype(BF)

            tiles(rows, body)
        for k in order:
            wires.start(("z", at, k), lined.at[z ^ k, :, cut], rz.at[k, :, cut], ("line", k))

    def stage_z(at):
        cut = cuts[at]
        for k in order:
            wires.arrived(("z", at, k))

        def body(r):
            mine = lined[z, r, cut].astype(F32)
            other = jnp.zeros_like(mine)
            for k in range(1, lines):
                term = rz[k, r, cut].astype(F32)
                if k % 2:
                    other = other + term
                else:
                    mine = mine + term
            slices[2 * p + y, r, cut] = mine.astype(BF)
            slices[2 * (1 - p) + y, r, cut] = other.astype(BF)

        tiles(rows, body)
        for q in range(2):
            block = slices.at[2 * q + y, :, cut]
            wires.start(("y", at, q), block, block, "group")

    def reduce_gains():
        held[0, 8:] = ln_gains[...]
        steps = ["head", "group", "x"]
        bit = 1
        while bit < lines:
            steps.append(("line", bit))
            bit *= 2
        for at, peer in enumerate(steps):
            wires.start(("gain", at), held.at[at], came.at[at], peer)
            wires.arrived(("gain", at))
            held[at + 1] = held[at] + came[at]
        gains[...] = held[len(steps)]

    exchange(
        part,
        None,
        rc,
        sums,
        ra,
        rb,
        ea,
        eb,
        sa,
        sb,
        wires,
        pointwise,
        (lambda: stage_x(0), lambda: stage_x(1)),
    )
    stage_x(2)
    stage_z(0)
    reduce_gains()
    for at in range(3, len(cuts)):
        stage_x(at)
        stage_z(at - 2)
    for at in range(len(cuts) - 2, len(cuts)):
        stage_z(at)
    for at in range(len(cuts)):
        wires.arrived(("y", at, 0), ("y", at, 1))
    wires.finish()


def exchange_scratch(rows, width):
    half = rows // 2
    return [
        pltpu.VMEM((4, rows, width), BF),
        pltpu.VMEM((4, rows, width), BF),
        pltpu.VMEM((2, half, width), BF),
        pltpu.VMEM((2, half, width), BF),
        pltpu.VMEM((half, width), BF),
        pltpu.VMEM((half, width), BF),
        pltpu.VMEM((half, width), BF),
        pltpu.VMEM((half, width), BF),
    ]


def semaphores(count):
    return [pltpu.SemaphoreType.DMA((count,)), pltpu.SemaphoreType.DMA((count,))]


def vmem():
    return pl.BlockSpec(memory_space=pltpu.VMEM)


def forward_exchange(part, x, gain, got, widths, batch):
    rows, width = x.shape
    lines = batch // 2
    n = len(widths)
    result = pl.pallas_call(
        functools.partial(forward_kernel, lines=lines, widths=widths),
        out_shape=(
            jax.ShapeDtypeStruct((4, 2, rows, width), BF),
            jax.ShapeDtypeStruct((rows, width), F32),
        )
        + tuple(jax.ShapeDtypeStruct((batch, width // batch, w), BF) for w in widths),
        in_specs=[vmem()] * (3 + lines),
        out_specs=(vmem(), vmem()) + tuple([pl.BlockSpec(memory_space=pl.ANY)] * n),
        scratch_shapes=exchange_scratch(rows, width)
        + semaphores(24 + lines * n)
        + [pltpu.SemaphoreType.DMA((lines * n,))],
        compiler_params=pltpu.CompilerParams(collective_id=0, has_side_effects=True, vmem_limit_bytes=46 * 2**20),
        cost_estimate=pl.CostEstimate(flops=10 * rows * width, bytes_accessed=300000000, transcendentals=0),
        name="forward_exchange",
    )(part.reshape(4, 2, rows, width), x, gain[None], *got)
    return result[0].reshape(8 * rows, width), result[1], [w.reshape(width, -1) for w in result[2:]]


def backward_exchange(part, hidden, cotangent, factor, gain, grads, batch):
    rows, width = hidden.shape
    lines = batch // 2
    block = (width // batch, grads.shape[1])
    whole, d_hidden, d_gain, lined = pl.pallas_call(
        functools.partial(backward_kernel, lines=lines),
        out_shape=(
            jax.ShapeDtypeStruct((4, 2, rows, width), BF),
            jax.ShapeDtypeStruct((rows, width), F32),
            jax.ShapeDtypeStruct((8, width), F32),
            jax.ShapeDtypeStruct((lines,) + block, BF),
        ),
        in_specs=[vmem()] * 3 + [pl.BlockSpec(memory_space=pltpu.SMEM), vmem(), vmem()],
        out_specs=(vmem(), vmem(), vmem(), vmem()),
        scratch_shapes=exchange_scratch(rows, width)
        + [pltpu.VMEM((lines,) + block, BF)]
        + semaphores(24 + lines),
        compiler_params=pltpu.CompilerParams(collective_id=1, has_side_effects=True, vmem_limit_bytes=50 * 2**20),
        cost_estimate=pl.CostEstimate(flops=10 * rows * width, bytes_accessed=300000000, transcendentals=0),
        name="backward_exchange",
    )(
        part.reshape(4, 2, rows, width),
        hidden,
        cotangent,
        factor.reshape(1, 1),
        gain[None],
        grads.reshape((batch,) + block),
    )
    return whole.reshape(8 * rows, width), d_hidden, d_gain, lined


def last_exchange(part, x, d_hidden, gain, ln_gains, grads, batch):
    rows, width = x.shape
    lines = batch // 2
    block = (width // batch, grads.shape[1])
    cuts = [pl.ds(c, 256) for c in range(0, block[1], 256)]
    steps = 2 + batch.bit_length() - 1
    d_inputs, gains, slices = pl.pallas_call(
        functools.partial(last_kernel, lines=lines, cuts=cuts),
        out_shape=(
            jax.ShapeDtypeStruct((rows, width), BF),
            jax.ShapeDtypeStruct((16, width), F32),
            jax.ShapeDtypeStruct((4,) + block, BF),
        ),
        in_specs=[vmem()] * 6,
        out_specs=(vmem(), vmem(), vmem()),
        scratch_shapes=exchange_scratch(rows, width)
        + [pltpu.VMEM((lines,) + block, BF)] * 3
        + [pltpu.VMEM((steps + 1, 16, width), F32), pltpu.VMEM((steps, 16, width), F32)]
        + semaphores(16 + steps + len(cuts) * (2 * lines + 1)),
        compiler_params=pltpu.CompilerParams(collective_id=3, has_side_effects=True, vmem_limit_bytes=50 * 2**20),
        cost_estimate=pl.CostEstimate(flops=10 * rows * width, bytes_accessed=300000000, transcendentals=0),
        name="last_exchange",
    )(part.reshape(4, 2, rows, width), x, d_hidden, gain[None], ln_gains, grads.reshape((batch,) + block))
    return d_inputs, gains, slices


class Place:
    def __init__(self):
        self.batch = lax.axis_size("batch")
        self.b = lax.axis_index("batch")
        self.y = lax.axis_index("group")
        self.c = lax.axis_index("head")
        self.lines = self.batch // 2
        self.z = self.b // 2
        self.x = self.b % 2
        self.p = self.z % 2
        self.slot = 2 * self.p + self.y

    def cut(self, array, axis):
        width = array.shape[axis] // 4
        own = lax.dynamic_slice_in_dim(array, self.slot * width, width, axis)
        other = lax.dynamic_slice_in_dim(array, (self.slot ^ 2) * width, width, axis)
        return own, other

    def along_lines(self, own, other):
        return [own] + [swap_batch(other if k % 2 else own, 2 * k) for k in range(1, self.lines)]

    def across(self, grads):
        blocks = grads.reshape(self.lines, 2, -1, grads.shape[1])
        keep = lax.dynamic_index_in_dim(blocks, self.x, 1, keepdims=False)
        give = lax.dynamic_index_in_dim(blocks, self.x ^ 1, 1, keepdims=False)
        return (keep.astype(F32) + swap_batch(give, 1).astype(F32)).astype(BF)

    def down_lines(self, lines):
        mine = lax.dynamic_index_in_dim(lines, self.z, 0, keepdims=False).astype(F32)
        other = jnp.zeros_like(mine)
        for k in range(1, self.lines):
            piece = lax.dynamic_index_in_dim(lines, self.z ^ k, 0, keepdims=False)
            piece = swap_batch(piece, 2 * k).astype(F32)
            if k % 2:
                other = other + piece
            else:
                mine = mine + piece
        first = self.p == 0
        here = jnp.stack([jnp.where(first, mine, other), jnp.where(first, other, mine)], axis=0).astype(BF)
        there = swap_group(here)
        low = self.y == 0
        pairs = jnp.stack([jnp.where(low, here, there), jnp.where(low, there, here)], axis=1)
        return pairs.reshape((4,) + mine.shape)


def columns(slices):
    return jnp.transpose(slices, (1, 0, 2)).reshape(slices.shape[1], -1).astype(F32)


def on_device(
    inputs,
    rms_gain,
    w_query,
    w_key,
    w_value,
    w_gate,
    w_out,
    ln_gain,
    w_up,
    w_down,
    cotangent,
    domain_of,
    domain_weight,
):
    here = Place()
    local = inputs[0].astype(F32)
    half = local.shape[0]
    length = 2 * half

    parts = [here.cut(w, 1) for w in (w_query, w_key, w_value, w_gate)]
    own = jnp.concatenate([own for own, _ in parts], axis=1)
    other = jnp.concatenate([other for _, other in parts], axis=1)
    out_own, out_other = [v.T for v in here.cut(w_out, 0)]
    (stacked, out_t), normed_all = gather_first(
        (own, out_own), (other, out_other), inputs[0], rms_gain, here.batch
    )

    factor = sequence_factor(domain_of, domain_weight)
    own_index = here.b * lax.axis_size("group") + here.y
    own_factor = lax.dynamic_index_in_dim(factor, own_index, 0, keepdims=False)
    d_out = cotangent[0].astype(F32) * own_factor

    up_parts, down_parts = here.cut(w_up, 1), here.cut(w_down, 0)
    both = [jnp.concatenate([u, v.T], axis=1) for u, v in zip(up_parts, down_parts)]
    both = [after(v, stacked) for v in both]
    got = here.along_lines(*both)
    d_ffn_all = spread(after(d_out.astype(BF), stacked))

    places = (jnp.arange(length, dtype=jnp.int32) + here.c * half) % length
    cosine, sine = rotary_tables(places, KEY)
    decays = decay_mask(places, here.c * 4 + here.slot)

    projected = mm(normed_all, stacked, 1, 0)

    def rotary(block):
        return block * cosine[None] + rotate_half(block) * sine[None]

    def unrotary(block):
        turned = block * sine[None]
        width = turned.shape[-1] // 2
        return block * cosine[None] + jnp.concatenate([turned[..., width:], -turned[..., :width]], axis=-1)

    queries = projected[:, :KEY].reshape(4, length, KEY)
    keys = projected[:, KEY : 2 * KEY].reshape(4, length, KEY)
    v_low = projected[:, 2 * KEY : 2 * KEY + VAL].astype(BF).reshape(4, length, VAL)
    gates = projected[:, 2 * KEY + VAL :].reshape(4, length, VAL)
    q_rot = rotary(queries).astype(BF)
    k_rot = rotary(keys).astype(BF)
    scores = jnp.einsum("snk,smk->snm", q_rot, k_rot, preferred_element_type=F32)
    weighted = (scores * decays[None]).astype(BF)
    retained = jnp.einsum("snm,smv->snv", weighted, v_low, preferred_element_type=F32)
    mixed, mix_back = jax.vjp(gate_mix, retained, gates)
    mixed_low = mixed.astype(BF).reshape(4 * length, VAL)
    ln_all, hidden, (up, down_t) = forward_exchange(
        mm(mixed_low, out_t, 1, 1, BF), inputs[0], ln_gain, got, (up_parts[0].shape[1], down_parts[0].shape[0]), here.batch
    )
    pre_act = mm(ln_all, up, 1, 0)
    lifted, gelu_back = jax.vjp(gelu_tanh, pre_act)
    lifted_low = lifted.astype(BF)

    d_lifted = mm(d_ffn_all, down_t, 1, 0)
    (d_pre,) = gelu_back(d_lifted)
    d_pre_low = d_pre.astype(BF)
    ffn_grads = jnp.concatenate([mm(ln_all, d_pre_low, 0, 0, BF), mm(d_ffn_all, lifted_low, 0, 0, BF)], axis=1)
    d_attn_all, d_hidden, d_ln_gain, ffn_lines = backward_exchange(
        mm(d_pre_low, up, 1, 1, BF), hidden, cotangent[0], own_factor, ln_gain, ffn_grads, here.batch
    )
    ffn_out = collect(mm(after(lifted_low, d_attn_all), down_t, 1, 1, BF))
    output = (hidden + ffn_out).astype(BF)[None]
    grad_ffn = here.down_lines(ffn_lines)
    grad_out = here.down_lines(here.across(mm(d_attn_all, mixed_low, 0, 0, BF)))

    d_mixed = mm(d_attn_all, out_t, 1, 0).reshape(4, length, VAL)
    d_retained, d_gates = mix_back(d_mixed)
    d_ret_low = d_retained.astype(BF)
    d_values = jnp.einsum("snm,snv->smv", weighted, d_ret_low, preferred_element_type=F32)
    d_weighted = jnp.einsum("snv,smv->snm", d_ret_low, v_low, preferred_element_type=F32)
    d_scores = (d_weighted * decays[None]).astype(BF)
    d_q_rot = jnp.einsum("snm,smk->snk", d_scores, k_rot, preferred_element_type=F32)
    d_k_rot = jnp.einsum("snm,snk->smk", d_scores, q_rot, preferred_element_type=F32)
    d_proj = jnp.concatenate(
        [unrotary(d_q_rot).astype(BF), unrotary(d_k_rot).astype(BF), d_values.astype(BF), d_gates.astype(BF)], axis=-1
    ).reshape(4 * length, -1)
    d_inputs, gains, grad_rows = last_exchange(
        mm(d_proj, stacked, 1, 1, BF),
        inputs[0],
        d_hidden,
        rms_gain,
        d_ln_gain,
        mm(normed_all, d_proj, 0, 0, BF),
        here.batch,
    )
    gain_rms = jnp.sum(gains[:8], axis=0)
    gain_ln = jnp.sum(gains[8:], axis=0)
    units = up_parts[0].shape[1]
    return (
        output,
        d_inputs[None],
        gain_rms,
        columns(grad_rows[:, :, :KEY]),
        columns(grad_rows[:, :, KEY : 2 * KEY]),
        columns(grad_rows[:, :, 2 * KEY : 2 * KEY + VAL]),
        columns(grad_rows[:, :, 2 * KEY + VAL :]),
        columns(grad_out).T,
        gain_ln,
        columns(grad_ffn[:, :, :units]),
        columns(grad_ffn[:, :, units:]).T,
    )


def solution(mesh):
    rows = P(("batch", "group"), "head", None)
    wide = P("batch", "head")
    tall = P("head", "batch")
    return jax.shard_map(
        on_device,
        mesh=mesh,
        in_specs=(rows, P(), wide, wide, wide, wide, tall, P(), wide, tall, rows, P(), P()),
        out_specs=(rows, rows, P(), wide, wide, wide, wide, tall, P(), wide, tall),
        check_vma=False,
    )
```

```python
import functools

import jax
import jax.numpy as jnp
import numpy as np
from jax import lax
from jax.experimental import pallas as pl
from jax.experimental.pallas import tpu as pltpu
from jax.sharding import PartitionSpec as P


KEY = 256
VAL = 512
BF = jnp.bfloat16
F32 = jnp.float32


def rotary_tables(places, width):
    ramp = jnp.linspace(jnp.float32(0.0), jnp.float32(1.0), width // 2).astype(F32)
    freqs = jnp.exp(-ramp * jnp.log(jnp.float32(10000.0)))
    angles = places.astype(F32)[:, None] * freqs[None, :]
    angles = jnp.concatenate([angles, angles], axis=1)
    return jnp.cos(angles), jnp.sin(angles)


def decay_mask(places, head_id):
    exponent = (jnp.float32(-5.0) - head_id.astype(F32)) * jnp.log(jnp.float32(2.0))
    log_keep = jnp.log1p(-jnp.exp(exponent))
    offset = places[:, None] - places[None, :]
    steps = jnp.maximum(offset, 0).astype(F32)
    return jnp.where(offset >= 0, jnp.exp(steps * log_keep), jnp.float32(0.0))


def sequence_factor(domain_of, domain_weight):
    same = (domain_of[:, None] == domain_of[None, :]).astype(F32)
    counts = jnp.sum(same, axis=1)
    domain_ids = jnp.arange(domain_weight.shape[0], dtype=jnp.int32)
    onehot = (domain_of[:, None] == domain_ids[None, :]).astype(F32)
    weight_seq = jnp.sum(onehot * domain_weight.astype(F32)[None, :], axis=1)
    total = jnp.sum(weight_seq / counts)
    return jnp.float32(domain_of.shape[0]) * weight_seq / (counts * total)


def gelu_tanh(pre_act):
    return jax.nn.gelu(pre_act, approximate=True)


def mm(left, right, left_dim, right_dim, out=F32):
    return lax.dot_general(
        left, right, (((left_dim,), (right_dim,)), ((), ())), preferred_element_type=F32
    ).astype(out)


TEAM = ("head", "batch", "group")


def peers(lines):
    b = lax.axis_index("batch")
    table = {
        "head": {"head": 1 - lax.axis_index("head")},
        "batch": {"batch": b ^ 2},
        "group": {"group": 1 - lax.axis_index("group")},
        "x": {"batch": b ^ 1},
    }
    for k in range(1, lines):
        table["line", k] = {"batch": b ^ (2 * k)}
    return table


def along(lines):
    return tuple(("line", k) for k in range(1, lines))


class Wires:
    def __init__(self, send, recv, lines=1):
        self.send, self.recv, self.made, self.peers = send, recv, {}, peers(lines)

    def enter(self, names):
        barrier = pltpu.get_barrier_semaphore()
        for name in names:
            pl.semaphore_signal(barrier, inc=1, device_id=self.peers[name], device_id_type=pl.DeviceIdType.MESH)
        pl.semaphore_wait(barrier, len(names))

    def start(self, name, source, target, peer):
        n = len(self.made)
        copy = pltpu.make_async_remote_copy(
            src_ref=source,
            dst_ref=target,
            send_sem=self.send.at[n],
            recv_sem=self.recv.at[n],
            device_id=self.peers[peer],
            device_id_type=pl.DeviceIdType.MESH,
        )
        copy.start()
        self.made[name] = copy

    def arrived(self, *names):
        for name in names:
            self.made[name].wait_recv()

    def finish(self):
        for copy in self.made.values():
            copy.wait_send()


class Moves:
    def __init__(self, sems):
        self.sems, self.made = sems, []

    def start(self, source, target):
        copy = pltpu.make_async_copy(source, target, self.sems.at[len(self.made)])
        copy.start()
        self.made.append(copy)

    def finish(self):
        for copy in self.made:
            copy.wait()


TILE = 16


def tiles(rows, body):
    def step(i, _):
        body(pl.ds(pl.multiple_of(i * TILE, TILE), TILE))
        return 0

    lax.fori_loop(0, rows // TILE, step, 0)


def exchange(part, whole, rc, sums, ra, rb, ea, eb, sa, sb, wires, pointwise, tag=""):
    rows = part.shape[2]
    half = rows // 2
    top, low = pl.ds(0, half), pl.ds(half, half)

    def start(name, *rest):
        wires.start(tag + name, *rest)

    def arrived(*names):
        wires.arrived(*[tag + name for name in names])

    def add(s, first):
        def body(r):
            rr = pl.ds(r.start + first, TILE)
            total = part[s, 0, rr, :].astype(F32) + rc[s, rr, :].astype(F32)
            sums[s, rr, :] = total.astype(BF)

        tiles(half, body)

    arrived("c3")
    add(3, 0)
    start("a3", sums.at[3, top], ra.at[0], "batch")
    add(3, half)
    start("b3", sums.at[3, low], rb.at[0], "group")
    arrived("c1")
    add(1, 0)
    start("a1", sums.at[1, top], ra.at[1], "batch")
    arrived("c2")
    add(2, half)
    start("b2", sums.at[2, low], rb.at[1], "group")
    add(2, 0)
    add(1, half)

    def second_a(r):
        sa[r, :] = (sums[2, r, :].astype(F32) + ra[0, r, :].astype(F32)).astype(BF)

    def second_b(r):
        rr = pl.ds(r.start + half, TILE)
        sb[r, :] = (sums[1, rr, :].astype(F32) + rb[0, r, :].astype(F32)).astype(BF)

    yield
    arrived("a3")
    tiles(half, second_a)
    start("a2", sa, ea, "group")
    arrived("b3")
    tiles(half, second_b)
    start("b1", sb, eb, "batch")

    def last(first, near, end):
        def body(r):
            rr = pl.ds(r.start + first, TILE)
            total = part[0, 0, rr, :].astype(F32) + rc[0, rr, :].astype(F32)
            total = total + near[1, r, :].astype(F32) + end[r, :].astype(F32)
            pointwise(rr, total)

        tiles(half, body)

    yield
    arrived("c0", "a1", "a2")
    last(0, ra, ea)
    if whole is not None:
        start("za", whole.at[0, 0, top], whole.at[1, 0, top], "batch")
    yield
    arrived("b2", "b1")
    last(half, rb, eb)
    if whole is None:
        return
    start("yb", whole.at[0, 0, low], whole.at[2, 0, low], "group")
    start("zb", whole.at[0, 0, low], whole.at[1, 0, low], "batch")
    start("ya", whole.at[0, 0, top], whole.at[2, 0, top], "group")
    start("own", whole.at[0, 0], whole.at[0, 1], "head")
    yield
    arrived("za")
    start("fa", whole.at[1, 0, top], whole.at[3, 0, top], "group")
    start("cza", whole.at[1, 0, top], whole.at[1, 1, top], "head")
    arrived("yb")
    start("fb", whole.at[2, 0, low], whole.at[3, 0, low], "batch")
    start("cyb", whole.at[2, 0, low], whole.at[2, 1, low], "head")
    yield
    arrived("zb")
    start("czb", whole.at[1, 0, low], whole.at[1, 1, low], "head")
    arrived("ya")
    start("cya", whole.at[2, 0, top], whole.at[2, 1, top], "head")
    yield
    arrived("fa")
    start("cfa", whole.at[3, 0, top], whole.at[3, 1, top], "head")
    arrived("fb")
    start("cfb", whole.at[3, 0, low], whole.at[3, 1, low], "head")
    arrived("own", "cza", "cyb", "czb", "cya", "cfa", "cfb")


def reduce_rows(part, rc, ry, rn, wires, pointwise, tag=""):
    rows = part.shape[2]
    half = rows // 2
    ends = [pl.ds(0, half), pl.ds(half, half)]

    def add(s, end):
        def body(r):
            rr = pl.ds(r.start + end.start, TILE)
            total = part[s, 0, rr, :].astype(F32) + rc[s, rr, :].astype(F32)
            part[s, 0, rr, :] = total.astype(BF)

        tiles(half, body)

    for s, at in ((3, 0), (2, 1)):
        wires.arrived(f"{tag}c{s}")
        for h, end in enumerate(ends):
            add(s, end)
            wires.start((tag, s, h), part.at[s, 0, end], ry.at[at, end], "group")
        yield
    wires.arrived(f"{tag}c1")
    for end in ends:
        add(1, end)
    yield
    for h, end in enumerate(ends):
        wires.arrived((tag, 3, h))

        def body(r):
            rr = pl.ds(r.start + end.start, TILE)
            total = part[1, 0, rr, :].astype(F32) + ry[0, rr, :].astype(F32)
            part[1, 0, rr, :] = total.astype(BF)

        tiles(half, body)
        wires.start((tag, 1, h), part.at[1, 0, end], rn.at[end], "batch")
    yield
    wires.arrived(f"{tag}c0")
    for h, end in enumerate(ends):
        wires.arrived((tag, 2, h), (tag, 1, h))

        def last(r):
            rr = pl.ds(r.start + end.start, TILE)
            total = part[0, 0, rr, :].astype(F32) + rc[0, rr, :].astype(F32)
            pointwise(rr, total + ry[1, rr, :].astype(F32) + rn[rr, :].astype(F32))

        tiles(half, last)


def send_cores(part, rc, wires, slots=(3, 1, 2, 0), tag=""):
    for s in slots:
        wires.start(tag + f"c{s}", part.at[s, 1], rc.at[s], "head")


def drive(steps, hooks=()):
    hooks = list(hooks)
    for _ in steps:
        if hooks:
            hook = hooks.pop(0)
            if hook:
                hook()
    for hook in hooks:
        hook()


def dot(left, right, left_dim, right_dim):
    return lax.dot_general(left, right, (((left_dim,), (right_dim,)), ((), ())), preferred_element_type=F32)


def blocks(count, body):
    def step(i, _):
        body(i)
        return 0

    lax.fori_loop(0, count, step, 0)


def span(i, size):
    return pl.ds(pl.multiple_of(i * size, size), size)


def gather_kernel(
    own,
    own_out,
    other,
    other_out,
    x,
    gain,
    cotangent,
    factor,
    stacked_hbm,
    out_t,
    normed_hbm,
    d_ffn,
    mixed,
    *rest,
    lines,
):
    saved_hbm, rest = rest[:7], rest[7:]
    stacked, whole, normed, d_rows, cosine, sine, decays, unit_full = rest[:8]
    saved, (send, recv, local) = rest[8:15], rest[15:]
    gates, unit, rstd, values, q_rot, k_rot, weighted = saved
    b, c = lax.axis_index("batch"), lax.axis_index("head")
    slot = 2 * ((b // 2) % 2) + lax.axis_index("group")
    wires, moves = Wires(send, recv, lines), Moves(local)
    wires.enter(("head", "group", "x") + along(lines))
    order = first_order(lines)
    half, wide = x.shape
    length = 2 * half
    key, val = q_rot.shape[2], values.shape[2]
    cuts = [(0, pl.ds(0, 512)), (0, pl.ds(512, 512)), (0, pl.ds(1024, 256)), (0, pl.ds(1280, 256))]
    cuts += [(1, pl.ds(0, 256)), (1, pl.ds(256, 256))]
    mine, others, weights = (own, own_out), (other, other_out), (stacked, out_t)

    def piece(i, cut):
        for k in order:
            source = others[i] if k % 2 else mine[i]
            wires.start((i, cut.start, k), source.at[:, cut], weights[i].at[b, :, cut], ("line", k))
        wires.start((i, cut.start, "x", 0), mine[i].at[:, cut], weights[i].at[b, :, cut], "x")

    def relay(i, cut):
        for k in order:
            wires.arrived((i, cut.start, k))
            block = weights[i].at[b ^ (2 * k), :, cut]
            wires.start((i, cut.start, "x", k), block, block, "x")

    def ready(i, cut):
        wires.arrived(*[(i, cut.start, "x", k) for k in range(lines)])

    def body(r):
        row = x[r, :].astype(F32)
        scale = lax.rsqrt(jnp.mean(row * row, axis=1, keepdims=True) + 1e-06)
        normed[r, :] = (row * scale * gain[...]).astype(BF)
        d_rows[r, :] = (cotangent[r, :].astype(F32) * factor[0, 0]).astype(BF)

    tiles(half, body)
    wires.start("z", normed, whole.at[1, 0], ("line", 1))
    wires.start("y", normed, whole.at[2, 0], "group")
    wires.start("own", normed, whole.at[0, 1], "head")
    moves.start(normed, whole.at[0, 0])
    for i in range(2):
        moves.start(mine[i], weights[i].at[b])
    for cut in cuts[:4]:
        piece(*cut)
    wires.start("dy", d_rows, d_ffn.at[2, 0], "group")
    wires.start("dz", d_rows, d_ffn.at[1, 0], ("line", 1))
    wires.start("down", d_rows, d_ffn.at[0, 1], "head")
    moves.start(d_rows, d_ffn.at[0, 0])
    for cut in cuts[4:]:
        piece(*cut)

    lane = lax.broadcasted_iota(jnp.int32, (half, key // 2), 1).astype(F32)
    freqs = jnp.exp(lane * jnp.float32(-np.log(10000.0) / (key // 2 - 1)))
    for h in range(2):
        first = (h * half + c * half) % length
        places = (lax.broadcasted_iota(jnp.int32, (half, key // 2), 0) + first).astype(F32)
        cosine[pl.ds(h * half, half), :] = jnp.cos(places * freqs)
        sine[pl.ds(h * half, half), :] = jnp.sin(places * freqs)
    head = 4 * c + slot
    log_keep = jnp.float32(0)
    for h in range(8):
        log_keep = jnp.where(head == h, jnp.float32(np.log1p(-(2.0 ** (-5 - h)))), log_keep)

    def decay_rows(r):
        n = lax.broadcasted_iota(jnp.int32, (TILE, length), 0) + r.start
        m = lax.broadcasted_iota(jnp.int32, (TILE, length), 1)
        offset = (n + c * half) % length - (m + c * half) % length
        steps = jnp.maximum(offset, 0).astype(F32)
        decays[r, :] = jnp.where(offset >= 0, jnp.exp(steps * log_keep), jnp.float32(0))

    tiles(length, decay_rows)

    rows = whole.reshape(4, length, wide)
    flat = stacked.reshape(wide, stacked.shape[2])

    def turn(s):
        total = dot(rows[s], flat[:, pl.ds(0, 2 * key)], 1, 0)
        for target, at in ((q_rot, 0), (k_rot, key)):
            a, b_ = total[:, at : at + key // 2], total[:, at + key // 2 : at + key]
            target[s, :, pl.ds(0, key // 2)] = (a * cosine[...] - b_ * sine[...]).astype(BF)
            target[s, :, pl.ds(key // 2, key // 2)] = (b_ * cosine[...] + a * sine[...]).astype(BF)

    def retain(s):
        values[s] = dot(rows[s], flat[:, pl.ds(2 * key, val)], 1, 0).astype(BF)
        weighted[s] = (dot(q_rot[s], k_rot[s], 1, 1) * decays[...]).astype(BF)

        def part(i):
            r = span(i, half)
            retained = dot(weighted[s, r, :], values[s], 1, 0)
            centered = retained - jnp.mean(retained, axis=1, keepdims=True)
            scale = lax.rsqrt(jnp.mean(centered * centered, axis=1, keepdims=True) + 1e-05)
            full = centered * scale
            unit_full[s, r, :] = full
            unit[s, r, :] = full.astype(BF)
            rstd[s, r, :] = jnp.broadcast_to(scale, (half, rstd.shape[2]))

        blocks(2, part)

    def mix(s):
        def part(i):
            r = span(i, half)
            gate = dot(rows[s, r, :], flat[:, pl.ds(2 * key + val, val)], 1, 0)
            gates[s, r, :] = gate.astype(BF)
            mixed[s, r, :] = (unit_full[s, r, :] * (gate * jax.nn.sigmoid(gate))).astype(BF)

        blocks(2, part)

    wires.arrived("z")
    wires.start("far", whole.at[1, 0], whole.at[3, 0], "group")
    wires.start("cz", whole.at[1, 0], whole.at[1, 1], "head")
    wires.arrived("y")
    wires.start("cy", whole.at[2, 0], whole.at[2, 1], "head")
    relay(*cuts[0])
    wires.arrived("far")
    wires.start("cfar", whole.at[3, 0], whole.at[3, 1], "head")
    relay(*cuts[1])
    wires.arrived("dz")
    wires.start("dfar", d_ffn.at[1, 0], d_ffn.at[3, 0], "group")
    wires.start("dcz", d_ffn.at[1, 0], d_ffn.at[1, 1], "head")
    moves.finish()
    wires.arrived("own", "cz", "cy", "cfar")
    ready(*cuts[0])
    keep = Moves(local.at[pl.ds(8, 10)])
    keep.start(whole, normed_hbm)
    turn(0)
    turn(1)
    relay(*cuts[2])
    turn(2)
    turn(3)
    relay(*cuts[3])
    ready(*cuts[1])
    retain(0)
    retain(1)
    wires.arrived("dy")
    wires.start("dcy", d_ffn.at[2, 0], d_ffn.at[2, 1], "head")
    retain(2)
    retain(3)
    relay(*cuts[4])
    ready(*cuts[2])
    ready(*cuts[3])
    keep.start(stacked, stacked_hbm)
    for n in range(1, 7):
        keep.start(saved[n], saved_hbm[n])
    mix(0)
    mix(1)
    relay(*cuts[5])
    mix(2)
    mix(3)
    keep.start(gates, saved_hbm[0])
    wires.arrived("dfar")
    wires.start("dcfar", d_ffn.at[3, 0], d_ffn.at[3, 1], "head")
    ready(*cuts[4])
    ready(*cuts[5])
    wires.arrived("down", "dcz", "dcy", "dcfar")
    keep.finish()
    wires.finish()


def gather_first(own, other, x, gain, cotangent, factor, key, batch):
    rows, width = x.shape
    lines = batch // 2
    length = 2 * rows
    val = own[1].shape[1]
    high, columns = own[0].shape
    saved = [
        jax.ShapeDtypeStruct((4, length, w), t)
        for w, t in ((val, BF), (val, BF), (128, F32), (val, BF), (key, BF), (key, BF), (length, BF))
    ]
    result = pl.pallas_call(
        functools.partial(gather_kernel, lines=lines),
        out_shape=(
            jax.ShapeDtypeStruct((batch, high, columns), BF),
            jax.ShapeDtypeStruct((batch, high, val), BF),
            jax.ShapeDtypeStruct((4, 2, rows, width), BF),
            jax.ShapeDtypeStruct((4, 2, rows, width), BF),
            jax.ShapeDtypeStruct((4, length, val), BF),
            *saved,
        ),
        in_specs=[vmem()] * 7 + [pl.BlockSpec(memory_space=pltpu.SMEM)],
        out_specs=(anywhere(), vmem(), anywhere(), anywhere(), vmem()) + tuple([anywhere()] * 7),
        scratch_shapes=[
            pltpu.VMEM((batch, high, columns), BF),
            pltpu.VMEM((4, 2, rows, width), BF),
            pltpu.VMEM((rows, width), BF),
            pltpu.VMEM((rows, width), BF),
            pltpu.VMEM((length, key // 2), F32),
            pltpu.VMEM((length, key // 2), F32),
            pltpu.VMEM((length, length), F32),
            pltpu.VMEM((4, length, val), F32),
        ]
        + [pltpu.VMEM(v.shape, v.dtype) for v in saved]
        + semaphores(6 * 2 * lines + 16)
        + [pltpu.SemaphoreType.DMA((18,))],
        compiler_params=pltpu.CompilerParams(collective_id=2, has_side_effects=True, vmem_limit_bytes=56 * 2**20),
        cost_estimate=pl.CostEstimate(flops=20 * 10**9, bytes_accessed=300000000, transcendentals=0),
        name="gather_first",
    )(*own, *other, x, gain[None], cotangent, factor.reshape(1, 1))
    stacked, out_t, normed, d_ffn, mixed = result[:5]
    return (
        stacked.reshape(-1, columns),
        out_t.reshape(-1, val),
        normed.reshape(8 * rows, width),
        d_ffn.reshape(8 * rows, width),
        mixed,
        result[5:],
    )


def forward_kernel(
    part, x, gain, own_up, own_down, other_up, other_down, whole, hidden, up, down, rc, sums, ra, rb, ea, eb, sa, sb, send, recv, local, *, lines
):
    b = lax.axis_index("batch")
    wires, moves = Wires(send, recv, lines), Moves(local)
    wires.enter(("head", "group", "x") + along(lines))
    order = first_order(lines)
    mine, others, weights = (own_up, own_down), (other_up, other_down), (up, down)

    def pointwise(r, total):
        row = x[r, :].astype(F32) + total
        hidden[r, :] = row
        shifted = row - jnp.mean(row, axis=1, keepdims=True)
        var_row = jnp.mean(shifted * shifted, axis=1, keepdims=True)
        whole[0, 0, r, :] = (shifted * lax.rsqrt(var_row + 1e-05) * gain[...]).astype(BF)

    def piece(i):
        for k in order:
            source = others[i] if k % 2 else mine[i]
            wires.start((i, k), source, weights[i].at[b], ("line", k))

    def relay(i):
        for k in order:
            wires.arrived((i, k))
            block = weights[i].at[b ^ (2 * k)]
            wires.start((i, "x", k), block, block, "x")

    send_cores(part, rc, wires)
    for i in range(2):
        wires.start((i, "x", 0), mine[i], weights[i].at[b], "x")
        moves.start(mine[i], weights[i].at[b])
    steps = exchange(part, whole, rc, sums, ra, rb, ea, eb, sa, sb, wires, pointwise)
    drive(steps, (lambda: piece(0), lambda: piece(1), None, lambda: relay(0), None, lambda: relay(1)))
    wires.arrived(*[(i, "x", k) for i in range(2) for k in range(lines)])
    moves.finish()
    wires.finish()


def backward_kernel(
    part,
    hidden,
    cotangent,
    factor,
    gain,
    grads,
    whole,
    d_hidden,
    d_gain,
    lines_out,
    rc,
    sums,
    ra,
    rb,
    ea,
    eb,
    sa,
    sb,
    rx,
    send,
    recv,
    *,
    lines,
):
    wires = Wires(send, recv, 2)
    wires.enter(TEAM + ("x",))
    x = lax.axis_index("batch") % 2
    for z in range(lines):
        wires.start(("x", z), grads.at[2 * z + 1 - x], rx.at[z], "x")
    d_gain[...] = jnp.zeros_like(d_gain)

    def pointwise(r, total):
        row = hidden[r, :]
        shifted = row - jnp.mean(row, axis=1, keepdims=True)
        var_row = jnp.mean(shifted * shifted, axis=1, keepdims=True)
        rstd = lax.rsqrt(var_row + 1e-05)
        unit = shifted * rstd
        terms = total * unit
        d_gain[...] += terms[:8] + terms[8:]
        d_unit = total * gain[...]
        mean_d = jnp.mean(d_unit, axis=1, keepdims=True)
        mean_du = jnp.mean(d_unit * unit, axis=1, keepdims=True)
        grad = cotangent[r, :].astype(F32) * factor[0, 0] + rstd * (d_unit - mean_d - unit * mean_du)
        d_hidden[r, :] = grad
        whole[0, 0, r, :] = grad.astype(BF)

    def join():
        for z in range(lines):
            wires.arrived(("x", z))

            def body(r):
                total = grads[2 * z + x, r, :].astype(F32) + rx[z, r, :].astype(F32)
                lines_out[z, r, :] = total.astype(BF)

            tiles(rx.shape[1], body)

    send_cores(part, rc, wires)
    drive(exchange(part, whole, rc, sums, ra, rb, ea, eb, sa, sb, wires, pointwise), (None, None, None, join))
    wires.finish()


def first_order(lines):
    return [k for k in (2, 3, 1) if k < lines] + list(range(4, lines))


class Lines:
    def __init__(self, wires, lined, rz, slices, lines, tag, pick=lambda line: line):
        self.wires, self.lined, self.rz, self.slices, self.lines, self.tag = wires, lined, rz, slices, lines, tag
        self.pick = pick
        self.z = lax.axis_index("batch") // 2
        self.p = self.z % 2
        self.y = lax.axis_index("group")
        self.order = first_order(lines)

    def send(self, cut):
        for k in self.order:
            source = self.lined.at[self.pick(self.z ^ k), :, cut]
            self.wires.start((self.tag, "z", cut.start, k), source, self.rz.at[k, :, cut], ("line", k))

    def join(self, cut):
        lined, rz, slices, p, y = self.lined, self.rz, self.slices, self.p, self.y
        for k in self.order:
            self.wires.arrived((self.tag, "z", cut.start, k))

        def body(r):
            mine = lined[self.pick(self.z), r, cut].astype(F32)
            other = jnp.zeros_like(mine)
            for k in range(1, self.lines):
                term = rz[k, r, cut].astype(F32)
                if k % 2:
                    other = other + term
                else:
                    mine = mine + term
            slices[2 * p + y, r, cut] = mine.astype(BF)
            slices[2 * (1 - p) + y, r, cut] = other.astype(BF)

        tiles(lined.shape[1], body)
        for q in range(2):
            block = slices.at[2 * q + y, :, cut]
            self.wires.start((self.tag, "y", cut.start, q), block, block, "group")

    def store(self, cut, target, first, width, stage):
        for q in range(2):
            self.wires.arrived((self.tag, "y", cut.start, q))
        for t in range(4):

            def fill(held):
                def body(r):
                    held[r, pl.ds(0, cut.size)] = self.slices[t, r, cut].astype(F32)

                tiles(target.shape[0], body)

            stage.put(fill, target.at[:, pl.ds(t * width + first, cut.size)], cut.size)


class Stage:
    def __init__(self, held, sems):
        self.held, self.sems, self.made = held, sems, []

    def put(self, fill, target, width):
        n, ring = len(self.made), self.held.shape[0]
        if n >= ring:
            self.made[n - ring].wait()
        held = self.held.at[n % ring]
        fill(held)
        copy = pltpu.make_async_copy(held.at[:, pl.ds(0, width)], target, self.sems.at[n])
        copy.start()
        self.made.append(copy)

    def finish(self):
        for copy in self.made[-self.held.shape[0] :]:
            copy.wait()


def across(wires, grads, rx, cut, lines, tag):
    other = 1 - lax.axis_index("batch") % 2
    for line in range(lines):
        wires.start((tag, "x", cut.start, line), grads.at[2 * line + other, :, cut], rx.at[line, :, cut], "x")


def across_join(wires, grads, rx, lined, cut, lines, tag, pick=lambda line: line):
    x = lax.axis_index("batch") % 2
    for line in range(lines):
        wires.arrived((tag, "x", cut.start, line))

        def body(r):
            total = grads[2 * line + x, r, cut].astype(F32) + rx[line, r, cut].astype(F32)
            lined[pick(line), r, cut] = total.astype(BF)

        tiles(rx.shape[1], body)


def middle_kernel(
    d_attn,
    w_out,
    mixed,
    gates,
    unit,
    rstd,
    values,
    q_rot,
    k_rot,
    weighted,
    decays,
    cosine,
    sine,
    lifted,
    down,
    hidden,
    ffn_lines,
    d_proj,
    output,
    d_up,
    d_down,
    d_out,
    part,
    rc,
    ry,
    rn,
    rz,
    slices,
    grads,
    rx,
    d_ret,
    d_scores,
    rz_out,
    slices_out,
    held,
    *rest,
    lines,
):
    buffers = rest[:7]
    fetch_sems, stage_sems, send, recv = rest[7:]
    wires = Wires(send, recv, lines)
    stage = Stage(held, stage_sems)
    fetched = {}

    def fetch(s):
        for n, (source, buffer) in enumerate(zip((gates, unit, rstd, values, q_rot, k_rot, weighted), buffers)):
            copy = pltpu.make_async_copy(source.at[s], buffer.at[s % 2], fetch_sems.at[7 * s + n])
            copy.start()
            fetched[s, n] = copy

    fetch(0)
    fetch(1)
    wires.enter(("head", "group", "x") + along(lines))
    length = d_attn.shape[1]
    half = length // 2
    wide = w_out.shape[0]
    val = w_out.shape[1]
    units = lifted.shape[2]
    key = q_rot.shape[2]
    step = 256
    ffn = Lines(wires, ffn_lines, rz, slices, lines, "ffn")
    cuts = [pl.ds(c, units) for c in (0, units)]
    xbit = lax.axis_index("batch") % 2

    def pick(line):
        return 2 * line + xbit

    outs = Lines(wires, grads, rz_out, slices_out, lines, "out", pick)
    out_cut = pl.ds(0, val)

    def partial(s):
        def body(i):
            cut = span(i, 512)
            total = dot(lifted[s], down[cut, :], 1, 1)
            part[s, 1, :, cut] = total[half:].astype(BF)
            part[s, 0, :, cut] = total[:half].astype(BF)

        blocks(wide // 512, body)
        send_cores(part, rc, wires, (s,))

    def pointwise(r, total):
        output[r, :] = (hidden[r, :] + total).astype(BF)

    def retention(s):
        for n in range(7):
            fetched[s, n].wait()
        gates_s, unit_s, rstd_s, values_s, q_s, k_s, weighted_s = [buffer.at[s % 2] for buffer in buffers]

        def mix(i):
            r = span(i, half)
            d_mixed = dot(d_attn[s, r, :], w_out[...], 1, 0)
            gate = gates_s[r, :].astype(F32)
            sig = jax.nn.sigmoid(gate)
            norm = unit_s[r, :].astype(F32)
            d_gate = d_mixed * norm * (sig * (1 + gate * (1 - sig)))
            d_proj[s, r, pl.ds(2 * key + val, val)] = d_gate.astype(BF)
            d_norm = d_mixed * (gate * sig)
            mean_d = jnp.mean(d_norm, axis=1, keepdims=True)
            mean_dn = jnp.mean(d_norm * norm, axis=1, keepdims=True)
            d_ret[r, :] = (rstd_s[r, :][:, :1] * (d_norm - mean_d - norm * mean_dn)).astype(BF)

        blocks(2, mix)
        d_proj[s, :, pl.ds(2 * key, val)] = dot(weighted_s[...], d_ret[...], 0, 0).astype(BF)
        d_scores[...] = (dot(d_ret[...], values_s[...], 1, 1) * decays[...]).astype(BF)

        def turn(grad, first):
            a, b = grad[:, : key // 2], grad[:, key // 2 :]
            d_proj[s, :, pl.ds(first, key // 2)] = (a * cosine[...] + b * sine[...]).astype(BF)
            d_proj[s, :, pl.ds(first + key // 2, key // 2)] = (b * cosine[...] - a * sine[...]).astype(BF)

        turn(dot(d_scores[...], k_s[...], 1, 0), 0)
        turn(dot(d_scores[...], q_s[...], 0, 0), key)
        if s < 2:
            fetch(s + 2)

    def out_grads():
        flat = grads.reshape(wide, val)

        def body(i):
            total = jnp.zeros((step, val), F32)
            for s in range(4):
                total = total + dot(d_attn[s, :, span(i, step)], mixed[s], 0, 0)
            flat[span(i, step), :] = total.astype(BF)

        blocks(wide // step, body)
        across(wires, grads, rx, pl.ds(0, val), lines, "out")

    steps = reduce_rows(part, rc, ry, rn, wires, pointwise)
    ffn.send(cuts[0])
    ffn.send(cuts[1])
    partial(3)
    partial(2)
    next(steps)
    partial(1)
    next(steps)
    partial(0)
    next(steps)
    out_grads()
    retention(0)
    retention(1)
    next(steps)
    retention(2)
    across_join(wires, grads, rx, grads, out_cut, lines, "out", pick)
    outs.send(out_cut)
    retention(3)
    ffn.join(cuts[0])
    ffn.join(cuts[1])
    for _ in steps:
        pass
    ffn.store(cuts[0], d_up, 0, units, stage)
    ffn.store(cuts[1], d_down, 0, units, stage)
    outs.join(out_cut)
    outs.store(out_cut, d_out, 0, val, stage)
    stage.finish()
    wires.finish()


def last_kernel(
    d_proj,
    x,
    d_hidden,
    gain,
    ln_gains,
    normed_hbm,
    stacked_hbm,
    d_inputs,
    gains,
    d_query,
    d_key,
    d_value,
    d_gate,
    normed,
    stacked,
    grads,
    part,
    rc,
    ry,
    rn,
    rx,
    rz,
    slices,
    held,
    came,
    staged,
    local,
    stage_sems,
    send,
    recv,
    *,
    lines,
):
    wires, moves = Wires(send, recv, lines), Moves(local)
    wide, columns = stacked.shape
    tokens = normed.shape[0]
    step = 256
    val = d_value.shape[1] // 4
    key = d_query.shape[1] // 4
    for i in range(wide // step):
        cut = pl.ds(i * step, step)
        moves.start(normed_hbm.at[:, cut], normed.at[:, cut])
    moves.start(stacked_hbm, stacked)
    wires.enter(("head", "group", "x") + along(lines))
    xbit = lax.axis_index("batch") % 2
    stage = Stage(staged, stage_sems)

    def pick(line):
        return 2 * line + xbit

    main = Lines(wires, grads, rz, slices, lines, "main", pick)
    cuts = [pl.ds(c, 256) for c in (2 * key + val, 2 * key + val + 256, 2 * key, 2 * key + 256, 0, key)]
    flat = grads.reshape(wide, columns)
    held[0] = jnp.zeros_like(held[0])
    rows_all = d_proj.reshape(tokens, columns)

    def pointwise(r, total):
        row = x[r, :].astype(F32)
        scale = lax.rsqrt(jnp.mean(row * row, axis=1, keepdims=True) + 1e-06)
        unit = row * scale
        terms = total * unit
        held[0, :8] += terms[:8] + terms[8:]
        d_unit = total * gain[...]
        mean_du = jnp.mean(d_unit * unit, axis=1, keepdims=True)
        d_inputs[r, :] = (d_hidden[r, :] + scale * (d_unit - unit * mean_du)).astype(BF)

    def weight_grads(first, wait=False):
        cut = pl.ds(first, 512)

        def body(i):
            flat[span(i, step), cut] = dot(normed[:, span(i, step)], rows_all[:, cut], 0, 0).astype(BF)

        if wait:
            for i in range(wide // step):
                moves.made[i].wait()
                body(i)
        else:
            blocks(wide // step, body)
        for c in (first, first + 256):
            across(wires, grads, rx, pl.ds(c, 256), lines, "main")

    def partial(s):
        rows = d_proj.shape[1] // 2

        def body(i):
            cut = span(i, 512)
            total = dot(d_proj[s], stacked[cut, :], 1, 1)
            part[s, 1, :, cut] = total[rows:].astype(BF)
            part[s, 0, :, cut] = total[:rows].astype(BF)

        blocks(wide // 512, body)
        send_cores(part, rc, wires, (s,))

    def stage_x(at):
        across_join(wires, grads, rx, grads, cuts[at], lines, "main", pick)
        main.send(cuts[at])

    def reduce_gains():
        held[0, 8:] = ln_gains[...]
        steps = ["head", "group", "x"]
        bit = 1
        while bit < lines:
            steps.append(("line", bit))
            bit *= 2
        for at, peer in enumerate(steps):
            wires.start(("gain", at), held.at[at], came.at[at], peer)
            wires.arrived(("gain", at))
            held[at + 1] = held[at] + came[at]
        gains[...] = held[len(steps)]

    targets = [(d_gate, val, 0), (d_gate, val, 256), (d_value, val, 0), (d_value, val, 256), (d_query, key, 0), (d_key, key, 0)]

    def store(at):
        target, width, first = targets[at]
        main.store(cuts[at], target, first, width, stage)

    steps = reduce_rows(part, rc, ry, rn, wires, pointwise)
    weight_grads(2 * key + val, True)
    moves.made[-1].wait()
    partial(3)
    partial(2)
    next(steps)
    weight_grads(2 * key)
    next(steps)
    stage_x(0)
    partial(1)
    weight_grads(0)
    next(steps)
    stage_x(1)
    partial(0)
    next(steps)
    stage_x(2)
    main.join(cuts[0])
    stage_x(3)
    main.join(cuts[1])
    stage_x(4)
    for _ in steps:
        pass
    main.join(cuts[2])
    reduce_gains()
    stage_x(5)
    store(0)
    store(1)
    main.join(cuts[3])
    store(2)
    main.join(cuts[4])
    store(3)
    main.join(cuts[5])
    store(4)
    store(5)
    stage.finish()
    wires.finish()


def exchange_scratch(rows, width):
    half = rows // 2
    return [
        pltpu.VMEM((4, rows, width), BF),
        pltpu.VMEM((4, rows, width), BF),
        pltpu.VMEM((2, half, width), BF),
        pltpu.VMEM((2, half, width), BF),
        pltpu.VMEM((half, width), BF),
        pltpu.VMEM((half, width), BF),
        pltpu.VMEM((half, width), BF),
        pltpu.VMEM((half, width), BF),
    ]


def lean_scratch(rows, width):
    return [
        pltpu.VMEM((4, 2, rows, width), BF),
        pltpu.VMEM((4, rows, width), BF),
        pltpu.VMEM((2, rows, width), BF),
        pltpu.VMEM((rows, width), BF),
    ]


def semaphores(count):
    return [pltpu.SemaphoreType.DMA((count,)), pltpu.SemaphoreType.DMA((count,))]


def anywhere():
    return pl.BlockSpec(memory_space=pl.ANY)


def vmem():
    return pl.BlockSpec(memory_space=pltpu.VMEM)


def forward_exchange(part, x, gain, own, other, batch):
    rows, width = x.shape
    lines = batch // 2
    result = pl.pallas_call(
        functools.partial(forward_kernel, lines=lines),
        out_shape=(
            jax.ShapeDtypeStruct((4, 2, rows, width), BF),
            jax.ShapeDtypeStruct((rows, width), F32),
        )
        + tuple(jax.ShapeDtypeStruct((batch,) + v.shape, BF) for v in own),
        in_specs=[vmem()] * 7,
        out_specs=(vmem(), vmem(), anywhere(), anywhere()),
        scratch_shapes=exchange_scratch(rows, width) + semaphores(24 + 4 * lines) + [pltpu.SemaphoreType.DMA((2,))],
        compiler_params=pltpu.CompilerParams(collective_id=0, has_side_effects=True, vmem_limit_bytes=46 * 2**20),
        cost_estimate=pl.CostEstimate(flops=10 * rows * width, bytes_accessed=300000000, transcendentals=0),
        name="forward_exchange",
    )(part.reshape(4, 2, rows, width), x, gain[None], *own, *other)
    return result[0].reshape(8 * rows, width), result[1], [w.reshape(width, -1) for w in result[2:]]


def backward_exchange(part, hidden, cotangent, factor, gain, grads, batch):
    rows, width = hidden.shape
    lines = batch // 2
    block = (width // batch, grads.shape[1])
    whole, d_hidden, d_gain, lined = pl.pallas_call(
        functools.partial(backward_kernel, lines=lines),
        out_shape=(
            jax.ShapeDtypeStruct((4, 2, rows, width), BF),
            jax.ShapeDtypeStruct((rows, width), F32),
            jax.ShapeDtypeStruct((8, width), F32),
            jax.ShapeDtypeStruct((lines,) + block, BF),
        ),
        in_specs=[vmem()] * 3 + [pl.BlockSpec(memory_space=pltpu.SMEM), vmem(), vmem()],
        out_specs=(vmem(), vmem(), vmem(), vmem()),
        scratch_shapes=exchange_scratch(rows, width)
        + [pltpu.VMEM((lines,) + block, BF)]
        + semaphores(24 + lines),
        compiler_params=pltpu.CompilerParams(collective_id=1, has_side_effects=True, vmem_limit_bytes=50 * 2**20),
        cost_estimate=pl.CostEstimate(flops=10 * rows * width, bytes_accessed=300000000, transcendentals=0),
        name="backward_exchange",
    )(
        part.reshape(4, 2, rows, width),
        hidden,
        cotangent,
        factor.reshape(1, 1),
        gain[None],
        grads.reshape((batch,) + block),
    )
    return whole.reshape(8 * rows, width), d_hidden, d_gain, lined


def middle_exchange(d_attn, w_out, mixed, saved, tables, lifted, down, hidden, ffn_lines, batch):
    rows, width = hidden.shape
    lines = batch // 2
    length = 2 * rows
    block = ffn_lines.shape[1:]
    val = w_out.shape[1]
    units = lifted.shape[1]
    gates, unit, rstd, values, q_rot, k_rot, weighted = saved
    columns = 2 * q_rot.shape[2] + 2 * val
    return pl.pallas_call(
        functools.partial(middle_kernel, lines=lines),
        out_shape=(
            jax.ShapeDtypeStruct((4, length, columns), BF),
            jax.ShapeDtypeStruct((rows, width), BF),
            jax.ShapeDtypeStruct((block[0], 4 * units), F32),
            jax.ShapeDtypeStruct((block[0], 4 * units), F32),
            jax.ShapeDtypeStruct((block[0], 4 * val), F32),
        ),
        in_specs=[vmem()] * 3 + [anywhere()] * 7 + [vmem()] * 7,
        out_specs=(vmem(), vmem(), anywhere(), anywhere(), anywhere()),
        scratch_shapes=lean_scratch(rows, width)
        + [
            pltpu.VMEM((lines,) + block, BF),
            pltpu.VMEM((4,) + block, BF),
            pltpu.VMEM((batch, block[0], val), BF),
            pltpu.VMEM((lines, block[0], val), BF),
            pltpu.VMEM((length, val), BF),
            pltpu.VMEM((length, length), BF),
            pltpu.VMEM((lines, block[0], val), BF),
            pltpu.VMEM((4, block[0], val), BF),
            pltpu.VMEM((2, block[0], units), F32),
        ]
        + [pltpu.VMEM((2,) + v.shape[1:], v.dtype) for v in saved]
        + [pltpu.SemaphoreType.DMA((28,)), pltpu.SemaphoreType.DMA((12,))]
        + semaphores(16 + 3 * (lines + 1) + lines),
        compiler_params=pltpu.CompilerParams(collective_id=4, has_side_effects=True, vmem_limit_bytes=63 * 2**20),
        cost_estimate=pl.CostEstimate(flops=20 * 10**9, bytes_accessed=200000000, transcendentals=0),
        name="middle_exchange",
    )(
        d_attn.reshape(4, length, width),
        w_out,
        mixed.reshape(4, length, val),
        gates,
        unit,
        rstd,
        values,
        q_rot,
        k_rot,
        weighted,
        *tables,
        lifted.reshape(4, length, units),
        down,
        hidden,
        ffn_lines,
    )


def last_exchange(d_proj, x, d_hidden, gain, ln_gains, normed, stacked, key, batch):
    rows, width = x.shape
    lines = batch // 2
    high = width // batch
    columns = stacked.shape[1]
    val = (columns - 2 * key) // 2
    steps = 2 + batch.bit_length() - 1
    return pl.pallas_call(
        functools.partial(last_kernel, lines=lines),
        out_shape=(
            jax.ShapeDtypeStruct((rows, width), BF),
            jax.ShapeDtypeStruct((16, width), F32),
            jax.ShapeDtypeStruct((high, 4 * key), F32),
            jax.ShapeDtypeStruct((high, 4 * key), F32),
            jax.ShapeDtypeStruct((high, 4 * val), F32),
            jax.ShapeDtypeStruct((high, 4 * val), F32),
        ),
        in_specs=[vmem()] * 5 + [anywhere()] * 2,
        out_specs=(vmem(), vmem()) + tuple([anywhere()] * 4),
        scratch_shapes=[
            pltpu.VMEM(normed.shape, BF),
            pltpu.VMEM(stacked.shape, BF),
            pltpu.VMEM((batch, high, columns), BF),
        ]
        + lean_scratch(rows, width)
        + [
            pltpu.VMEM((lines, high, columns), BF),
            pltpu.VMEM((lines, high, columns), BF),
            pltpu.VMEM((4, high, columns), BF),
            pltpu.VMEM((steps + 1, 16, width), F32),
            pltpu.VMEM((steps, 16, width), F32),
            pltpu.VMEM((2, high, val), F32),
            pltpu.SemaphoreType.DMA((width // 256 + 1,)),
            pltpu.SemaphoreType.DMA((4 * (columns // 256),)),
        ]
        + semaphores(16 + steps + (columns // 256) * (2 * lines + 1)),
        compiler_params=pltpu.CompilerParams(collective_id=3, has_side_effects=True, vmem_limit_bytes=63 * 2**20),
        cost_estimate=pl.CostEstimate(flops=26 * 10**9, bytes_accessed=300000000, transcendentals=0),
        name="last_exchange",
    )(d_proj, x, d_hidden, gain[None], ln_gains, normed, stacked)


class Place:
    def __init__(self):
        self.batch = lax.axis_size("batch")
        self.b = lax.axis_index("batch")
        self.y = lax.axis_index("group")
        self.c = lax.axis_index("head")
        self.lines = self.batch // 2
        self.z = self.b // 2
        self.x = self.b % 2
        self.p = self.z % 2
        self.slot = 2 * self.p + self.y

    def cut(self, array, axis):
        width = array.shape[axis] // 4
        own = lax.dynamic_slice_in_dim(array, self.slot * width, width, axis)
        other = lax.dynamic_slice_in_dim(array, (self.slot ^ 2) * width, width, axis)
        return own, other

def on_device(
    inputs,
    rms_gain,
    w_query,
    w_key,
    w_value,
    w_gate,
    w_out,
    ln_gain,
    w_up,
    w_down,
    cotangent,
    domain_of,
    domain_weight,
):
    here = Place()
    half = inputs.shape[1]
    length = 2 * half

    parts = [here.cut(w, 1) for w in (w_query, w_key, w_value, w_gate)]
    own = jnp.concatenate([own for own, _ in parts], axis=1)
    other = jnp.concatenate([other for _, other in parts], axis=1)
    out_own, out_other = [v.T for v in here.cut(w_out, 0)]
    factor = sequence_factor(domain_of, domain_weight)
    own_index = here.b * lax.axis_size("group") + here.y
    own_factor = lax.dynamic_index_in_dim(factor, own_index, 0, keepdims=False)
    stacked, out_t, normed_all, d_ffn_all, mixed, saved = gather_first(
        (own, out_own), (other, out_other), inputs[0], rms_gain, cotangent[0], own_factor, KEY, here.batch
    )
    up_parts = here.cut(w_up, 1)
    down_parts = [v.T for v in here.cut(w_down, 0)]
    mixed_low = mixed.reshape(-1, VAL)
    ln_all, hidden, (up, down_t) = forward_exchange(
        mm(mixed_low, out_t, 1, 1, BF),
        inputs[0],
        ln_gain,
        (up_parts[0], down_parts[0]),
        (up_parts[1], down_parts[1]),
        here.batch,
    )
    pre_act = mm(ln_all, up, 1, 0)
    lifted, gelu_back = jax.vjp(gelu_tanh, pre_act)
    lifted_low = lifted.astype(BF)

    d_lifted = mm(d_ffn_all, down_t, 1, 0)
    (d_pre,) = gelu_back(d_lifted)
    d_pre_low = d_pre.astype(BF)
    ffn_grads = jnp.concatenate([mm(ln_all, d_pre_low, 0, 0, BF), mm(d_ffn_all, lifted_low, 0, 0, BF)], axis=1)
    d_attn_all, d_hidden, d_ln_gain, ffn_lines = backward_exchange(
        mm(d_pre_low, up, 1, 1, BF), hidden, cotangent[0], own_factor, ln_gain, ffn_grads, here.batch
    )
    places = (jnp.arange(length, dtype=jnp.int32) + here.c * half) % length
    cosine, sine = rotary_tables(places, KEY)
    decays = decay_mask(places, here.c * 4 + here.slot)
    quarter = KEY // 2
    d_proj, output, d_up, d_down, d_w_out = middle_exchange(
        d_attn_all,
        out_t,
        mixed_low,
        saved,
        (decays, cosine[:, :quarter], sine[:, :quarter]),
        lifted_low,
        down_t,
        hidden,
        ffn_lines,
        here.batch,
    )
    d_inputs, gains, d_query, d_key, d_value, d_gate = last_exchange(
        d_proj, inputs[0], d_hidden, rms_gain, d_ln_gain, normed_all, stacked, KEY, here.batch
    )
    gain_rms = jnp.sum(gains[:8], axis=0)
    gain_ln = jnp.sum(gains[8:], axis=0)
    return (
        output[None],
        d_inputs[None],
        gain_rms,
        d_query,
        d_key,
        d_value,
        d_gate,
        d_w_out.T,
        gain_ln,
        d_up,
        d_down.T,
    )


def solution(mesh):
    rows = P(("batch", "group"), "head", None)
    wide = P("batch", "head")
    tall = P("head", "batch")
    return jax.shard_map(
        on_device,
        mesh=mesh,
        in_specs=(rows, P(), wide, wide, wide, wide, tall, P(), wide, tall, rows, P(), P()),
        out_specs=(rows, rows, P(), wide, wide, wide, wide, tall, P(), wide, tall),
        check_vma=False,
    )
```

```python
import functools

import jax
import jax.numpy as jnp
import numpy as np
from jax import lax
from jax.experimental import pallas as pl
from jax.experimental.pallas import tpu as pltpu
from jax.sharding import PartitionSpec as P


KEY = 256
VAL = 512
GELU = 0.7978845608028654
BF = jnp.bfloat16
F32 = jnp.float32


def sequence_factor(domain_of, domain_weight):
    same = (domain_of[:, None] == domain_of[None, :]).astype(F32)
    counts = jnp.sum(same, axis=1)
    domain_ids = jnp.arange(domain_weight.shape[0], dtype=jnp.int32)
    onehot = (domain_of[:, None] == domain_ids[None, :]).astype(F32)
    weight_seq = jnp.sum(onehot * domain_weight.astype(F32)[None, :], axis=1)
    total = jnp.sum(weight_seq / counts)
    return jnp.float32(domain_of.shape[0]) * weight_seq / (counts * total)


TEAM = ("head", "batch", "group")


def peers(lines):
    b = lax.axis_index("batch")
    table = {
        "head": {"head": 1 - lax.axis_index("head")},
        "batch": {"batch": b ^ 2},
        "group": {"group": 1 - lax.axis_index("group")},
        "x": {"batch": b ^ 1},
    }
    for k in range(1, lines):
        table["line", k] = {"batch": b ^ (2 * k)}
    return table


def along(lines):
    return tuple(("line", k) for k in range(1, lines))


class Wires:
    def __init__(self, send, recv, lines=1):
        self.send, self.recv, self.made, self.peers = send, recv, {}, peers(lines)

    def enter(self, names):
        barrier = pltpu.get_barrier_semaphore()
        for name in names:
            pl.semaphore_signal(barrier, inc=1, device_id=self.peers[name], device_id_type=pl.DeviceIdType.MESH)
        pl.semaphore_wait(barrier, len(names))

    def start(self, name, source, target, peer, go=True):
        n = len(self.made)
        copy = pltpu.make_async_remote_copy(
            src_ref=source,
            dst_ref=target,
            send_sem=self.send.at[n],
            recv_sem=self.recv.at[n],
            device_id=self.peers[peer],
            device_id_type=pl.DeviceIdType.MESH,
        )
        if go:
            copy.start()
        self.made[name] = copy

    def plan(self, *copy):
        self.start(*copy, go=False)

    def go(self, names):
        for name in names:
            self.made[name].start()

    def arrived(self, *names):
        for name in names:
            self.made[name].wait_recv()

    def finish(self):
        for copy in self.made.values():
            copy.wait_send()


class Moves:
    def __init__(self, sems):
        self.sems, self.made = sems, []

    def start(self, source, target):
        copy = pltpu.make_async_copy(source, target, self.sems.at[len(self.made)])
        copy.start()
        self.made.append(copy)

    def finish(self):
        for copy in self.made:
            copy.wait()


TILE = 16


def tiles(rows, body):
    def step(i, _):
        body(pl.ds(pl.multiple_of(i * TILE, TILE), TILE))
        return 0

    lax.fori_loop(0, rows // TILE, step, 0)


def exchange(part, whole, rc, sums, ra, rb, ea, eb, sa, sb, wires, pointwise, tag=""):
    rows = part.shape[2]
    half = rows // 2
    top, low = pl.ds(0, half), pl.ds(half, half)

    def start(name, *rest):
        wires.start(tag + name, *rest)

    def arrived(*names):
        wires.arrived(*[tag + name for name in names])

    def add(s, first):
        def body(r):
            rr = pl.ds(r.start + first, TILE)
            total = part[s, 0, rr, :].astype(F32) + rc[s, rr, :].astype(F32)
            sums[s, rr, :] = total.astype(BF)

        tiles(half, body)

    arrived("c3")
    add(3, 0)
    start("a3", sums.at[3, top], ra.at[0], "batch")
    add(3, half)
    start("b3", sums.at[3, low], rb.at[0], "group")
    arrived("c1")
    add(1, 0)
    start("a1", sums.at[1, top], ra.at[1], "batch")
    arrived("c2")
    add(2, half)
    start("b2", sums.at[2, low], rb.at[1], "group")
    add(2, 0)
    add(1, half)

    def second_a(r):
        sa[r, :] = (sums[2, r, :].astype(F32) + ra[0, r, :].astype(F32)).astype(BF)

    def second_b(r):
        rr = pl.ds(r.start + half, TILE)
        sb[r, :] = (sums[1, rr, :].astype(F32) + rb[0, r, :].astype(F32)).astype(BF)

    yield
    arrived("a3")
    tiles(half, second_a)
    start("a2", sa, ea, "group")
    arrived("b3")
    tiles(half, second_b)
    start("b1", sb, eb, "batch")

    def last(first, near, end):
        def body(r):
            rr = pl.ds(r.start + first, TILE)
            total = part[0, 0, rr, :].astype(F32) + rc[0, rr, :].astype(F32)
            total = total + near[1, r, :].astype(F32) + end[r, :].astype(F32)
            pointwise(rr, total)

        tiles(half, body)

    yield
    arrived("c0", "a1", "a2")
    last(0, ra, ea)
    if whole is not None:
        start("za", whole.at[0, 0, top], whole.at[1, 0, top], "batch")
    yield
    arrived("b2", "b1")
    last(half, rb, eb)
    if whole is None:
        return
    start("yb", whole.at[0, 0, low], whole.at[2, 0, low], "group")
    start("zb", whole.at[0, 0, low], whole.at[1, 0, low], "batch")
    start("ya", whole.at[0, 0, top], whole.at[2, 0, top], "group")
    start("own", whole.at[0, 0], whole.at[0, 1], "head")
    yield
    arrived("za")
    start("fa", whole.at[1, 0, top], whole.at[3, 0, top], "group")
    start("cza", whole.at[1, 0, top], whole.at[1, 1, top], "head")
    arrived("yb")
    start("fb", whole.at[2, 0, low], whole.at[3, 0, low], "batch")
    start("cyb", whole.at[2, 0, low], whole.at[2, 1, low], "head")
    yield
    arrived("zb")
    start("czb", whole.at[1, 0, low], whole.at[1, 1, low], "head")
    arrived("ya")
    start("cya", whole.at[2, 0, top], whole.at[2, 1, top], "head")
    yield


def reduce_rows(part, rc, ry, rn, wires, pointwise, tag=""):
    rows = part.shape[2]
    half = rows // 2
    ends = [pl.ds(0, half), pl.ds(half, half)]

    def add(s, end):
        def body(r):
            rr = pl.ds(r.start + end.start, TILE)
            total = part[s, 0, rr, :].astype(F32) + rc[s, rr, :].astype(F32)
            part[s, 0, rr, :] = total.astype(BF)

        tiles(half, body)

    for s, at in ((3, 0), (2, 1)):
        wires.arrived(f"{tag}c{s}")
        for h, end in enumerate(ends):
            add(s, end)
            wires.start((tag, s, h), part.at[s, 0, end], ry.at[at, end], "group")
        yield
    wires.arrived(f"{tag}c1")
    for end in ends:
        add(1, end)
    yield
    for h, end in enumerate(ends):
        wires.arrived((tag, 3, h))

        def body(r):
            rr = pl.ds(r.start + end.start, TILE)
            total = part[1, 0, rr, :].astype(F32) + ry[0, rr, :].astype(F32)
            part[1, 0, rr, :] = total.astype(BF)

        tiles(half, body)
        wires.start((tag, 1, h), part.at[1, 0, end], rn.at[end], "batch")
    yield
    wires.arrived(f"{tag}c0")
    for h, end in enumerate(ends):
        wires.arrived((tag, 2, h), (tag, 1, h))

        def last(r):
            rr = pl.ds(r.start + end.start, TILE)
            total = part[0, 0, rr, :].astype(F32) + rc[0, rr, :].astype(F32)
            pointwise(rr, total + ry[1, rr, :].astype(F32) + rn[rr, :].astype(F32))

        tiles(half, last)


def send_cores(part, rc, wires, slots=(3, 1, 2, 0), tag=""):
    for s in slots:
        wires.start(tag + f"c{s}", part.at[s, 1], rc.at[s], "head")


def dot(left, right, left_dim, right_dim):
    return lax.dot_general(left, right, (((left_dim,), (right_dim,)), ((), ())), preferred_element_type=F32)


def blocks(count, body):
    def step(i, _):
        body(i)
        return 0

    lax.fori_loop(0, count, step, 0)


def span(i, size):
    return pl.ds(pl.multiple_of(i * size, size), size)


def gather_kernel(
    own,
    own_out,
    other,
    other_out,
    x,
    gain,
    cotangent,
    factor,
    stacked_hbm,
    out_t,
    normed_hbm,
    d_ffn,
    mixed,
    *rest,
    lines,
):
    saved_hbm, tables_hbm, rest = rest[:7], rest[7:10], rest[10:]
    stacked, whole, normed, d_rows, cosine, sine, decays, unit_full = rest[:8]
    saved, (send, recv, local) = rest[8:15], rest[15:]
    gates, unit, rstd, values, q_rot, k_rot, weighted = saved
    b, c = lax.axis_index("batch"), lax.axis_index("head")
    slot = 2 * ((b // 2) % 2) + lax.axis_index("group")
    wires, moves = Wires(send, recv, lines), Moves(local)
    wires.enter(("head", "group", "x") + along(lines))
    order = first_order(lines)
    half, wide = x.shape
    length = 2 * half
    key, val = q_rot.shape[2], values.shape[2]
    cuts = [(0, pl.ds(0, 512)), (0, pl.ds(512, 512)), (0, pl.ds(1024, 256)), (0, pl.ds(1280, 256))]
    cuts += [(1, pl.ds(0, 256)), (1, pl.ds(256, 256))]
    mine, others, weights = (own, own_out), (other, other_out), (stacked, out_t)

    def piece(i, cut):
        for k in order:
            source = others[i] if k % 2 else mine[i]
            wires.plan((i, cut.start, k), source.at[:, cut], weights[i].at[b, :, cut], ("line", k))
        wires.start((i, cut.start, "x", 0), mine[i].at[:, cut], weights[i].at[b, :, cut], "x")

    def relay(i, cut):
        for k in order:
            wires.arrived((i, cut.start, k))
            block = weights[i].at[b ^ (2 * k), :, cut]
            wires.start((i, cut.start, "x", k), block, block, "x")

    def ready(i, cut):
        wires.arrived(*[(i, cut.start, "x", k) for k in range(lines)])

    def body(r):
        row = x[r, :].astype(F32)
        scale = lax.rsqrt(jnp.mean(row * row, axis=1, keepdims=True) + 1e-06)
        normed[r, :] = (row * scale * gain[...]).astype(BF)
        d_rows[r, :] = (cotangent[r, :].astype(F32) * factor[0, 0]).astype(BF)

    tiles(half, body)
    wires.start("y", normed, whole.at[2, 0], "group")
    wires.start("own", normed, whole.at[0, 1], "head")
    wires.plan("z", normed, whole.at[1, 0], ("line", 1))
    wires.plan("dz", d_rows, d_ffn.at[1, 0], ("line", 1))
    for cut in cuts:
        piece(*cut)
    near_first = sorted(order)

    def names(cuts_now, ks):
        return [(i, cut.start, k) for i, cut in cuts_now for k in ks]

    @pl.when(c == 0)
    def _():
        wires.go(["z", "dz"] + names(cuts, near_first))

    @pl.when(c == 1)
    def _():
        wires.go(names(cuts[:2], order) + ["z", "dz"] + names(cuts[2:], order))

    moves.start(normed, whole.at[0, 0])
    for i in range(2):
        moves.start(mine[i], weights[i].at[b])
    wires.start("dy", d_rows, d_ffn.at[2, 0], "group")
    wires.start("down", d_rows, d_ffn.at[0, 1], "head")
    moves.start(d_rows, d_ffn.at[0, 0])

    lane = lax.broadcasted_iota(jnp.int32, (half, key // 2), 1).astype(F32)
    freqs = jnp.exp(lane * jnp.float32(-np.log(10000.0) / (key // 2 - 1)))
    for h in range(2):
        first = (h * half + c * half) % length
        places = (lax.broadcasted_iota(jnp.int32, (half, key // 2), 0) + first).astype(F32)
        cosine[pl.ds(h * half, half), :] = jnp.cos(places * freqs)
        sine[pl.ds(h * half, half), :] = jnp.sin(places * freqs)
    head = 4 * c + slot
    log_keep = jnp.float32(0)
    for h in range(8):
        log_keep = jnp.where(head == h, jnp.float32(np.log1p(-(2.0 ** (-5 - h)))), log_keep)

    def decay_rows(r):
        n = lax.broadcasted_iota(jnp.int32, (TILE, length), 0) + r.start
        m = lax.broadcasted_iota(jnp.int32, (TILE, length), 1)
        offset = (n + c * half) % length - (m + c * half) % length
        steps = jnp.maximum(offset, 0).astype(F32)
        decays[r, :] = jnp.where(offset >= 0, jnp.exp(steps * log_keep), jnp.float32(0))

    tiles(length, decay_rows)

    rows = whole.reshape(4, length, wide)
    flat = stacked.reshape(wide, stacked.shape[2])

    def turn(s):
        total = dot(rows[s], flat[:, pl.ds(0, 2 * key)], 1, 0)
        for target, at in ((q_rot, 0), (k_rot, key)):
            a, b_ = total[:, at : at + key // 2], total[:, at + key // 2 : at + key]
            target[s, :, pl.ds(0, key // 2)] = (a * cosine[...] - b_ * sine[...]).astype(BF)
            target[s, :, pl.ds(key // 2, key // 2)] = (b_ * cosine[...] + a * sine[...]).astype(BF)

    def retain(s):
        values[s] = dot(rows[s], flat[:, pl.ds(2 * key, val)], 1, 0).astype(BF)
        weighted[s] = (dot(q_rot[s], k_rot[s], 1, 1) * decays[...]).astype(BF)

        def part(i):
            r = span(i, half)
            retained = dot(weighted[s, r, :], values[s], 1, 0)
            centered = retained - jnp.mean(retained, axis=1, keepdims=True)
            scale = lax.rsqrt(jnp.mean(centered * centered, axis=1, keepdims=True) + 1e-05)
            full = centered * scale
            unit_full[s, r, :] = full
            unit[s, r, :] = full.astype(BF)
            rstd[s, r, :] = jnp.broadcast_to(scale, (half, rstd.shape[2]))

        blocks(2, part)

    def mix(s):
        def part(i):
            r = span(i, half)
            gate = dot(rows[s, r, :], flat[:, pl.ds(2 * key + val, val)], 1, 0)
            gates[s, r, :] = gate.astype(BF)
            mixed[s, r, :] = (unit_full[s, r, :] * (gate * jax.nn.sigmoid(gate))).astype(BF)

        blocks(2, part)

    wires.arrived("z")
    wires.start("far", whole.at[1, 0], whole.at[3, 0], "group")
    wires.start("cz", whole.at[1, 0], whole.at[1, 1], "head")
    wires.arrived("y")
    wires.start("cy", whole.at[2, 0], whole.at[2, 1], "head")
    relay(*cuts[0])
    wires.arrived("far")
    wires.start("cfar", whole.at[3, 0], whole.at[3, 1], "head")
    relay(*cuts[1])
    moves.finish()
    wires.arrived("own", "cz", "cy", "cfar")
    ready(*cuts[0])
    keep = Moves(local.at[pl.ds(8, 13)])
    keep.start(whole, normed_hbm)
    keep.start(decays, tables_hbm[0])
    keep.start(cosine, tables_hbm[1])
    keep.start(sine, tables_hbm[2])
    turn(0)
    turn(1)
    relay(*cuts[2])
    turn(2)
    turn(3)
    ready(*cuts[1])
    retain(0)
    relay(*cuts[3])
    retain(1)
    wires.arrived("dy")
    wires.start("dcy", d_ffn.at[2, 0], d_ffn.at[2, 1], "head")
    retain(2)
    relay(*cuts[4])
    retain(3)
    wires.arrived("dz")
    wires.start("dfar", d_ffn.at[1, 0], d_ffn.at[3, 0], "group")
    wires.start("dcz", d_ffn.at[1, 0], d_ffn.at[1, 1], "head")
    ready(*cuts[2])
    ready(*cuts[3])
    keep.start(stacked, stacked_hbm)
    for n in range(1, 7):
        keep.start(saved[n], saved_hbm[n])
    mix(0)
    mix(1)
    relay(*cuts[5])
    mix(2)
    mix(3)
    keep.start(gates, saved_hbm[0])
    wires.arrived("dfar")
    wires.start("dcfar", d_ffn.at[3, 0], d_ffn.at[3, 1], "head")
    ready(*cuts[4])
    ready(*cuts[5])
    wires.arrived("down", "dcz", "dcy", "dcfar")
    keep.finish()
    wires.finish()


def gather_first(own, other, x, gain, cotangent, factor, key, batch):
    rows, width = x.shape
    lines = batch // 2
    length = 2 * rows
    val = own[1].shape[1]
    high, columns = own[0].shape
    saved = [
        jax.ShapeDtypeStruct((4, length, w), t)
        for w, t in ((val, BF), (val, BF), (128, F32), (val, BF), (key, BF), (key, BF), (length, BF))
    ]
    result = pl.pallas_call(
        functools.partial(gather_kernel, lines=lines),
        out_shape=(
            jax.ShapeDtypeStruct((batch, high, columns), BF),
            jax.ShapeDtypeStruct((batch, high, val), BF),
            jax.ShapeDtypeStruct((4, 2, rows, width), BF),
            jax.ShapeDtypeStruct((4, 2, rows, width), BF),
            jax.ShapeDtypeStruct((4, length, val), BF),
            *saved,
            jax.ShapeDtypeStruct((length, length), F32),
            jax.ShapeDtypeStruct((length, key // 2), F32),
            jax.ShapeDtypeStruct((length, key // 2), F32),
        ),
        in_specs=[vmem()] * 7 + [pl.BlockSpec(memory_space=pltpu.SMEM)],
        out_specs=(anywhere(), vmem(), anywhere(), anywhere(), vmem()) + tuple([anywhere()] * 10),
        scratch_shapes=[
            pltpu.VMEM((batch, high, columns), BF),
            pltpu.VMEM((4, 2, rows, width), BF),
            pltpu.VMEM((rows, width), BF),
            pltpu.VMEM((rows, width), BF),
            pltpu.VMEM((length, key // 2), F32),
            pltpu.VMEM((length, key // 2), F32),
            pltpu.VMEM((length, length), F32),
            pltpu.VMEM((4, length, val), F32),
        ]
        + [pltpu.VMEM(v.shape, v.dtype) for v in saved]
        + semaphores(6 * 2 * lines + 16)
        + [pltpu.SemaphoreType.DMA((21,))],
        compiler_params=pltpu.CompilerParams(collective_id=2, has_side_effects=True, vmem_limit_bytes=56 * 2**20),
        cost_estimate=pl.CostEstimate(flops=20 * 10**9, bytes_accessed=300000000, transcendentals=0),
        name="gather_first",
    )(*own, *other, x, gain[None], cotangent, factor.reshape(1, 1))
    stacked, out_t, normed, d_ffn, mixed = result[:5]
    return (
        stacked.reshape(-1, columns),
        out_t.reshape(-1, val),
        normed.reshape(8 * rows, width),
        d_ffn.reshape(8 * rows, width),
        mixed,
        result[5:12],
        result[12:],
    )


def partial_rows(part, rc, wires, rows, weights, s):
    half = part.shape[2]

    def body(i):
        cut = span(i, 512)
        total = dot(rows[...], weights[cut, :], 1, 1)
        part[s, 1, :, cut] = total[half:].astype(BF)
        part[s, 0, :, cut] = total[:half].astype(BF)

    blocks(weights.shape[0] // 512, body)
    send_cores(part, rc, wires, (s,))


def part_sums(part):
    return part.at[:, 0]


def forward_kernel(
    mixed,
    out_t,
    x,
    gain,
    own_up,
    own_down,
    other_up,
    other_down,
    d_ffn,
    whole,
    hidden,
    up,
    down,
    lifted,
    d_pre,
    part,
    rc,
    ra,
    rb,
    ea,
    eb,
    sa,
    sb,
    d_lifted,
    d_rows,
    send,
    recv,
    local,
    *,
    lines,
):
    b = lax.axis_index("batch")
    wires, moves = Wires(send, recv, lines), Moves(local)
    wires.enter(("head", "group", "x") + along(lines))
    order = first_order(lines)
    mine, others, weights = (own_up, own_down), (other_up, other_down), (up, down)
    half, wide = x.shape
    units = lifted.shape[2]

    def pointwise(r, total):
        row = x[r, :].astype(F32) + total
        hidden[r, :] = row
        shifted = row - jnp.mean(row, axis=1, keepdims=True)
        var_row = jnp.mean(shifted * shifted, axis=1, keepdims=True)
        whole[0, 0, r, :] = (shifted * lax.rsqrt(var_row + 1e-05) * gain[...]).astype(BF)

    def piece(i):
        for k in order:
            source = others[i] if k % 2 else mine[i]
            wires.start((i, k), source, weights[i].at[b], ("line", k))

    def relay(i):
        for k in order:
            wires.arrived((i, k))
            block = weights[i].at[b ^ (2 * k)]
            wires.start((i, "x", k), block, block, "x")

    def fetch(s):
        moves.start(d_ffn.at[s], d_rows.at[s % 2])

    def lift_back(s):
        moves.made[2 + s].wait()

        def body(i):
            r = span(i, half)
            d_lifted[s, r, :] = dot(d_rows[s % 2, r, :], down.reshape(wide, units)[...], 1, 0)

        blocks(2, body)
        if s < 2:
            fetch(s + 2)

    def lift(s):
        def body(i):
            r = span(i, half)
            act = dot(whole[s, i], up.reshape(wide, units)[...], 1, 0)
            square = act * act
            turn = jnp.tanh(GELU * act * (1 + 0.044715 * square))
            lifted[s, r, :] = (0.5 * act * (1 + turn)).astype(BF)
            slope = 0.5 * (1 + turn) + 0.5 * act * (1 - turn * turn) * GELU * (1 + 3 * 0.044715 * square)
            d_pre[s, r, :] = (d_lifted[s, r, :] * slope).astype(BF)

        blocks(2, body)

    for i in range(2):
        moves.start(mine[i], weights[i].at[b])
    fetch(0)
    fetch(1)
    piece(1)
    for i in (1, 0):
        wires.start((i, "x", 0), mine[i], weights[i].at[b], "x")
    for s in (3, 1, 2, 0):
        partial_rows(part, rc, wires, mixed.at[s], out_t, s)
    steps = exchange(part, whole, rc, part_sums(part), ra, rb, ea, eb, sa, sb, wires, pointwise)
    next(steps)
    relay(1)
    next(steps)
    piece(0)
    next(steps)
    next(steps)
    moves.made[0].wait()
    moves.made[1].wait()
    wires.arrived(*[(1, "x", k) for k in range(lines)])
    lift_back(0)
    next(steps)
    relay(0)
    lift_back(1)
    next(steps)
    lift_back(2)
    lift_back(3)
    wires.arrived(*[(0, "x", k) for k in range(lines)])
    wires.arrived("own")
    lift(0)
    wires.arrived("fa")
    wires.start("cfa", whole.at[3, 0, pl.ds(0, half // 2)], whole.at[3, 1, pl.ds(0, half // 2)], "head")
    wires.arrived("cza", "czb")
    lift(1)
    wires.arrived("fb")
    wires.start("cfb", whole.at[3, 0, pl.ds(half // 2, half // 2)], whole.at[3, 1, pl.ds(half // 2, half // 2)], "head")
    wires.arrived("cya", "cyb")
    lift(2)
    wires.arrived("cfa", "cfb")
    lift(3)
    wires.finish()


def backward_kernel(
    d_pre,
    up,
    ln_all,
    lifted,
    hidden,
    cotangent,
    factor,
    gain,
    d_ffn,
    whole,
    d_hidden,
    d_gain,
    lines_out,
    part,
    rc,
    ra,
    rb,
    ea,
    eb,
    sa,
    sb,
    grads,
    rx,
    d_cols,
    send,
    recv,
    local,
    *,
    lines,
):
    wires, moves = Wires(send, recv, 2), Moves(local)
    wires.enter(TEAM + ("x",))
    wide, units = up.shape
    step = 256
    tokens = ln_all.shape[0]
    xbit = lax.axis_index("batch") % 2
    flat = grads.reshape(wide, 2 * units)
    d_flat = d_pre.reshape(tokens, units)
    l_flat = lifted.reshape(tokens, units)
    cuts = [pl.ds(0, units), pl.ds(units, units)]
    count = wide // step

    def fetch(i):
        moves.start(d_ffn.at[:, pl.ds(i * step, step)], d_cols.at[i % 2])

    fetch(0)
    fetch(1)
    d_gain[...] = jnp.zeros_like(d_gain)

    def pointwise(r, total):
        row = hidden[r, :]
        shifted = row - jnp.mean(row, axis=1, keepdims=True)
        var_row = jnp.mean(shifted * shifted, axis=1, keepdims=True)
        rstd = lax.rsqrt(var_row + 1e-05)
        unit = shifted * rstd
        terms = total * unit
        d_gain[...] += terms[:8] + terms[8:]
        d_unit = total * gain[...]
        mean_d = jnp.mean(d_unit, axis=1, keepdims=True)
        mean_du = jnp.mean(d_unit * unit, axis=1, keepdims=True)
        grad = cotangent[r, :].astype(F32) * factor[0, 0] + rstd * (d_unit - mean_d - unit * mean_du)
        d_hidden[r, :] = grad
        whole[0, 0, r, :] = grad.astype(BF)

    def up_grads():
        def body(i):
            flat[span(i, step), cuts[0]] = dot(ln_all[:, span(i, step)], d_flat[...], 0, 0).astype(BF)

        blocks(count, body)
        across(wires, grads, rx, cuts[0], lines, "ffn")

    def down_grads():
        for i in range(count):
            moves.made[i].wait()
            flat[pl.ds(i * step, step), cuts[1]] = dot(d_cols[i % 2], l_flat[...], 0, 0).astype(BF)
            if i + 2 < count:
                fetch(i + 2)
        across(wires, grads, rx, cuts[1], lines, "ffn")

    def join(cut):
        for line in range(lines):
            wires.arrived(("ffn", "x", cut.start, line))

            def body(r):
                total = grads[2 * line + xbit, r, cut].astype(F32) + rx[line, r, cut].astype(F32)
                lines_out[line, r, cut] = total.astype(BF)

            tiles(rx.shape[1], body)

    for s in (3, 1, 2, 0):
        partial_rows(part, rc, wires, d_pre.at[s], up, s)
    steps = exchange(part, whole, rc, part_sums(part), ra, rb, ea, eb, sa, sb, wires, pointwise)
    next(steps)
    up_grads()
    next(steps)
    down_grads()
    next(steps)
    next(steps)
    join(cuts[0])
    next(steps)
    next(steps)
    join(cuts[1])
    for _ in steps:
        pass
    half = whole.shape[2] // 2
    for name, end, first in (("fa", "cfa", 0), ("fb", "cfb", half)):
        wires.arrived(name)
        block = pl.ds(first, half)
        wires.start(end, whole.at[3, 0, block], whole.at[3, 1, block], "head")
    wires.arrived("own", "cza", "cyb", "czb", "cya", "cfa", "cfb")
    wires.finish()


def first_order(lines):
    return [k for k in (2, 3, 1) if k < lines] + list(range(4, lines))


class Lines:
    def __init__(self, wires, lined, rz, slices, lines, tag, pick=lambda line: line):
        self.wires, self.lined, self.rz, self.slices, self.lines, self.tag = wires, lined, rz, slices, lines, tag
        self.pick = pick
        self.z = lax.axis_index("batch") // 2
        self.p = self.z % 2
        self.y = lax.axis_index("group")
        self.order = first_order(lines)

    def send(self, cut):
        for k in self.order:
            source = self.lined.at[self.pick(self.z ^ k), :, cut]
            self.wires.start((self.tag, "z", cut.start, k), source, self.rz.at[k, :, cut], ("line", k))

    def join(self, cut):
        lined, rz, slices, p, y = self.lined, self.rz, self.slices, self.p, self.y
        for k in self.order:
            self.wires.arrived((self.tag, "z", cut.start, k))

        def body(r):
            mine = lined[self.pick(self.z), r, cut].astype(F32)
            other = jnp.zeros_like(mine)
            for k in range(1, self.lines):
                term = rz[k, r, cut].astype(F32)
                if k % 2:
                    other = other + term
                else:
                    mine = mine + term
            slices[2 * p + y, r, cut] = mine.astype(BF)
            slices[2 * (1 - p) + y, r, cut] = other.astype(BF)

        tiles(lined.shape[1], body)
        for q in range(2):
            block = slices.at[2 * q + y, :, cut]
            self.wires.start((self.tag, "y", cut.start, q), block, block, "group")

    def store(self, cut, target, first, width, stage, turned=False):
        for q in range(2):
            self.wires.arrived((self.tag, "y", cut.start, q))
        for t in range(4):

            def fill(held):
                def body(r):
                    held[r, pl.ds(0, cut.size)] = self.slices[t, r, cut].astype(F32)

                tiles(target.shape[0], body)

            def fill_turned(held):
                for c in range(0, cut.size, 256):
                    held[pl.ds(c, 256), :] = self.slices[t, :, pl.ds(cut.start + c, 256)].astype(F32).T

            where = pl.ds(t * width + first, cut.size)
            if turned:
                stage.put(fill_turned, target.at[where, :])
            else:
                stage.put(fill, target.at[:, where], cut.size)


class Stage:
    def __init__(self, held, sems):
        self.held, self.sems, self.made = held, sems, []

    def put(self, fill, target, width=None):
        n, ring = len(self.made), self.held.shape[0]
        if n >= ring:
            self.made[n - ring].wait()
        held = self.held.at[n % ring]
        fill(held)
        source = held if width is None else held.at[:, pl.ds(0, width)]
        copy = pltpu.make_async_copy(source, target, self.sems.at[n])
        copy.start()
        self.made.append(copy)

    def finish(self):
        for copy in self.made[-self.held.shape[0] :]:
            copy.wait()


def across(wires, grads, rx, cut, lines, tag):
    other = 1 - lax.axis_index("batch") % 2
    for line in range(lines):
        wires.start((tag, "x", cut.start, line), grads.at[2 * line + other, :, cut], rx.at[line, :, cut], "x")


def across_join(wires, grads, rx, lined, cut, lines, tag, pick=lambda line: line):
    x = lax.axis_index("batch") % 2
    for line in range(lines):
        wires.arrived((tag, "x", cut.start, line))

        def body(r):
            total = grads[2 * line + x, r, cut].astype(F32) + rx[line, r, cut].astype(F32)
            lined[pick(line), r, cut] = total.astype(BF)

        tiles(rx.shape[1], body)


def middle_kernel(
    d_attn,
    w_out,
    mixed,
    gates,
    unit,
    rstd,
    values,
    q_rot,
    k_rot,
    weighted,
    decays,
    cosine,
    sine,
    lifted,
    down,
    hidden,
    ffn_lines,
    d_proj,
    output,
    d_up,
    d_down,
    d_out,
    part,
    rc,
    ry,
    rn,
    rz,
    slices,
    grads,
    rx,
    d_ret,
    d_scores,
    rz_out,
    slices_out,
    held,
    *rest,
    lines,
):
    buffers = rest[:7]
    turned, fetch_sems, stage_sems, turn_sems, send, recv = rest[7:]
    wires = Wires(send, recv, lines)
    stage = Stage(held, stage_sems)
    turner = Stage(turned, turn_sems)
    fetched = {}

    def fetch(s):
        for n, (source, buffer) in enumerate(zip((gates, unit, rstd, values, q_rot, k_rot, weighted), buffers)):
            copy = pltpu.make_async_copy(source.at[s], buffer.at[s % 2], fetch_sems.at[7 * s + n])
            copy.start()
            fetched[s, n] = copy

    fetch(0)
    fetch(1)
    wires.enter(("head", "group", "x") + along(lines))
    length = d_attn.shape[1]
    half = length // 2
    wide = w_out.shape[0]
    val = w_out.shape[1]
    units = lifted.shape[2]
    key = q_rot.shape[2]
    step = 256
    ffn = Lines(wires, ffn_lines, rz, slices, lines, "ffn")
    cuts = [pl.ds(c, units) for c in (0, units)]
    xbit = lax.axis_index("batch") % 2

    def pick(line):
        return 2 * line + xbit

    outs = Lines(wires, grads, rz_out, slices_out, lines, "out", pick)
    out_cut = pl.ds(0, val)

    def partial(s):
        def body(i):
            cut = span(i, 512)
            total = dot(lifted[s], down[cut, :], 1, 1)
            part[s, 1, :, cut] = total[half:].astype(BF)
            part[s, 0, :, cut] = total[:half].astype(BF)

        blocks(wide // 512, body)
        send_cores(part, rc, wires, (s,))

    def pointwise(r, total):
        output[r, :] = (hidden[r, :] + total).astype(BF)

    def retention(s):
        for n in range(7):
            fetched[s, n].wait()
        gates_s, unit_s, rstd_s, values_s, q_s, k_s, weighted_s = [buffer.at[s % 2] for buffer in buffers]

        def mix(i):
            r = span(i, half)
            d_mixed = dot(d_attn[s, r, :], w_out[...], 1, 0)
            gate = gates_s[r, :].astype(F32)
            sig = jax.nn.sigmoid(gate)
            norm = unit_s[r, :].astype(F32)
            d_gate = d_mixed * norm * (sig * (1 + gate * (1 - sig)))
            d_proj[s, r, pl.ds(2 * key + val, val)] = d_gate.astype(BF)
            d_norm = d_mixed * (gate * sig)
            mean_d = jnp.mean(d_norm, axis=1, keepdims=True)
            mean_dn = jnp.mean(d_norm * norm, axis=1, keepdims=True)
            d_ret[r, :] = (rstd_s[r, :][:, :1] * (d_norm - mean_d - norm * mean_dn)).astype(BF)

        blocks(2, mix)
        d_proj[s, :, pl.ds(2 * key, val)] = dot(weighted_s[...], d_ret[...], 0, 0).astype(BF)
        d_scores[...] = (dot(d_ret[...], values_s[...], 1, 1) * decays[...]).astype(BF)

        def turn(grad, first):
            a, b = grad[:, : key // 2], grad[:, key // 2 :]
            d_proj[s, :, pl.ds(first, key // 2)] = (a * cosine[...] + b * sine[...]).astype(BF)
            d_proj[s, :, pl.ds(first + key // 2, key // 2)] = (b * cosine[...] - a * sine[...]).astype(BF)

        turn(dot(d_scores[...], k_s[...], 1, 0), 0)
        turn(dot(d_scores[...], q_s[...], 0, 0), key)
        if s < 2:
            fetch(s + 2)

    def out_grads():
        flat = grads.reshape(wide, val)

        def body(i):
            total = jnp.zeros((step, val), F32)
            for s in range(4):
                total = total + dot(d_attn[s, :, span(i, step)], mixed[s], 0, 0)
            flat[span(i, step), :] = total.astype(BF)

        blocks(wide // step, body)
        across(wires, grads, rx, pl.ds(0, val), lines, "out")

    steps = reduce_rows(part, rc, ry, rn, wires, pointwise)
    ffn.send(cuts[0])
    ffn.send(cuts[1])
    partial(3)
    partial(2)
    next(steps)
    partial(1)
    next(steps)
    partial(0)
    next(steps)
    out_grads()
    retention(0)
    retention(1)
    next(steps)
    retention(2)
    across_join(wires, grads, rx, grads, out_cut, lines, "out", pick)
    outs.send(out_cut)
    retention(3)
    ffn.join(cuts[0])
    ffn.join(cuts[1])
    for _ in steps:
        pass
    ffn.store(cuts[0], d_up, 0, units, stage)
    ffn.store(cuts[1], d_down, 0, units, turner, True)
    outs.join(out_cut)
    outs.store(out_cut, d_out, 0, val, turner, True)
    stage.finish()
    turner.finish()
    wires.finish()


def last_kernel(
    d_proj,
    x,
    d_hidden,
    gain,
    ln_gains,
    normed_hbm,
    stacked_hbm,
    d_inputs,
    gains,
    d_query,
    d_key,
    d_value,
    d_gate,
    normed,
    stacked,
    grads,
    part,
    rc,
    ry,
    rn,
    rx,
    rz,
    slices,
    held,
    came,
    staged,
    local,
    stage_sems,
    send,
    recv,
    *,
    lines,
):
    wires, moves = Wires(send, recv, lines), Moves(local)
    wide, columns = stacked.shape
    tokens = normed.shape[0]
    step = 256
    val = d_value.shape[1] // 4
    key = d_query.shape[1] // 4
    for i in range(wide // step):
        cut = pl.ds(i * step, step)
        moves.start(normed_hbm.at[:, cut], normed.at[:, cut])
    moves.start(stacked_hbm, stacked)
    wires.enter(("head", "group", "x") + along(lines))
    xbit = lax.axis_index("batch") % 2
    stage = Stage(staged, stage_sems)

    def pick(line):
        return 2 * line + xbit

    main = Lines(wires, grads, rz, slices, lines, "main", pick)
    cuts = [pl.ds(c, 256) for c in (2 * key + val, 2 * key + val + 256, 2 * key, 2 * key + 256, 0, key)]
    flat = grads.reshape(wide, columns)
    held[0] = jnp.zeros_like(held[0])
    rows_all = d_proj.reshape(tokens, columns)

    def pointwise(r, total):
        row = x[r, :].astype(F32)
        scale = lax.rsqrt(jnp.mean(row * row, axis=1, keepdims=True) + 1e-06)
        unit = row * scale
        terms = total * unit
        held[0, :8] += terms[:8] + terms[8:]
        d_unit = total * gain[...]
        mean_du = jnp.mean(d_unit * unit, axis=1, keepdims=True)
        d_inputs[r, :] = (d_hidden[r, :] + scale * (d_unit - unit * mean_du)).astype(BF)

    def weight_grads(first, wait=False):
        cut = pl.ds(first, 512)

        def body(i):
            flat[span(i, step), cut] = dot(normed[:, span(i, step)], rows_all[:, cut], 0, 0).astype(BF)

        if wait:
            for i in range(wide // step):
                moves.made[i].wait()
                body(i)
        else:
            blocks(wide // step, body)
        for c in (first, first + 256):
            across(wires, grads, rx, pl.ds(c, 256), lines, "main")

    def partial(s):
        rows = d_proj.shape[1] // 2

        def body(i):
            cut = span(i, 512)
            total = dot(d_proj[s], stacked[cut, :], 1, 1)
            part[s, 1, :, cut] = total[rows:].astype(BF)
            part[s, 0, :, cut] = total[:rows].astype(BF)

        blocks(wide // 512, body)
        send_cores(part, rc, wires, (s,))

    def stage_x(at):
        across_join(wires, grads, rx, grads, cuts[at], lines, "main", pick)
        main.send(cuts[at])

    hops = ["head", "group", "x"]
    bit = 1
    while bit < lines:
        hops.append(("line", bit))
        bit *= 2

    def hop(at):
        if at:
            wires.arrived(("gain", at - 1))
            held[at] = held[at - 1] + came[at - 1]
        else:
            held[0, 8:] = ln_gains[...]
        if at < len(hops):
            wires.start(("gain", at), held.at[at], came.at[at], hops[at])
        else:
            gains[...] = held[at]

    targets = [(d_gate, val, 0), (d_gate, val, 256), (d_value, val, 0), (d_value, val, 256), (d_query, key, 0), (d_key, key, 0)]

    def store(at):
        target, width, first = targets[at]
        main.store(cuts[at], target, first, width, stage)

    steps = reduce_rows(part, rc, ry, rn, wires, pointwise)
    weight_grads(2 * key + val, True)
    moves.made[-1].wait()
    partial(3)
    partial(2)
    next(steps)
    weight_grads(2 * key)
    next(steps)
    stage_x(0)
    partial(1)
    weight_grads(0)
    next(steps)
    stage_x(1)
    partial(0)
    next(steps)
    stage_x(2)
    main.join(cuts[0])
    stage_x(3)
    main.join(cuts[1])
    stage_x(4)
    stage_x(5)
    main.join(cuts[2])
    for _ in steps:
        pass
    hop(0)
    main.join(cuts[3])
    hop(1)
    store(0)
    store(1)
    hop(2)
    store(2)
    main.join(cuts[4])
    hop(3)
    store(3)
    hop(4)
    main.join(cuts[5])
    store(4)
    store(5)
    for at in range(5, len(hops) + 1):
        hop(at)
    stage.finish()
    wires.finish()


def exchange_scratch(rows, width):
    half = rows // 2
    return [
        pltpu.VMEM((4, 2, rows, width), BF),
        pltpu.VMEM((4, rows, width), BF),
        pltpu.VMEM((2, half, width), BF),
        pltpu.VMEM((2, half, width), BF),
        pltpu.VMEM((half, width), BF),
        pltpu.VMEM((half, width), BF),
        pltpu.VMEM((half, width), BF),
        pltpu.VMEM((half, width), BF),
    ]


def lean_scratch(rows, width):
    return [
        pltpu.VMEM((4, 2, rows, width), BF),
        pltpu.VMEM((4, rows, width), BF),
        pltpu.VMEM((2, rows, width), BF),
        pltpu.VMEM((rows, width), BF),
    ]


def semaphores(count):
    return [pltpu.SemaphoreType.DMA((count,)), pltpu.SemaphoreType.DMA((count,))]


def anywhere():
    return pl.BlockSpec(memory_space=pl.ANY)


def vmem():
    return pl.BlockSpec(memory_space=pltpu.VMEM)


def forward_exchange(mixed, out_t, x, gain, own, other, d_ffn, batch):
    rows, width = x.shape
    lines = batch // 2
    high, units = own[0].shape
    length = 2 * rows
    whole, hidden, up, down, lifted, d_pre = pl.pallas_call(
        functools.partial(forward_kernel, lines=lines),
        out_shape=(
            jax.ShapeDtypeStruct((4, 2, rows, width), BF),
            jax.ShapeDtypeStruct((rows, width), F32),
            jax.ShapeDtypeStruct((batch, high, units), BF),
            jax.ShapeDtypeStruct((batch, high, units), BF),
            jax.ShapeDtypeStruct((4, length, units), BF),
            jax.ShapeDtypeStruct((4, length, units), BF),
        ),
        in_specs=[vmem()] * 8 + [anywhere()],
        out_specs=tuple([vmem()] * 6),
        scratch_shapes=exchange_scratch(rows, width)
        + [pltpu.VMEM((4, length, units), F32), pltpu.VMEM((2, length, width), BF)]
        + semaphores(24 + 4 * lines)
        + [pltpu.SemaphoreType.DMA((6,))],
        compiler_params=pltpu.CompilerParams(collective_id=0, has_side_effects=True, vmem_limit_bytes=58 * 2**20),
        cost_estimate=pl.CostEstimate(flops=12 * 10**9, bytes_accessed=300000000, transcendentals=0),
        name="forward_exchange",
    )(mixed, out_t, x, gain[None], *own, *other, d_ffn.reshape(4, length, width))
    return whole.reshape(8 * rows, width), hidden, up.reshape(width, -1), down.reshape(width, -1), lifted, d_pre


def backward_exchange(d_pre, up, ln_all, lifted, hidden, cotangent, factor, gain, d_ffn, batch):
    rows, width = hidden.shape
    lines = batch // 2
    block = (width // batch, 2 * up.shape[1])
    whole, d_hidden, d_gain, lined = pl.pallas_call(
        functools.partial(backward_kernel, lines=lines),
        out_shape=(
            jax.ShapeDtypeStruct((4, 2, rows, width), BF),
            jax.ShapeDtypeStruct((rows, width), F32),
            jax.ShapeDtypeStruct((8, width), F32),
            jax.ShapeDtypeStruct((lines,) + block, BF),
        ),
        in_specs=[vmem()] * 6 + [pl.BlockSpec(memory_space=pltpu.SMEM), vmem(), anywhere()],
        out_specs=(vmem(), vmem(), vmem(), vmem()),
        scratch_shapes=exchange_scratch(rows, width)
        + [
            pltpu.VMEM((batch,) + block, BF),
            pltpu.VMEM((lines,) + block, BF),
            pltpu.VMEM((2, 8 * rows, 256), BF),
        ]
        + semaphores(24 + 2 * lines)
        + [pltpu.SemaphoreType.DMA((width // 256,))],
        compiler_params=pltpu.CompilerParams(collective_id=1, has_side_effects=True, vmem_limit_bytes=63 * 2**20),
        cost_estimate=pl.CostEstimate(flops=14 * 10**9, bytes_accessed=300000000, transcendentals=0),
        name="backward_exchange",
    )(d_pre, up, ln_all, lifted, hidden, cotangent, factor.reshape(1, 1), gain[None], d_ffn)
    return whole.reshape(8 * rows, width), d_hidden, d_gain, lined


def middle_exchange(d_attn, w_out, mixed, saved, tables, lifted, down, hidden, ffn_lines, batch):
    rows, width = hidden.shape
    lines = batch // 2
    length = 2 * rows
    block = ffn_lines.shape[1:]
    val = w_out.shape[1]
    units = lifted.shape[2]
    gates, unit, rstd, values, q_rot, k_rot, weighted = saved
    columns = 2 * q_rot.shape[2] + 2 * val
    return pl.pallas_call(
        functools.partial(middle_kernel, lines=lines),
        out_shape=(
            jax.ShapeDtypeStruct((4, length, columns), BF),
            jax.ShapeDtypeStruct((rows, width), BF),
            jax.ShapeDtypeStruct((block[0], 4 * units), F32),
            jax.ShapeDtypeStruct((4 * units, block[0]), F32),
            jax.ShapeDtypeStruct((4 * val, block[0]), F32),
        ),
        in_specs=[vmem()] * 3 + [anywhere()] * 7 + [vmem()] * 7,
        out_specs=(vmem(), vmem(), anywhere(), anywhere(), anywhere()),
        scratch_shapes=lean_scratch(rows, width)
        + [
            pltpu.VMEM((lines,) + block, BF),
            pltpu.VMEM((4,) + block, BF),
            pltpu.VMEM((batch, block[0], val), BF),
            pltpu.VMEM((lines, block[0], val), BF),
            pltpu.VMEM((length, val), BF),
            pltpu.VMEM((length, length), BF),
            pltpu.VMEM((lines, block[0], val), BF),
            pltpu.VMEM((4, block[0], val), BF),
            pltpu.VMEM((2, block[0], units), F32),
        ]
        + [pltpu.VMEM((2,) + v.shape[1:], v.dtype) for v in saved]
        + [pltpu.VMEM((2, units, block[0]), F32)]
        + [pltpu.SemaphoreType.DMA((28,)), pltpu.SemaphoreType.DMA((4,)), pltpu.SemaphoreType.DMA((8,))]
        + semaphores(16 + 3 * (lines + 1) + lines),
        compiler_params=pltpu.CompilerParams(collective_id=4, has_side_effects=True, vmem_limit_bytes=63 * 2**20),
        cost_estimate=pl.CostEstimate(flops=20 * 10**9, bytes_accessed=200000000, transcendentals=0),
        name="middle_exchange",
    )(
        d_attn.reshape(4, length, width),
        w_out,
        mixed,
        gates,
        unit,
        rstd,
        values,
        q_rot,
        k_rot,
        weighted,
        *tables,
        lifted,
        down,
        hidden,
        ffn_lines,
    )


def last_exchange(d_proj, x, d_hidden, gain, ln_gains, normed, stacked, key, batch):
    rows, width = x.shape
    lines = batch // 2
    high = width // batch
    columns = stacked.shape[1]
    val = (columns - 2 * key) // 2
    steps = 2 + batch.bit_length() - 1
    return pl.pallas_call(
        functools.partial(last_kernel, lines=lines),
        out_shape=(
            jax.ShapeDtypeStruct((rows, width), BF),
            jax.ShapeDtypeStruct((16, width), F32),
            jax.ShapeDtypeStruct((high, 4 * key), F32),
            jax.ShapeDtypeStruct((high, 4 * key), F32),
            jax.ShapeDtypeStruct((high, 4 * val), F32),
            jax.ShapeDtypeStruct((high, 4 * val), F32),
        ),
        in_specs=[vmem()] * 5 + [anywhere()] * 2,
        out_specs=(vmem(), vmem()) + tuple([anywhere()] * 4),
        scratch_shapes=[
            pltpu.VMEM(normed.shape, BF),
            pltpu.VMEM(stacked.shape, BF),
            pltpu.VMEM((batch, high, columns), BF),
        ]
        + lean_scratch(rows, width)
        + [
            pltpu.VMEM((lines, high, columns), BF),
            pltpu.VMEM((lines, high, columns), BF),
            pltpu.VMEM((4, high, columns), BF),
            pltpu.VMEM((steps + 1, 16, width), F32),
            pltpu.VMEM((steps, 16, width), F32),
            pltpu.VMEM((2, high, val), F32),
            pltpu.SemaphoreType.DMA((width // 256 + 1,)),
            pltpu.SemaphoreType.DMA((4 * (columns // 256),)),
        ]
        + semaphores(16 + steps + (columns // 256) * (2 * lines + 1)),
        compiler_params=pltpu.CompilerParams(collective_id=3, has_side_effects=True, vmem_limit_bytes=63 * 2**20),
        cost_estimate=pl.CostEstimate(flops=26 * 10**9, bytes_accessed=300000000, transcendentals=0),
        name="last_exchange",
    )(d_proj, x, d_hidden, gain[None], ln_gains, normed, stacked)


class Place:
    def __init__(self):
        self.batch = lax.axis_size("batch")
        self.b = lax.axis_index("batch")
        self.y = lax.axis_index("group")
        self.c = lax.axis_index("head")
        self.lines = self.batch // 2
        self.z = self.b // 2
        self.x = self.b % 2
        self.p = self.z % 2
        self.slot = 2 * self.p + self.y

    def cut(self, array, axis):
        width = array.shape[axis] // 4
        own = lax.dynamic_slice_in_dim(array, self.slot * width, width, axis)
        other = lax.dynamic_slice_in_dim(array, (self.slot ^ 2) * width, width, axis)
        return own, other

def on_device(
    inputs,
    rms_gain,
    w_query,
    w_key,
    w_value,
    w_gate,
    w_out,
    ln_gain,
    w_up,
    w_down,
    cotangent,
    domain_of,
    domain_weight,
):
    here = Place()

    parts = [here.cut(w, 1) for w in (w_query, w_key, w_value, w_gate)]
    own = jnp.concatenate([own for own, _ in parts], axis=1)
    other = jnp.concatenate([other for _, other in parts], axis=1)
    out_own, out_other = [v.T for v in here.cut(w_out, 0)]
    factor = sequence_factor(domain_of, domain_weight)
    own_index = here.b * lax.axis_size("group") + here.y
    own_factor = lax.dynamic_index_in_dim(factor, own_index, 0, keepdims=False)
    stacked, out_t, normed_all, d_ffn_all, mixed, saved, tables = gather_first(
        (own, out_own), (other, out_other), inputs[0], rms_gain, cotangent[0], own_factor, KEY, here.batch
    )
    up_parts = here.cut(w_up, 1)
    down_parts = [v.T for v in here.cut(w_down, 0)]
    ln_all, hidden, up, down_t, lifted, d_pre = forward_exchange(
        mixed,
        out_t,
        inputs[0],
        ln_gain,
        (up_parts[0], down_parts[0]),
        (up_parts[1], down_parts[1]),
        d_ffn_all,
        here.batch,
    )
    d_attn_all, d_hidden, d_ln_gain, ffn_lines = backward_exchange(
        d_pre, up, ln_all, lifted, hidden, cotangent[0], own_factor, ln_gain, d_ffn_all, here.batch
    )
    d_proj, output, d_up, d_down, d_w_out = middle_exchange(
        d_attn_all,
        out_t,
        mixed,
        saved,
        tables,
        lifted,
        down_t,
        hidden,
        ffn_lines,
        here.batch,
    )
    d_inputs, gains, d_query, d_key, d_value, d_gate = last_exchange(
        d_proj, inputs[0], d_hidden, rms_gain, d_ln_gain, normed_all, stacked, KEY, here.batch
    )
    gain_rms = jnp.sum(gains[:8], axis=0)
    gain_ln = jnp.sum(gains[8:], axis=0)
    return (
        output[None],
        d_inputs[None],
        gain_rms,
        d_query,
        d_key,
        d_value,
        d_gate,
        d_w_out,
        gain_ln,
        d_up,
        d_down,
    )


def solution(mesh):
    rows = P(("batch", "group"), "head", None)
    wide = P("batch", "head")
    tall = P("head", "batch")
    return jax.shard_map(
        on_device,
        mesh=mesh,
        in_specs=(rows, P(), wide, wide, wide, wide, tall, P(), wide, tall, rows, P(), P()),
        out_specs=(rows, rows, P(), wide, wide, wide, wide, tall, P(), wide, tall),
        check_vma=False,
    )
```

```python
import functools

import jax
import jax.numpy as jnp
import numpy as np
from jax import lax
from jax.experimental import pallas as pl
from jax.experimental.pallas import tpu as pltpu
from jax.sharding import PartitionSpec as P


KEY = 256
VAL = 512
GELU = 0.7978845608028654
BF = jnp.bfloat16
F32 = jnp.float32


def own_share(domains, domain_of, domain_weight):
    me = domain_of[lax.axis_index("batch") * lax.axis_size("group") + lax.axis_index("group")]
    row = domains[...]
    total = count = weight = jnp.zeros((1, 1), F32)
    for d in range(domain_weight.shape[0]):
        n = jnp.sum((row == d).astype(F32), axis=1, keepdims=True)
        w = domain_weight[d].astype(F32)
        total = total + jnp.where(n > 0, n * (w / jnp.maximum(n, 1.0)), 0.0)
        count = count + jnp.where(me == d, n, 0.0)
        weight = weight + jnp.where(me == d, w, 0.0)
    return jnp.float32(domains.shape[1]) * weight / (count * total)


TEAM = ("head", "batch", "group")


def peers(lines):
    b = lax.axis_index("batch")
    table = {
        "head": {"head": 1 - lax.axis_index("head")},
        "batch": {"batch": b ^ 2},
        "group": {"group": 1 - lax.axis_index("group")},
        "x": {"batch": b ^ 1},
    }
    for k in range(1, lines):
        table["line", k] = {"batch": b ^ (2 * k)}
    return table


def along(lines):
    return tuple(("line", k) for k in range(1, lines))


class Wires:
    def __init__(self, send, recv, lines=1):
        self.send, self.recv, self.made, self.peers = send, recv, {}, peers(lines)

    def enter(self, names):
        barrier = pltpu.get_barrier_semaphore()
        for name in names:
            pl.semaphore_signal(barrier, inc=1, device_id=self.peers[name], device_id_type=pl.DeviceIdType.MESH)
        pl.semaphore_wait(barrier, len(names))

    def start(self, name, source, target, peer, go=True):
        n = len(self.made)
        copy = pltpu.make_async_remote_copy(
            src_ref=source,
            dst_ref=target,
            send_sem=self.send.at[n],
            recv_sem=self.recv.at[n],
            device_id=self.peers[peer],
            device_id_type=pl.DeviceIdType.MESH,
        )
        if go:
            copy.start()
        self.made[name] = copy

    def plan(self, *copy):
        self.start(*copy, go=False)

    def go(self, names):
        for name in names:
            self.made[name].start()

    def arrived(self, *names):
        for name in names:
            self.made[name].wait_recv()

    def finish(self):
        for copy in self.made.values():
            copy.wait_send()


class Moves:
    def __init__(self, sems):
        self.sems, self.made = sems, []

    def start(self, source, target):
        copy = pltpu.make_async_copy(source, target, self.sems.at[len(self.made)])
        copy.start()
        self.made.append(copy)

    def finish(self):
        for copy in self.made:
            copy.wait()


TILE = 16


def tiles(rows, body):
    def step(i, _):
        body(pl.ds(pl.multiple_of(i * TILE, TILE), TILE))
        return 0

    lax.fori_loop(0, rows // TILE, step, 0)


def exchange(part, whole, rc, sums, ra, rb, ea, eb, sa, sb, wires, pointwise, tag=""):
    rows = part.shape[2]
    half = rows // 2
    top, low = pl.ds(0, half), pl.ds(half, half)

    def start(name, *rest):
        wires.start(tag + name, *rest)

    def arrived(*names):
        wires.arrived(*[tag + name for name in names])

    def add(s, first):
        def body(r):
            rr = pl.ds(r.start + first, TILE)
            total = part[s, 0, rr, :].astype(F32) + rc[s, rr, :].astype(F32)
            sums[s, rr, :] = total.astype(BF)

        tiles(half, body)

    arrived("c3")
    add(3, 0)
    start("a3", sums.at[3, top], ra.at[0], "batch")
    add(3, half)
    start("b3", sums.at[3, low], rb.at[0], "group")
    arrived("c1")
    add(1, 0)
    start("a1", sums.at[1, top], ra.at[1], "batch")
    arrived("c2")
    add(2, half)
    start("b2", sums.at[2, low], rb.at[1], "group")
    add(2, 0)
    add(1, half)

    def second_a(r):
        sa[r, :] = (sums[2, r, :].astype(F32) + ra[0, r, :].astype(F32)).astype(BF)

    def second_b(r):
        rr = pl.ds(r.start + half, TILE)
        sb[r, :] = (sums[1, rr, :].astype(F32) + rb[0, r, :].astype(F32)).astype(BF)

    yield
    arrived("a3")
    tiles(half, second_a)
    start("a2", sa, ea, "group")
    arrived("b3")
    tiles(half, second_b)
    start("b1", sb, eb, "batch")

    def last(first, near, end):
        def body(r):
            rr = pl.ds(r.start + first, TILE)
            total = part[0, 0, rr, :].astype(F32) + rc[0, rr, :].astype(F32)
            total = total + near[1, r, :].astype(F32) + end[r, :].astype(F32)
            pointwise(rr, total)

        tiles(half, body)

    yield
    arrived("c0", "a1", "a2")
    last(0, ra, ea)
    if whole is not None:
        start("za", whole.at[0, 0, top], whole.at[1, 0, top], "batch")
    yield
    arrived("b2", "b1")
    last(half, rb, eb)
    if whole is None:
        return
    start("yb", whole.at[0, 0, low], whole.at[2, 0, low], "group")
    start("zb", whole.at[0, 0, low], whole.at[1, 0, low], "batch")
    start("ya", whole.at[0, 0, top], whole.at[2, 0, top], "group")
    start("own", whole.at[0, 0], whole.at[0, 1], "head")
    yield
    arrived("za")
    start("fa", whole.at[1, 0, top], whole.at[3, 0, top], "group")
    start("cza", whole.at[1, 0, top], whole.at[1, 1, top], "head")
    arrived("yb")
    start("fb", whole.at[2, 0, low], whole.at[3, 0, low], "batch")
    start("cyb", whole.at[2, 0, low], whole.at[2, 1, low], "head")
    yield
    arrived("zb")
    start("czb", whole.at[1, 0, low], whole.at[1, 1, low], "head")
    arrived("ya")
    start("cya", whole.at[2, 0, top], whole.at[2, 1, top], "head")
    yield


def reduce_rows(part, rc, ry, rn, wires, pointwise, tag=""):
    rows = part.shape[2]
    half = rows // 2
    ends = [pl.ds(0, half), pl.ds(half, half)]

    def add(s, end):
        def body(r):
            rr = pl.ds(r.start + end.start, TILE)
            total = part[s, 0, rr, :].astype(F32) + rc[s, rr, :].astype(F32)
            part[s, 0, rr, :] = total.astype(BF)

        tiles(half, body)

    for s, at in ((3, 0), (2, 1)):
        wires.arrived(f"{tag}c{s}")
        for h, end in enumerate(ends):
            add(s, end)
            wires.start((tag, s, h), part.at[s, 0, end], ry.at[at, end], "group")
        yield
    wires.arrived(f"{tag}c1")
    for end in ends:
        add(1, end)
    yield
    for h, end in enumerate(ends):
        wires.arrived((tag, 3, h))

        def body(r):
            rr = pl.ds(r.start + end.start, TILE)
            total = part[1, 0, rr, :].astype(F32) + ry[0, rr, :].astype(F32)
            part[1, 0, rr, :] = total.astype(BF)

        tiles(half, body)
        wires.start((tag, 1, h), part.at[1, 0, end], rn.at[end], "batch")
    yield
    wires.arrived(f"{tag}c0")
    for h, end in enumerate(ends):
        wires.arrived((tag, 2, h), (tag, 1, h))

        def last(r):
            rr = pl.ds(r.start + end.start, TILE)
            total = part[0, 0, rr, :].astype(F32) + rc[0, rr, :].astype(F32)
            pointwise(rr, total + ry[1, rr, :].astype(F32) + rn[rr, :].astype(F32))

        tiles(half, last)


def send_cores(part, rc, wires, slots=(3, 1, 2, 0), tag=""):
    for s in slots:
        wires.start(tag + f"c{s}", part.at[s, 1], rc.at[s], "head")


def dot(left, right, left_dim, right_dim):
    return lax.dot_general(left, right, (((left_dim,), (right_dim,)), ((), ())), preferred_element_type=F32)


def blocks(count, body):
    def step(i, _):
        body(i)
        return 0

    lax.fori_loop(0, count, step, 0)


def span(i, size):
    return pl.ds(pl.multiple_of(i * size, size), size)


def gather_kernel(
    own,
    own_out,
    other,
    other_out,
    x,
    gain,
    cotangent,
    domains,
    domain_of,
    domain_weight,
    stacked_hbm,
    out_t,
    normed_hbm,
    d_ffn,
    mixed,
    *rest,
    lines,
):
    saved_hbm, tables_hbm, rest = rest[:7], rest[7:10], rest[10:]
    stacked, whole, normed, d_rows, cosine, sine, decays, unit_full = rest[:8]
    saved, (send, recv, local) = rest[8:15], rest[15:]
    gates, unit, rstd, values, q_rot, k_rot, weighted = saved
    b, c = lax.axis_index("batch"), lax.axis_index("head")
    slot = 2 * ((b // 2) % 2) + lax.axis_index("group")
    wires, moves = Wires(send, recv, lines), Moves(local)
    wires.enter(("head", "group", "x") + along(lines))
    order = first_order(lines)
    half, wide = x.shape
    length = 2 * half
    key, val = q_rot.shape[2], values.shape[2]
    cuts = [(0, pl.ds(0, 512)), (0, pl.ds(512, 512)), (0, pl.ds(1024, 256)), (0, pl.ds(1280, 256))]
    cuts += [(1, pl.ds(0, 256)), (1, pl.ds(256, 256))]
    mine, others, weights = (own, own_out), (other, other_out), (stacked, out_t)

    def piece(i, cut):
        for k in order:
            source = others[i] if k % 2 else mine[i]
            wires.plan((i, cut.start, k), source.at[:, cut], weights[i].at[b, :, cut], ("line", k))
        wires.start((i, cut.start, "x", 0), mine[i].at[:, cut], weights[i].at[b, :, cut], "x")

    def relay(i, cut):
        for k in order:
            wires.arrived((i, cut.start, k))
            block = weights[i].at[b ^ (2 * k), :, cut]
            wires.start((i, cut.start, "x", k), block, block, "x")

    def ready(i, cut):
        wires.arrived(*[(i, cut.start, "x", k) for k in range(lines)])

    share = own_share(domains, domain_of, domain_weight)

    def body(r):
        row = x[r, :].astype(F32)
        scale = lax.rsqrt(jnp.mean(row * row, axis=1, keepdims=True) + 1e-06)
        normed[r, :] = (row * scale * gain[...]).astype(BF)
        d_rows[r, :] = (cotangent[r, :].astype(F32) * share).astype(BF)

    tiles(half, body)
    wires.start("y", normed, whole.at[2, 0], "group")
    wires.start("own", normed, whole.at[0, 1], "head")
    wires.plan("z", normed, whole.at[1, 0], ("line", 1))
    wires.plan("dz", d_rows, d_ffn.at[1, 0], ("line", 1))
    for cut in cuts:
        piece(*cut)
    near_first = sorted(order)

    def names(cuts_now, ks):
        return [(i, cut.start, k) for i, cut in cuts_now for k in ks]

    @pl.when(c == 0)
    def _():
        wires.go(["z"] + names(cuts[:1], near_first) + ["dz"] + names(cuts[1:], near_first))

    @pl.when(c == 1)
    def _():
        wires.go(names(cuts[:1], order) + ["z"] + names(cuts[1:2], order) + ["dz"] + names(cuts[2:], order))

    moves.start(normed, whole.at[0, 0])
    for i in range(2):
        moves.start(mine[i], weights[i].at[b])
    wires.start("dy", d_rows, d_ffn.at[2, 0], "group")
    wires.start("down", d_rows, d_ffn.at[0, 1], "head")
    moves.start(d_rows, d_ffn.at[0, 0])

    lane = lax.broadcasted_iota(jnp.int32, (half, key // 2), 1).astype(F32)
    freqs = jnp.exp(lane * jnp.float32(-np.log(10000.0) / (key // 2 - 1)))
    for h in range(2):
        first = (h * half + c * half) % length
        places = (lax.broadcasted_iota(jnp.int32, (half, key // 2), 0) + first).astype(F32)
        cosine[pl.ds(h * half, half), :] = jnp.cos(places * freqs)
        sine[pl.ds(h * half, half), :] = jnp.sin(places * freqs)
    head = 4 * c + slot
    log_keep = jnp.float32(0)
    for h in range(8):
        log_keep = jnp.where(head == h, jnp.float32(np.log1p(-(2.0 ** (-5 - h)))), log_keep)

    def decay_rows(r):
        n = lax.broadcasted_iota(jnp.int32, (TILE, length), 0) + r.start
        m = lax.broadcasted_iota(jnp.int32, (TILE, length), 1)
        offset = (n + c * half) % length - (m + c * half) % length
        steps = jnp.maximum(offset, 0).astype(F32)
        decays[r, :] = jnp.where(offset >= 0, jnp.exp(steps * log_keep), jnp.float32(0))

    tiles(length, decay_rows)

    rows = whole.reshape(4, length, wide)
    flat = stacked.reshape(wide, stacked.shape[2])

    def turn(s):
        total = dot(rows[s], flat[:, pl.ds(0, 2 * key)], 1, 0)
        for target, at in ((q_rot, 0), (k_rot, key)):
            a, b_ = total[:, at : at + key // 2], total[:, at + key // 2 : at + key]
            target[s, :, pl.ds(0, key // 2)] = (a * cosine[...] - b_ * sine[...]).astype(BF)
            target[s, :, pl.ds(key // 2, key // 2)] = (b_ * cosine[...] + a * sine[...]).astype(BF)

    def retain(s):
        values[s] = dot(rows[s], flat[:, pl.ds(2 * key, val)], 1, 0).astype(BF)
        weighted[s] = (dot(q_rot[s], k_rot[s], 1, 1) * decays[...]).astype(BF)

        def part(i):
            r = span(i, half)
            retained = dot(weighted[s, r, :], values[s], 1, 0)
            centered = retained - jnp.mean(retained, axis=1, keepdims=True)
            scale = lax.rsqrt(jnp.mean(centered * centered, axis=1, keepdims=True) + 1e-05)
            full = centered * scale
            unit_full[s, r, :] = full
            unit[s, r, :] = full.astype(BF)
            rstd[s, r, :] = jnp.broadcast_to(scale, (half, rstd.shape[2]))

        blocks(2, part)

    def mix(s):
        def part(i):
            r = span(i, half)
            gate = dot(rows[s, r, :], flat[:, pl.ds(2 * key + val, val)], 1, 0)
            gates[s, r, :] = gate.astype(BF)
            mixed[s, r, :] = (unit_full[s, r, :] * (gate * jax.nn.sigmoid(gate))).astype(BF)

        blocks(2, part)

    wires.arrived("z")
    wires.start("far", whole.at[1, 0], whole.at[3, 0], "group")
    wires.start("cz", whole.at[1, 0], whole.at[1, 1], "head")
    wires.arrived("y")
    wires.start("cy", whole.at[2, 0], whole.at[2, 1], "head")
    relay(*cuts[0])
    wires.arrived("far")
    wires.start("cfar", whole.at[3, 0], whole.at[3, 1], "head")
    moves.finish()
    wires.arrived("own", "cz", "cy")
    ready(*cuts[0])
    keep = Moves(local.at[pl.ds(8, 13)])
    keep.start(decays, tables_hbm[0])
    keep.start(cosine, tables_hbm[1])
    keep.start(sine, tables_hbm[2])
    turn(0)
    turn(1)
    turn(2)
    relay(*cuts[1])
    wires.arrived("dz")
    wires.start("dfar", d_ffn.at[1, 0], d_ffn.at[3, 0], "group")
    wires.start("dcz", d_ffn.at[1, 0], d_ffn.at[1, 1], "head")
    relay(*cuts[2])
    wires.arrived("cfar")
    keep.start(whole, normed_hbm)
    turn(3)
    ready(*cuts[1])
    retain(0)
    relay(*cuts[3])
    retain(1)
    wires.arrived("dy")
    wires.start("dcy", d_ffn.at[2, 0], d_ffn.at[2, 1], "head")
    retain(2)
    relay(*cuts[4])
    retain(3)
    ready(*cuts[2])
    ready(*cuts[3])
    keep.start(stacked, stacked_hbm)
    for n in range(1, 7):
        keep.start(saved[n], saved_hbm[n])
    mix(0)
    mix(1)
    relay(*cuts[5])
    wires.arrived("dfar")
    wires.start("dcfar", d_ffn.at[3, 0], d_ffn.at[3, 1], "head")
    mix(2)
    mix(3)
    keep.start(gates, saved_hbm[0])
    ready(*cuts[4])
    ready(*cuts[5])
    wires.arrived("down", "dcz", "dcy", "dcfar")
    keep.finish()
    wires.finish()


def gather_first(own, other, x, gain, cotangent, domains, key, batch):
    rows, width = x.shape
    lines = batch // 2
    length = 2 * rows
    val = own[1].shape[1]
    high, columns = own[0].shape
    saved = [
        jax.ShapeDtypeStruct((4, length, w), t)
        for w, t in ((val, BF), (val, BF), (128, F32), (val, BF), (key, BF), (key, BF), (length, BF))
    ]
    result = pl.pallas_call(
        functools.partial(gather_kernel, lines=lines),
        out_shape=(
            jax.ShapeDtypeStruct((batch, high, columns), BF),
            jax.ShapeDtypeStruct((batch, high, val), BF),
            jax.ShapeDtypeStruct((4, 2, rows, width), BF),
            jax.ShapeDtypeStruct((4, 2, rows, width), BF),
            jax.ShapeDtypeStruct((4, length, val), BF),
            *saved,
            jax.ShapeDtypeStruct((length, length), F32),
            jax.ShapeDtypeStruct((length, key // 2), F32),
            jax.ShapeDtypeStruct((length, key // 2), F32),
        ),
        in_specs=[anywhere()] * 4 + [vmem()] * 4 + [pl.BlockSpec(memory_space=pltpu.SMEM)] * 2,
        out_specs=(anywhere(), vmem(), anywhere(), anywhere(), vmem()) + tuple([anywhere()] * 10),
        scratch_shapes=[
            pltpu.VMEM((batch, high, columns), BF),
            pltpu.VMEM((4, 2, rows, width), BF),
            pltpu.VMEM((rows, width), BF),
            pltpu.VMEM((rows, width), BF),
            pltpu.VMEM((length, key // 2), F32),
            pltpu.VMEM((length, key // 2), F32),
            pltpu.VMEM((length, length), F32),
            pltpu.VMEM((4, length, val), F32),
        ]
        + [pltpu.VMEM(v.shape, v.dtype) for v in saved]
        + semaphores(6 * 2 * lines + 16)
        + [pltpu.SemaphoreType.DMA((21,))],
        compiler_params=pltpu.CompilerParams(collective_id=2, has_side_effects=True, vmem_limit_bytes=56 * 2**20),
        cost_estimate=pl.CostEstimate(flops=20 * 10**9, bytes_accessed=300000000, transcendentals=0),
        name="gather_first",
    )(*own, *other, x, gain[None], cotangent, *domains)
    stacked, out_t, normed, d_ffn, mixed = result[:5]
    return (
        stacked.reshape(-1, columns),
        out_t.reshape(-1, val),
        normed.reshape(8 * rows, width),
        d_ffn.reshape(8 * rows, width),
        mixed,
        result[5:12],
        result[12:],
    )


def partial_rows(part, rc, wires, rows, weights, s):
    half = part.shape[2]

    def body(i):
        cut = span(i, 512)
        total = dot(rows[...], weights[cut, :], 1, 1)
        part[s, 1, :, cut] = total[half:].astype(BF)
        part[s, 0, :, cut] = total[:half].astype(BF)

    blocks(weights.shape[0] // 512, body)
    send_cores(part, rc, wires, (s,))


def part_sums(part):
    return part.at[:, 0]


def forward_kernel(
    mixed,
    out_t,
    x,
    gain,
    own_up,
    own_down,
    other_up,
    other_down,
    d_ffn,
    whole,
    hidden,
    up,
    down,
    lifted,
    d_pre,
    part,
    rc,
    ra,
    rb,
    ea,
    eb,
    sa,
    sb,
    d_lifted,
    d_rows,
    send,
    recv,
    local,
    *,
    lines,
):
    b = lax.axis_index("batch")
    wires, moves = Wires(send, recv, lines), Moves(local)
    wires.enter(("head", "group", "x") + along(lines))
    order = first_order(lines)
    mine, others, weights = (own_up, own_down), (other_up, other_down), (up, down)
    half, wide = x.shape
    units = lifted.shape[2]

    def pointwise(r, total):
        row = x[r, :].astype(F32) + total
        hidden[r, :] = row
        shifted = row - jnp.mean(row, axis=1, keepdims=True)
        var_row = jnp.mean(shifted * shifted, axis=1, keepdims=True)
        whole[0, 0, r, :] = (shifted * lax.rsqrt(var_row + 1e-05) * gain[...]).astype(BF)

    def piece(i):
        for k in order:
            source = others[i] if k % 2 else mine[i]
            wires.start((i, k), source, weights[i].at[b], ("line", k))

    def relay(i):
        for k in order:
            wires.arrived((i, k))
            block = weights[i].at[b ^ (2 * k)]
            wires.start((i, "x", k), block, block, "x")

    def fetch(s):
        moves.start(d_ffn.at[s], d_rows.at[s % 2])

    def lift_back(s):
        moves.made[2 + s].wait()

        def body(i):
            r = span(i, half)
            d_lifted[s, r, :] = dot(d_rows[s % 2, r, :], down.reshape(wide, units)[...], 1, 0)

        blocks(2, body)
        if s < 2:
            fetch(s + 2)

    def lift(s):
        def body(i):
            r = span(i, half)
            act = dot(whole[s, i], up.reshape(wide, units)[...], 1, 0)
            square = act * act
            turn = jnp.tanh(GELU * act * (1 + 0.044715 * square))
            lifted[s, r, :] = (0.5 * act * (1 + turn)).astype(BF)
            slope = 0.5 * (1 + turn) + 0.5 * act * (1 - turn * turn) * GELU * (1 + 3 * 0.044715 * square)
            d_pre[s, r, :] = (d_lifted[s, r, :] * slope).astype(BF)

        blocks(2, body)

    for i in range(2):
        moves.start(mine[i], weights[i].at[b])
    fetch(0)
    fetch(1)
    piece(1)
    for i in (1, 0):
        wires.start((i, "x", 0), mine[i], weights[i].at[b], "x")
    for s in (3, 1, 2, 0):
        partial_rows(part, rc, wires, mixed.at[s], out_t, s)
    steps = exchange(part, whole, rc, part_sums(part), ra, rb, ea, eb, sa, sb, wires, pointwise)
    next(steps)
    relay(1)
    next(steps)
    piece(0)
    next(steps)
    next(steps)
    moves.made[0].wait()
    moves.made[1].wait()
    wires.arrived(*[(1, "x", k) for k in range(lines)])
    lift_back(0)
    next(steps)
    relay(0)
    lift_back(1)
    next(steps)
    lift_back(2)
    lift_back(3)
    wires.arrived(*[(0, "x", k) for k in range(lines)])
    wires.arrived("own")
    lift(0)
    wires.arrived("fa")
    wires.start("cfa", whole.at[3, 0, pl.ds(0, half // 2)], whole.at[3, 1, pl.ds(0, half // 2)], "head")
    wires.arrived("cza", "czb")
    lift(1)
    wires.arrived("fb")
    wires.start("cfb", whole.at[3, 0, pl.ds(half // 2, half // 2)], whole.at[3, 1, pl.ds(half // 2, half // 2)], "head")
    wires.arrived("cya", "cyb")
    lift(2)
    wires.arrived("cfa", "cfb")
    lift(3)
    wires.finish()


def backward_kernel(
    d_pre,
    up,
    ln_all,
    lifted,
    hidden,
    cotangent,
    gain,
    domains,
    domain_of,
    domain_weight,
    d_ffn,
    whole,
    d_hidden,
    d_gain,
    lines_out,
    part,
    rc,
    ra,
    rb,
    ea,
    eb,
    sa,
    sb,
    grads,
    rx,
    d_cols,
    send,
    recv,
    local,
    *,
    lines,
):
    wires, moves = Wires(send, recv, 2), Moves(local)
    wires.enter(TEAM + ("x",))
    wide, units = up.shape
    step = 256
    tokens = ln_all.shape[0]
    xbit = lax.axis_index("batch") % 2
    flat = grads.reshape(wide, 2 * units)
    d_flat = d_pre.reshape(tokens, units)
    l_flat = lifted.reshape(tokens, units)
    cuts = [pl.ds(0, units), pl.ds(units, units)]
    count = wide // step

    def fetch(i):
        moves.start(d_ffn.at[:, pl.ds(i * step, step)], d_cols.at[i % 2])

    fetch(0)
    fetch(1)
    d_gain[...] = jnp.zeros_like(d_gain)
    share = own_share(domains, domain_of, domain_weight)

    def pointwise(r, total):
        row = hidden[r, :]
        shifted = row - jnp.mean(row, axis=1, keepdims=True)
        var_row = jnp.mean(shifted * shifted, axis=1, keepdims=True)
        rstd = lax.rsqrt(var_row + 1e-05)
        unit = shifted * rstd
        terms = total * unit
        d_gain[...] += terms[:8] + terms[8:]
        d_unit = total * gain[...]
        mean_d = jnp.mean(d_unit, axis=1, keepdims=True)
        mean_du = jnp.mean(d_unit * unit, axis=1, keepdims=True)
        grad = cotangent[r, :].astype(F32) * share + rstd * (d_unit - mean_d - unit * mean_du)
        d_hidden[r, :] = grad
        whole[0, 0, r, :] = grad.astype(BF)

    def up_grads():
        def body(i):
            flat[span(i, step), cuts[0]] = dot(ln_all[:, span(i, step)], d_flat[...], 0, 0).astype(BF)

        blocks(count, body)
        across(wires, grads, rx, cuts[0], lines, "ffn")

    def down_grads():
        for i in range(count):
            moves.made[i].wait()
            flat[pl.ds(i * step, step), cuts[1]] = dot(d_cols[i % 2], l_flat[...], 0, 0).astype(BF)
            if i + 2 < count:
                fetch(i + 2)
        across(wires, grads, rx, cuts[1], lines, "ffn")

    def join(cut):
        for line in range(lines):
            wires.arrived(("ffn", "x", cut.start, line))

            def body(r):
                total = grads[2 * line + xbit, r, cut].astype(F32) + rx[line, r, cut].astype(F32)
                lines_out[line, r, cut] = total.astype(BF)

            tiles(rx.shape[1], body)

    for s in (3, 1, 2, 0):
        partial_rows(part, rc, wires, d_pre.at[s], up, s)
    steps = exchange(part, whole, rc, part_sums(part), ra, rb, ea, eb, sa, sb, wires, pointwise)
    next(steps)
    up_grads()
    next(steps)
    down_grads()
    next(steps)
    next(steps)
    join(cuts[0])
    next(steps)
    next(steps)
    join(cuts[1])
    for _ in steps:
        pass
    half = whole.shape[2] // 2
    for name, end, first in (("fa", "cfa", 0), ("fb", "cfb", half)):
        wires.arrived(name)
        block = pl.ds(first, half)
        wires.start(end, whole.at[3, 0, block], whole.at[3, 1, block], "head")
    wires.arrived("own", "cza", "cyb", "czb", "cya", "cfa", "cfb")
    wires.finish()


def first_order(lines):
    return [k for k in (2, 3, 1) if k < lines] + list(range(4, lines))


class Lines:
    def __init__(self, wires, lined, rz, slices, lines, tag, pick=lambda line: line):
        self.wires, self.lined, self.rz, self.slices, self.lines, self.tag = wires, lined, rz, slices, lines, tag
        self.pick = pick
        self.z = lax.axis_index("batch") // 2
        self.p = self.z % 2
        self.y = lax.axis_index("group")
        self.order = first_order(lines)

    def send(self, cut):
        for k in self.order:
            source = self.lined.at[self.pick(self.z ^ k), :, cut]
            self.wires.start((self.tag, "z", cut.start, k), source, self.rz.at[k, :, cut], ("line", k))

    def join(self, cut):
        lined, rz, slices, p, y = self.lined, self.rz, self.slices, self.p, self.y
        for k in self.order:
            self.wires.arrived((self.tag, "z", cut.start, k))

        def body(r):
            mine = lined[self.pick(self.z), r, cut].astype(F32)
            other = jnp.zeros_like(mine)
            for k in range(1, self.lines):
                term = rz[k, r, cut].astype(F32)
                if k % 2:
                    other = other + term
                else:
                    mine = mine + term
            slices[2 * p + y, r, cut] = mine.astype(BF)
            slices[2 * (1 - p) + y, r, cut] = other.astype(BF)

        tiles(lined.shape[1], body)
        for q in range(2):
            block = slices.at[2 * q + y, :, cut]
            self.wires.start((self.tag, "y", cut.start, q), block, block, "group")

    def store(self, cut, target, first, width, stage, turned=False):
        for q in range(2):
            self.wires.arrived((self.tag, "y", cut.start, q))
        for t in range(4):

            def fill(held):
                def body(r):
                    held[r, pl.ds(0, cut.size)] = self.slices[t, r, cut].astype(F32)

                tiles(target.shape[0], body)

            def fill_turned(held):
                for c in range(0, cut.size, 256):
                    held[pl.ds(c, 256), :] = self.slices[t, :, pl.ds(cut.start + c, 256)].astype(F32).T

            where = pl.ds(t * width + first, cut.size)
            if turned:
                stage.put(fill_turned, target.at[where, :])
            else:
                stage.put(fill, target.at[:, where], cut.size)


class Stage:
    def __init__(self, held, sems):
        self.held, self.sems, self.made = held, sems, []

    def put(self, fill, target, width=None):
        n, ring = len(self.made), self.held.shape[0]
        if n >= ring:
            self.made[n - ring].wait()
        held = self.held.at[n % ring]
        fill(held)
        source = held if width is None else held.at[:, pl.ds(0, width)]
        copy = pltpu.make_async_copy(source, target, self.sems.at[n])
        copy.start()
        self.made.append(copy)

    def finish(self):
        for copy in self.made[-self.held.shape[0] :]:
            copy.wait()


def across(wires, grads, rx, cut, lines, tag):
    other = 1 - lax.axis_index("batch") % 2
    for line in range(lines):
        wires.start((tag, "x", cut.start, line), grads.at[2 * line + other, :, cut], rx.at[line, :, cut], "x")


def across_join(wires, grads, rx, lined, cut, lines, tag, pick=lambda line: line):
    x = lax.axis_index("batch") % 2
    for line in range(lines):
        wires.arrived((tag, "x", cut.start, line))

        def body(r):
            total = grads[2 * line + x, r, cut].astype(F32) + rx[line, r, cut].astype(F32)
            lined[pick(line), r, cut] = total.astype(BF)

        tiles(rx.shape[1], body)


def middle_kernel(
    d_attn,
    w_out,
    mixed,
    gates,
    unit,
    rstd,
    values,
    q_rot,
    k_rot,
    weighted,
    decays,
    cosine,
    sine,
    lifted,
    down,
    hidden,
    ffn_lines,
    d_proj,
    output,
    d_up,
    d_down,
    d_out,
    part,
    rc,
    ry,
    rn,
    rz,
    slices,
    grads,
    rx,
    d_ret,
    d_scores,
    rz_out,
    slices_out,
    held,
    *rest,
    lines,
):
    buffers = rest[:7]
    turned, fetch_sems, stage_sems, turn_sems, send, recv = rest[7:]
    wires = Wires(send, recv, lines)
    stage = Stage(held, stage_sems)
    turner = Stage(turned, turn_sems)
    fetched = {}

    def fetch(s):
        for n, (source, buffer) in enumerate(zip((gates, unit, rstd, values, q_rot, k_rot, weighted), buffers)):
            copy = pltpu.make_async_copy(source.at[s], buffer.at[s % 2], fetch_sems.at[7 * s + n])
            copy.start()
            fetched[s, n] = copy

    fetch(0)
    fetch(1)
    wires.enter(("head", "group", "x") + along(lines))
    length = d_attn.shape[1]
    half = length // 2
    wide = w_out.shape[0]
    val = w_out.shape[1]
    units = lifted.shape[2]
    key = q_rot.shape[2]
    step = 256
    ffn = Lines(wires, ffn_lines, rz, slices, lines, "ffn")
    cuts = [pl.ds(c, units) for c in (0, units)]
    xbit = lax.axis_index("batch") % 2

    def pick(line):
        return 2 * line + xbit

    outs = Lines(wires, grads, rz_out, slices_out, lines, "out", pick)
    out_cut = pl.ds(0, val)

    def partial(s):
        def body(i):
            cut = span(i, 512)
            total = dot(lifted[s], down[cut, :], 1, 1)
            part[s, 1, :, cut] = total[half:].astype(BF)
            part[s, 0, :, cut] = total[:half].astype(BF)

        blocks(wide // 512, body)
        send_cores(part, rc, wires, (s,))

    def pointwise(r, total):
        output[r, :] = (hidden[r, :] + total).astype(BF)

    def retention(s):
        for n in range(7):
            fetched[s, n].wait()
        gates_s, unit_s, rstd_s, values_s, q_s, k_s, weighted_s = [buffer.at[s % 2] for buffer in buffers]

        def mix(i):
            r = span(i, half)
            d_mixed = dot(d_attn[s, r, :], w_out[...], 1, 0)
            gate = gates_s[r, :].astype(F32)
            sig = jax.nn.sigmoid(gate)
            norm = unit_s[r, :].astype(F32)
            d_gate = d_mixed * norm * (sig * (1 + gate * (1 - sig)))
            d_proj[s, r, pl.ds(2 * key + val, val)] = d_gate.astype(BF)
            d_norm = d_mixed * (gate * sig)
            mean_d = jnp.mean(d_norm, axis=1, keepdims=True)
            mean_dn = jnp.mean(d_norm * norm, axis=1, keepdims=True)
            d_ret[r, :] = (rstd_s[r, :][:, :1] * (d_norm - mean_d - norm * mean_dn)).astype(BF)

        blocks(2, mix)
        d_proj[s, :, pl.ds(2 * key, val)] = dot(weighted_s[...], d_ret[...], 0, 0).astype(BF)
        d_scores[...] = (dot(d_ret[...], values_s[...], 1, 1) * decays[...]).astype(BF)

        def turn(grad, first):
            a, b = grad[:, : key // 2], grad[:, key // 2 :]
            d_proj[s, :, pl.ds(first, key // 2)] = (a * cosine[...] + b * sine[...]).astype(BF)
            d_proj[s, :, pl.ds(first + key // 2, key // 2)] = (b * cosine[...] - a * sine[...]).astype(BF)

        turn(dot(d_scores[...], k_s[...], 1, 0), 0)
        turn(dot(d_scores[...], q_s[...], 0, 0), key)
        if s < 2:
            fetch(s + 2)

    def out_grads():
        flat = grads.reshape(wide, val)

        def body(i):
            total = jnp.zeros((step, val), F32)
            for s in range(4):
                total = total + dot(d_attn[s, :, span(i, step)], mixed[s], 0, 0)
            flat[span(i, step), :] = total.astype(BF)

        blocks(wide // step, body)
        across(wires, grads, rx, pl.ds(0, val), lines, "out")

    steps = reduce_rows(part, rc, ry, rn, wires, pointwise)
    ffn.send(cuts[0])
    ffn.send(cuts[1])
    partial(3)
    partial(2)
    next(steps)
    out_grads()
    partial(1)
    next(steps)
    partial(0)
    next(steps)
    retention(0)
    next(steps)
    retention(1)
    across_join(wires, grads, rx, grads, out_cut, lines, "out", pick)
    outs.send(out_cut)
    retention(2)
    ffn.join(cuts[0])
    ffn.join(cuts[1])
    retention(3)
    for _ in steps:
        pass
    ffn.store(cuts[0], d_up, 0, units, stage)
    ffn.store(cuts[1], d_down, 0, units, turner, True)
    outs.join(out_cut)
    outs.store(out_cut, d_out, 0, val, turner, True)
    stage.finish()
    turner.finish()
    wires.finish()


def last_kernel(
    d_proj,
    x,
    d_hidden,
    gain,
    ln_gains,
    normed_hbm,
    stacked_hbm,
    d_inputs,
    gains,
    d_query,
    d_key,
    d_value,
    d_gate,
    normed,
    stacked,
    grads,
    part,
    rc,
    ry,
    rn,
    rx,
    rz,
    slices,
    held,
    came,
    staged,
    local,
    stage_sems,
    send,
    recv,
    *,
    lines,
):
    wires, moves = Wires(send, recv, lines), Moves(local)
    wide, columns = stacked.shape
    tokens = normed.shape[0]
    step = 256
    val = d_value.shape[1] // 4
    key = d_query.shape[1] // 4
    for i in range(wide // step):
        cut = pl.ds(i * step, step)
        moves.start(normed_hbm.at[:, cut], normed.at[:, cut])
    moves.start(stacked_hbm, stacked)
    wires.enter(("head", "group", "x") + along(lines))
    xbit = lax.axis_index("batch") % 2
    stage = Stage(staged, stage_sems)

    def pick(line):
        return 2 * line + xbit

    main = Lines(wires, grads, rz, slices, lines, "main", pick)
    cuts = [pl.ds(c, 256) for c in (2 * key + val, 2 * key + val + 256, 2 * key, 2 * key + 256, 0, key)]
    flat = grads.reshape(wide, columns)
    held[0] = jnp.zeros_like(held[0])
    rows_all = d_proj.reshape(tokens, columns)

    def pointwise(r, total):
        row = x[r, :].astype(F32)
        scale = lax.rsqrt(jnp.mean(row * row, axis=1, keepdims=True) + 1e-06)
        unit = row * scale
        terms = total * unit
        held[0, :8] += terms[:8] + terms[8:]
        d_unit = total * gain[...]
        mean_du = jnp.mean(d_unit * unit, axis=1, keepdims=True)
        d_inputs[r, :] = (d_hidden[r, :] + scale * (d_unit - unit * mean_du)).astype(BF)

    def weight_grads(first, wait=False):
        cut = pl.ds(first, 512)

        def body(i):
            flat[span(i, step), cut] = dot(normed[:, span(i, step)], rows_all[:, cut], 0, 0).astype(BF)

        if wait:
            for i in range(wide // step):
                moves.made[i].wait()
                body(i)
        else:
            blocks(wide // step, body)
        for c in (first, first + 256):
            across(wires, grads, rx, pl.ds(c, 256), lines, "main")

    def partial(s):
        rows = d_proj.shape[1] // 2

        def body(i):
            cut = span(i, 512)
            total = dot(d_proj[s], stacked[cut, :], 1, 1)
            part[s, 1, :, cut] = total[rows:].astype(BF)
            part[s, 0, :, cut] = total[:rows].astype(BF)

        blocks(wide // 512, body)
        send_cores(part, rc, wires, (s,))

    def stage_x(at):
        across_join(wires, grads, rx, grads, cuts[at], lines, "main", pick)
        main.send(cuts[at])

    hops = ["head", "group", "x"]
    bit = 1
    while bit < lines:
        hops.append(("line", bit))
        bit *= 2

    def hop(at):
        if at:
            wires.arrived(("gain", at - 1))
            held[at] = held[at - 1] + came[at - 1]
        else:
            held[0, 8:] = ln_gains[...]
        if at < len(hops):
            wires.start(("gain", at), held.at[at], came.at[at], hops[at])
        else:
            gains[...] = held[at]

    targets = [(d_gate, val, 0), (d_gate, val, 256), (d_value, val, 0), (d_value, val, 256), (d_query, key, 0), (d_key, key, 0)]

    def store(at):
        target, width, first = targets[at]
        main.store(cuts[at], target, first, width, stage)

    steps = reduce_rows(part, rc, ry, rn, wires, pointwise)
    weight_grads(2 * key + val, True)
    moves.made[-1].wait()
    partial(3)
    partial(2)
    next(steps)
    weight_grads(2 * key)
    next(steps)
    stage_x(0)
    partial(1)
    weight_grads(0)
    next(steps)
    stage_x(1)
    partial(0)
    next(steps)
    stage_x(2)
    main.join(cuts[0])
    stage_x(3)
    main.join(cuts[1])
    stage_x(4)
    stage_x(5)
    main.join(cuts[2])
    for _ in steps:
        pass
    hop(0)
    main.join(cuts[3])
    hop(1)
    store(0)
    store(1)
    hop(2)
    store(2)
    main.join(cuts[4])
    hop(3)
    store(3)
    hop(4)
    main.join(cuts[5])
    store(4)
    store(5)
    for at in range(5, len(hops) + 1):
        hop(at)
    stage.finish()
    wires.finish()


def exchange_scratch(rows, width):
    half = rows // 2
    return [
        pltpu.VMEM((4, 2, rows, width), BF),
        pltpu.VMEM((4, rows, width), BF),
        pltpu.VMEM((2, half, width), BF),
        pltpu.VMEM((2, half, width), BF),
        pltpu.VMEM((half, width), BF),
        pltpu.VMEM((half, width), BF),
        pltpu.VMEM((half, width), BF),
        pltpu.VMEM((half, width), BF),
    ]


def lean_scratch(rows, width):
    return [
        pltpu.VMEM((4, 2, rows, width), BF),
        pltpu.VMEM((4, rows, width), BF),
        pltpu.VMEM((2, rows, width), BF),
        pltpu.VMEM((rows, width), BF),
    ]


def semaphores(count):
    return [pltpu.SemaphoreType.DMA((count,)), pltpu.SemaphoreType.DMA((count,))]


def anywhere():
    return pl.BlockSpec(memory_space=pl.ANY)


def vmem():
    return pl.BlockSpec(memory_space=pltpu.VMEM)


def forward_exchange(mixed, out_t, x, gain, own, other, d_ffn, batch):
    rows, width = x.shape
    lines = batch // 2
    high, units = own[0].shape
    length = 2 * rows
    whole, hidden, up, down, lifted, d_pre = pl.pallas_call(
        functools.partial(forward_kernel, lines=lines),
        out_shape=(
            jax.ShapeDtypeStruct((4, 2, rows, width), BF),
            jax.ShapeDtypeStruct((rows, width), F32),
            jax.ShapeDtypeStruct((batch, high, units), BF),
            jax.ShapeDtypeStruct((batch, high, units), BF),
            jax.ShapeDtypeStruct((4, length, units), BF),
            jax.ShapeDtypeStruct((4, length, units), BF),
        ),
        in_specs=[vmem()] * 8 + [anywhere()],
        out_specs=tuple([vmem()] * 6),
        scratch_shapes=exchange_scratch(rows, width)
        + [pltpu.VMEM((4, length, units), F32), pltpu.VMEM((2, length, width), BF)]
        + semaphores(24 + 4 * lines)
        + [pltpu.SemaphoreType.DMA((6,))],
        compiler_params=pltpu.CompilerParams(collective_id=0, has_side_effects=True, vmem_limit_bytes=58 * 2**20),
        cost_estimate=pl.CostEstimate(flops=12 * 10**9, bytes_accessed=300000000, transcendentals=0),
        name="forward_exchange",
    )(mixed, out_t, x, gain[None], *own, *other, d_ffn.reshape(4, length, width))
    return whole.reshape(8 * rows, width), hidden, up.reshape(width, -1), down.reshape(width, -1), lifted, d_pre


def backward_exchange(d_pre, up, ln_all, lifted, hidden, cotangent, gain, domains, d_ffn, batch):
    rows, width = hidden.shape
    lines = batch // 2
    block = (width // batch, 2 * up.shape[1])
    whole, d_hidden, d_gain, lined = pl.pallas_call(
        functools.partial(backward_kernel, lines=lines),
        out_shape=(
            jax.ShapeDtypeStruct((4, 2, rows, width), BF),
            jax.ShapeDtypeStruct((rows, width), F32),
            jax.ShapeDtypeStruct((8, width), F32),
            jax.ShapeDtypeStruct((lines,) + block, BF),
        ),
        in_specs=[vmem()] * 8 + [pl.BlockSpec(memory_space=pltpu.SMEM)] * 2 + [anywhere()],
        out_specs=(vmem(), vmem(), vmem(), vmem()),
        scratch_shapes=exchange_scratch(rows, width)
        + [
            pltpu.VMEM((batch,) + block, BF),
            pltpu.VMEM((lines,) + block, BF),
            pltpu.VMEM((2, 8 * rows, 256), BF),
        ]
        + semaphores(24 + 2 * lines)
        + [pltpu.SemaphoreType.DMA((width // 256,))],
        compiler_params=pltpu.CompilerParams(collective_id=1, has_side_effects=True, vmem_limit_bytes=63 * 2**20),
        cost_estimate=pl.CostEstimate(flops=14 * 10**9, bytes_accessed=300000000, transcendentals=0),
        name="backward_exchange",
    )(d_pre, up, ln_all, lifted, hidden, cotangent, gain[None], *domains, d_ffn)
    return whole.reshape(8 * rows, width), d_hidden, d_gain, lined


def middle_exchange(d_attn, w_out, mixed, saved, tables, lifted, down, hidden, ffn_lines, batch):
    rows, width = hidden.shape
    lines = batch // 2
    length = 2 * rows
    block = ffn_lines.shape[1:]
    val = w_out.shape[1]
    units = lifted.shape[2]
    gates, unit, rstd, values, q_rot, k_rot, weighted = saved
    columns = 2 * q_rot.shape[2] + 2 * val
    return pl.pallas_call(
        functools.partial(middle_kernel, lines=lines),
        out_shape=(
            jax.ShapeDtypeStruct((4, length, columns), BF),
            jax.ShapeDtypeStruct((rows, width), BF),
            jax.ShapeDtypeStruct((block[0], 4 * units), F32),
            jax.ShapeDtypeStruct((4 * units, block[0]), F32),
            jax.ShapeDtypeStruct((4 * val, block[0]), F32),
        ),
        in_specs=[vmem()] * 3 + [anywhere()] * 7 + [vmem()] * 7,
        out_specs=(vmem(), vmem(), anywhere(), anywhere(), anywhere()),
        scratch_shapes=lean_scratch(rows, width)
        + [
            pltpu.VMEM((lines,) + block, BF),
            pltpu.VMEM((4,) + block, BF),
            pltpu.VMEM((batch, block[0], val), BF),
            pltpu.VMEM((lines, block[0], val), BF),
            pltpu.VMEM((length, val), BF),
            pltpu.VMEM((length, length), BF),
            pltpu.VMEM((lines, block[0], val), BF),
            pltpu.VMEM((4, block[0], val), BF),
            pltpu.VMEM((2, block[0], units), F32),
        ]
        + [pltpu.VMEM((2,) + v.shape[1:], v.dtype) for v in saved]
        + [pltpu.VMEM((2, units, block[0]), F32)]
        + [pltpu.SemaphoreType.DMA((28,)), pltpu.SemaphoreType.DMA((4,)), pltpu.SemaphoreType.DMA((8,))]
        + semaphores(16 + 3 * (lines + 1) + lines),
        compiler_params=pltpu.CompilerParams(collective_id=4, has_side_effects=True, vmem_limit_bytes=63 * 2**20),
        cost_estimate=pl.CostEstimate(flops=20 * 10**9, bytes_accessed=200000000, transcendentals=0),
        name="middle_exchange",
    )(
        d_attn.reshape(4, length, width),
        w_out,
        mixed,
        gates,
        unit,
        rstd,
        values,
        q_rot,
        k_rot,
        weighted,
        *tables,
        lifted,
        down,
        hidden,
        ffn_lines,
    )


def last_exchange(d_proj, x, d_hidden, gain, ln_gains, normed, stacked, key, batch):
    rows, width = x.shape
    lines = batch // 2
    high = width // batch
    columns = stacked.shape[1]
    val = (columns - 2 * key) // 2
    steps = 2 + batch.bit_length() - 1
    return pl.pallas_call(
        functools.partial(last_kernel, lines=lines),
        out_shape=(
            jax.ShapeDtypeStruct((rows, width), BF),
            jax.ShapeDtypeStruct((16, width), F32),
            jax.ShapeDtypeStruct((high, 4 * key), F32),
            jax.ShapeDtypeStruct((high, 4 * key), F32),
            jax.ShapeDtypeStruct((high, 4 * val), F32),
            jax.ShapeDtypeStruct((high, 4 * val), F32),
        ),
        in_specs=[vmem()] * 5 + [anywhere()] * 2,
        out_specs=(vmem(), vmem()) + tuple([anywhere()] * 4),
        scratch_shapes=[
            pltpu.VMEM(normed.shape, BF),
            pltpu.VMEM(stacked.shape, BF),
            pltpu.VMEM((batch, high, columns), BF),
        ]
        + lean_scratch(rows, width)
        + [
            pltpu.VMEM((lines, high, columns), BF),
            pltpu.VMEM((lines, high, columns), BF),
            pltpu.VMEM((4, high, columns), BF),
            pltpu.VMEM((steps + 1, 16, width), F32),
            pltpu.VMEM((steps, 16, width), F32),
            pltpu.VMEM((2, high, val), F32),
            pltpu.SemaphoreType.DMA((width // 256 + 1,)),
            pltpu.SemaphoreType.DMA((4 * (columns // 256),)),
        ]
        + semaphores(16 + steps + (columns // 256) * (2 * lines + 1)),
        compiler_params=pltpu.CompilerParams(collective_id=3, has_side_effects=True, vmem_limit_bytes=63 * 2**20),
        cost_estimate=pl.CostEstimate(flops=26 * 10**9, bytes_accessed=300000000, transcendentals=0),
        name="last_exchange",
    )(d_proj, x, d_hidden, gain[None], ln_gains, normed, stacked)


class Place:
    def __init__(self):
        self.batch = lax.axis_size("batch")
        self.b = lax.axis_index("batch")
        self.y = lax.axis_index("group")
        self.c = lax.axis_index("head")
        self.lines = self.batch // 2
        self.z = self.b // 2
        self.x = self.b % 2
        self.p = self.z % 2
        self.slot = 2 * self.p + self.y

    def cut(self, array, axis):
        width = array.shape[axis] // 4
        own = lax.dynamic_slice_in_dim(array, self.slot * width, width, axis)
        other = lax.dynamic_slice_in_dim(array, (self.slot ^ 2) * width, width, axis)
        return own, other

def on_device(
    inputs,
    rms_gain,
    w_query,
    w_key,
    w_value,
    w_gate,
    w_out,
    ln_gain,
    w_up,
    w_down,
    cotangent,
    domain_of,
    domain_weight,
):
    here = Place()

    parts = [here.cut(w, 1) for w in (w_query, w_key, w_value, w_gate)]
    own = jnp.concatenate([own for own, _ in parts], axis=1)
    other = jnp.concatenate([other for _, other in parts], axis=1)
    out_own, out_other = [v.T for v in here.cut(w_out, 0)]
    domains = (domain_of[None], domain_of, domain_weight)
    stacked, out_t, normed_all, d_ffn_all, mixed, saved, tables = gather_first(
        (own, out_own), (other, out_other), inputs[0], rms_gain, cotangent[0], domains, KEY, here.batch
    )
    up_parts = here.cut(w_up, 1)
    down_parts = [v.T for v in here.cut(w_down, 0)]
    ln_all, hidden, up, down_t, lifted, d_pre = forward_exchange(
        mixed,
        out_t,
        inputs[0],
        ln_gain,
        (up_parts[0], down_parts[0]),
        (up_parts[1], down_parts[1]),
        d_ffn_all,
        here.batch,
    )
    d_attn_all, d_hidden, d_ln_gain, ffn_lines = backward_exchange(
        d_pre, up, ln_all, lifted, hidden, cotangent[0], ln_gain, domains, d_ffn_all, here.batch
    )
    d_proj, output, d_up, d_down, d_w_out = middle_exchange(
        d_attn_all,
        out_t,
        mixed,
        saved,
        tables,
        lifted,
        down_t,
        hidden,
        ffn_lines,
        here.batch,
    )
    d_inputs, gains, d_query, d_key, d_value, d_gate = last_exchange(
        d_proj, inputs[0], d_hidden, rms_gain, d_ln_gain, normed_all, stacked, KEY, here.batch
    )
    gain_rms = jnp.sum(gains[:8], axis=0)
    gain_ln = jnp.sum(gains[8:], axis=0)
    return (
        output[None],
        d_inputs[None],
        gain_rms,
        d_query,
        d_key,
        d_value,
        d_gate,
        d_w_out,
        gain_ln,
        d_up,
        d_down,
    )


def solution(mesh):
    rows = P(("batch", "group"), "head", None)
    wide = P("batch", "head")
    tall = P("head", "batch")
    return jax.shard_map(
        on_device,
        mesh=mesh,
        in_specs=(rows, P(), wide, wide, wide, wide, tall, P(), wide, tall, rows, P(), P()),
        out_specs=(rows, rows, P(), wide, wide, wide, wide, tall, P(), wide, tall),
        check_vma=False,
    )
```

```python
import functools

import jax
import jax.numpy as jnp
import numpy as np
from jax import lax
from jax.experimental import pallas as pl
from jax.experimental.pallas import tpu as pltpu
from jax.sharding import PartitionSpec as P


KEY = 256
VAL = 512
GELU = 0.7978845608028654
BF = jnp.bfloat16
F32 = jnp.float32


def own_share(domains, domain_of, domain_weight):
    me = domain_of[lax.axis_index("batch") * lax.axis_size("group") + lax.axis_index("group")]
    row = domains[...]
    total = count = weight = jnp.zeros((1, 1), F32)
    for d in range(domain_weight.shape[0]):
        n = jnp.sum((row == d).astype(F32), axis=1, keepdims=True)
        w = domain_weight[d].astype(F32)
        total = total + jnp.where(n > 0, n * (w / jnp.maximum(n, 1.0)), 0.0)
        count = count + jnp.where(me == d, n, 0.0)
        weight = weight + jnp.where(me == d, w, 0.0)
    return jnp.float32(domains.shape[1]) * weight / (count * total)


TEAM = ("head", "batch", "group")


def peers(lines):
    b = lax.axis_index("batch")
    table = {
        "head": {"head": 1 - lax.axis_index("head")},
        "batch": {"batch": b ^ 2},
        "group": {"group": 1 - lax.axis_index("group")},
        "x": {"batch": b ^ 1},
    }
    for k in range(1, lines):
        table["line", k] = {"batch": b ^ (2 * k)}
    return table


def along(lines):
    return tuple(("line", k) for k in range(1, lines))


class Wires:
    def __init__(self, send, recv, lines=1):
        self.send, self.recv, self.made, self.peers = send, recv, {}, peers(lines)

    def enter(self, names):
        barrier = pltpu.get_barrier_semaphore()
        for name in names:
            pl.semaphore_signal(barrier, inc=1, device_id=self.peers[name], device_id_type=pl.DeviceIdType.MESH)
        pl.semaphore_wait(barrier, len(names))

    def start(self, name, source, target, peer, go=True):
        n = len(self.made)
        copy = pltpu.make_async_remote_copy(
            src_ref=source,
            dst_ref=target,
            send_sem=self.send.at[n],
            recv_sem=self.recv.at[n],
            device_id=self.peers[peer],
            device_id_type=pl.DeviceIdType.MESH,
        )
        if go:
            copy.start()
        self.made[name] = copy

    def plan(self, *copy):
        self.start(*copy, go=False)

    def go(self, names):
        for name in names:
            self.made[name].start()

    def arrived(self, *names):
        for name in names:
            self.made[name].wait_recv()

    def finish(self):
        for copy in self.made.values():
            copy.wait_send()


class Moves:
    def __init__(self, sems):
        self.sems, self.made = sems, []

    def start(self, source, target):
        copy = pltpu.make_async_copy(source, target, self.sems.at[len(self.made)])
        copy.start()
        self.made.append(copy)

    def finish(self):
        for copy in self.made:
            copy.wait()


TILE = 16


def tiles(rows, body):
    def step(i, _):
        body(pl.ds(pl.multiple_of(i * TILE, TILE), TILE))
        return 0

    lax.fori_loop(0, rows // TILE, step, 0)


def exchange(part, whole, rc, sums, ra, rb, ea, eb, sa, sb, wires, pointwise, tag=""):
    rows = part.shape[2]
    half = rows // 2
    top, low = pl.ds(0, half), pl.ds(half, half)

    def start(name, *rest):
        wires.start(tag + name, *rest)

    def arrived(*names):
        wires.arrived(*[tag + name for name in names])

    def add(s, first):
        def body(r):
            rr = pl.ds(r.start + first, TILE)
            total = part[s, 0, rr, :].astype(F32) + rc[s, rr, :].astype(F32)
            sums[s, rr, :] = total.astype(BF)

        tiles(half, body)

    arrived("c3")
    add(3, 0)
    start("a3", sums.at[3, top], ra.at[0], "batch")
    add(3, half)
    start("b3", sums.at[3, low], rb.at[0], "group")
    arrived("c1")
    add(1, 0)
    start("a1", sums.at[1, top], ra.at[1], "batch")
    arrived("c2")
    add(2, half)
    start("b2", sums.at[2, low], rb.at[1], "group")
    add(2, 0)
    add(1, half)

    def second_a(r):
        sa[r, :] = (sums[2, r, :].astype(F32) + ra[0, r, :].astype(F32)).astype(BF)

    def second_b(r):
        rr = pl.ds(r.start + half, TILE)
        sb[r, :] = (sums[1, rr, :].astype(F32) + rb[0, r, :].astype(F32)).astype(BF)

    yield
    arrived("a3")
    tiles(half, second_a)
    start("a2", sa, ea, "group")
    arrived("b3")
    tiles(half, second_b)
    start("b1", sb, eb, "batch")

    def last(first, near, end):
        def body(r):
            rr = pl.ds(r.start + first, TILE)
            total = part[0, 0, rr, :].astype(F32) + rc[0, rr, :].astype(F32)
            total = total + near[1, r, :].astype(F32) + end[r, :].astype(F32)
            pointwise(rr, total)

        tiles(half, body)

    yield
    arrived("c0", "a1", "a2")
    last(0, ra, ea)
    if whole is not None:
        start("za", whole.at[0, 0, top], whole.at[1, 0, top], "batch")
    yield
    arrived("b2", "b1")
    last(half, rb, eb)
    if whole is None:
        return
    start("yb", whole.at[0, 0, low], whole.at[2, 0, low], "group")
    start("zb", whole.at[0, 0, low], whole.at[1, 0, low], "batch")
    start("ya", whole.at[0, 0, top], whole.at[2, 0, top], "group")
    start("own", whole.at[0, 0], whole.at[0, 1], "head")
    yield
    arrived("za")
    start("fa", whole.at[1, 0, top], whole.at[3, 0, top], "group")
    start("cza", whole.at[1, 0, top], whole.at[1, 1, top], "head")
    arrived("yb")
    start("fb", whole.at[2, 0, low], whole.at[3, 0, low], "batch")
    start("cyb", whole.at[2, 0, low], whole.at[2, 1, low], "head")
    yield
    arrived("zb")
    start("czb", whole.at[1, 0, low], whole.at[1, 1, low], "head")
    arrived("ya")
    start("cya", whole.at[2, 0, top], whole.at[2, 1, top], "head")
    yield


def reduce_rows(part, rc, ry, rn, wires, pointwise, tag=""):
    rows = part.shape[2]
    half = rows // 2
    ends = [pl.ds(0, half), pl.ds(half, half)]

    def add(s, end):
        def body(r):
            rr = pl.ds(r.start + end.start, TILE)
            total = part[s, 0, rr, :].astype(F32) + rc[s, rr, :].astype(F32)
            part[s, 0, rr, :] = total.astype(BF)

        tiles(half, body)

    for s, at in ((3, 0), (2, 1)):
        wires.arrived(f"{tag}c{s}")
        for h, end in enumerate(ends):
            add(s, end)
            wires.start((tag, s, h), part.at[s, 0, end], ry.at[at, end], "group")
        yield
    wires.arrived(f"{tag}c1")
    for end in ends:
        add(1, end)
    yield
    for h, end in enumerate(ends):
        wires.arrived((tag, 3, h))

        def body(r):
            rr = pl.ds(r.start + end.start, TILE)
            total = part[1, 0, rr, :].astype(F32) + ry[0, rr, :].astype(F32)
            part[1, 0, rr, :] = total.astype(BF)

        tiles(half, body)
        wires.start((tag, 1, h), part.at[1, 0, end], rn.at[end], "batch")
    yield
    wires.arrived(f"{tag}c0")
    for h, end in enumerate(ends):
        wires.arrived((tag, 2, h), (tag, 1, h))

        def last(r):
            rr = pl.ds(r.start + end.start, TILE)
            total = part[0, 0, rr, :].astype(F32) + rc[0, rr, :].astype(F32)
            pointwise(rr, total + ry[1, rr, :].astype(F32) + rn[rr, :].astype(F32))

        tiles(half, last)


def send_cores(part, rc, wires, slots=(3, 1, 2, 0), tag=""):
    for s in slots:
        wires.start(tag + f"c{s}", part.at[s, 1], rc.at[s], "head")


def dot(left, right, left_dim, right_dim):
    return lax.dot_general(left, right, (((left_dim,), (right_dim,)), ((), ())), preferred_element_type=F32)


def blocks(count, body):
    def step(i, _):
        body(i)
        return 0

    lax.fori_loop(0, count, step, 0)


def span(i, size):
    return pl.ds(pl.multiple_of(i * size, size), size)


def gather_kernel(
    own,
    own_out,
    other,
    other_out,
    x,
    gain,
    cotangent,
    domains,
    domain_of,
    domain_weight,
    stacked_hbm,
    out_t,
    normed_hbm,
    d_ffn,
    mixed,
    *rest,
    lines,
):
    saved_hbm, tables_hbm, rest = rest[:7], rest[7:10], rest[10:]
    stacked, whole, normed, d_rows, cosine, sine, decays, unit_full = rest[:8]
    saved, (send, recv, local) = rest[8:15], rest[15:]
    gates, unit, rstd, values, q_rot, k_rot, weighted = saved
    b, c = lax.axis_index("batch"), lax.axis_index("head")
    slot = 2 * ((b // 2) % 2) + lax.axis_index("group")
    wires, moves = Wires(send, recv, lines), Moves(local)
    wires.enter(("head", "group", "x") + along(lines))
    order = first_order(lines)
    half, wide = x.shape
    length = 2 * half
    key, val = q_rot.shape[2], values.shape[2]
    cuts = [(0, pl.ds(0, 512)), (0, pl.ds(512, 512)), (0, pl.ds(1024, 256)), (0, pl.ds(1280, 256))]
    cuts += [(1, pl.ds(0, 256)), (1, pl.ds(256, 256))]
    mine, others, weights = (own, own_out), (other, other_out), (stacked, out_t)

    def piece(i, cut):
        for k in order:
            source = others[i] if k % 2 else mine[i]
            wires.plan((i, cut.start, k), source.at[:, cut], weights[i].at[b, :, cut], ("line", k))
        wires.start((i, cut.start, "x", 0), mine[i].at[:, cut], weights[i].at[b, :, cut], "x")

    def relay(i, cut):
        for k in order:
            wires.arrived((i, cut.start, k))
            block = weights[i].at[b ^ (2 * k), :, cut]
            wires.start((i, cut.start, "x", k), block, block, "x")

    def ready(i, cut):
        wires.arrived(*[(i, cut.start, "x", k) for k in range(lines)])

    share = own_share(domains, domain_of, domain_weight)

    def body(r):
        row = x[r, :].astype(F32)
        scale = lax.rsqrt(jnp.mean(row * row, axis=1, keepdims=True) + 1e-06)
        normed[r, :] = (row * scale * gain[...]).astype(BF)
        d_rows[r, :] = (cotangent[r, :].astype(F32) * share).astype(BF)

    tiles(half, body)
    wires.start("y", normed, whole.at[2, 0], "group")
    wires.start("own", normed, whole.at[0, 1], "head")
    wires.plan("z", normed, whole.at[1, 0], ("line", 1))
    wires.plan("dz", d_rows, d_ffn.at[1, 0], ("line", 1))
    for cut in cuts:
        piece(*cut)
    near_first = sorted(order)

    def names(cuts_now, ks):
        return [(i, cut.start, k) for i, cut in cuts_now for k in ks]

    @pl.when(c == 0)
    def _():
        wires.go(["z"] + names(cuts[:1], near_first) + ["dz"] + names(cuts[1:], near_first))

    @pl.when(c == 1)
    def _():
        wires.go(names(cuts[:1], order) + ["z"] + names(cuts[1:2], order) + ["dz"] + names(cuts[2:], order))

    moves.start(normed, whole.at[0, 0])
    for i in range(2):
        moves.start(mine[i], weights[i].at[b])
    wires.start("dy", d_rows, d_ffn.at[2, 0], "group")
    wires.start("down", d_rows, d_ffn.at[0, 1], "head")
    moves.start(d_rows, d_ffn.at[0, 0])

    lane = lax.broadcasted_iota(jnp.int32, (half, key // 2), 1).astype(F32)
    freqs = jnp.exp(lane * jnp.float32(-np.log(10000.0) / (key // 2 - 1)))
    for h in range(2):
        first = (h * half + c * half) % length
        places = (lax.broadcasted_iota(jnp.int32, (half, key // 2), 0) + first).astype(F32)
        cosine[pl.ds(h * half, half), :] = jnp.cos(places * freqs)
        sine[pl.ds(h * half, half), :] = jnp.sin(places * freqs)
    head = 4 * c + slot
    log_keep = jnp.float32(0)
    for h in range(8):
        log_keep = jnp.where(head == h, jnp.float32(np.log1p(-(2.0 ** (-5 - h)))), log_keep)

    def decay_rows(r):
        n = lax.broadcasted_iota(jnp.int32, (TILE, length), 0) + r.start
        m = lax.broadcasted_iota(jnp.int32, (TILE, length), 1)
        offset = (n + c * half) % length - (m + c * half) % length
        steps = jnp.maximum(offset, 0).astype(F32)
        decays[r, :] = jnp.where(offset >= 0, jnp.exp(steps * log_keep), jnp.float32(0))

    tiles(length, decay_rows)

    rows = whole.reshape(4, length, wide)
    flat = stacked.reshape(wide, stacked.shape[2])

    def turn(s):
        total = dot(rows[s], flat[:, pl.ds(0, 2 * key)], 1, 0)
        for target, at in ((q_rot, 0), (k_rot, key)):
            a, b_ = total[:, at : at + key // 2], total[:, at + key // 2 : at + key]
            target[s, :, pl.ds(0, key // 2)] = (a * cosine[...] - b_ * sine[...]).astype(BF)
            target[s, :, pl.ds(key // 2, key // 2)] = (b_ * cosine[...] + a * sine[...]).astype(BF)

    def retain(s):
        values[s] = dot(rows[s], flat[:, pl.ds(2 * key, val)], 1, 0).astype(BF)
        weighted[s] = (dot(q_rot[s], k_rot[s], 1, 1) * decays[...]).astype(BF)

        def part(i):
            r = span(i, half)
            retained = dot(weighted[s, r, :], values[s], 1, 0)
            centered = retained - jnp.mean(retained, axis=1, keepdims=True)
            scale = lax.rsqrt(jnp.mean(centered * centered, axis=1, keepdims=True) + 1e-05)
            full = centered * scale
            unit_full[s, r, :] = full
            unit[s, r, :] = full.astype(BF)
            rstd[s, r, :] = jnp.broadcast_to(scale, (half, rstd.shape[2]))

        blocks(2, part)

    def mix(s):
        def part(i):
            r = span(i, half)
            gate = dot(rows[s, r, :], flat[:, pl.ds(2 * key + val, val)], 1, 0)
            gates[s, r, :] = gate.astype(BF)
            mixed[s, r, :] = (unit_full[s, r, :] * (gate * jax.nn.sigmoid(gate))).astype(BF)

        blocks(2, part)

    wires.arrived("z")
    wires.start("far", whole.at[1, 0], whole.at[3, 0], "group")
    wires.start("cz", whole.at[1, 0], whole.at[1, 1], "head")
    wires.arrived("y")
    wires.start("cy", whole.at[2, 0], whole.at[2, 1], "head")
    relay(*cuts[0])
    wires.arrived("far")
    wires.start("cfar", whole.at[3, 0], whole.at[3, 1], "head")
    moves.finish()
    wires.arrived("own", "cz", "cy")
    ready(*cuts[0])
    keep = Moves(local.at[pl.ds(8, 13)])
    keep.start(decays, tables_hbm[0])
    keep.start(cosine, tables_hbm[1])
    keep.start(sine, tables_hbm[2])
    turn(0)
    turn(1)
    turn(2)
    relay(*cuts[1])
    wires.arrived("dz")
    wires.start("dfar", d_ffn.at[1, 0], d_ffn.at[3, 0], "group")
    wires.start("dcz", d_ffn.at[1, 0], d_ffn.at[1, 1], "head")
    relay(*cuts[2])
    wires.arrived("cfar")
    keep.start(whole, normed_hbm)
    turn(3)
    ready(*cuts[1])
    retain(0)
    relay(*cuts[3])
    retain(1)
    wires.arrived("dy")
    wires.start("dcy", d_ffn.at[2, 0], d_ffn.at[2, 1], "head")
    retain(2)
    relay(*cuts[4])
    retain(3)
    ready(*cuts[2])
    ready(*cuts[3])
    keep.start(stacked, stacked_hbm)
    for n in range(1, 7):
        keep.start(saved[n], saved_hbm[n])
    mix(0)
    mix(1)
    relay(*cuts[5])
    wires.arrived("dfar")
    wires.start("dcfar", d_ffn.at[3, 0], d_ffn.at[3, 1], "head")
    mix(2)
    mix(3)
    keep.start(gates, saved_hbm[0])
    ready(*cuts[4])
    ready(*cuts[5])
    wires.arrived("down", "dcz", "dcy", "dcfar")
    keep.finish()
    wires.finish()


def gather_first(own, other, x, gain, cotangent, domains, key, batch):
    rows, width = x.shape
    lines = batch // 2
    length = 2 * rows
    val = own[1].shape[1]
    high, columns = own[0].shape
    saved = [
        jax.ShapeDtypeStruct((4, length, w), t)
        for w, t in ((val, BF), (val, BF), (128, F32), (val, BF), (key, BF), (key, BF), (length, BF))
    ]
    result = pl.pallas_call(
        functools.partial(gather_kernel, lines=lines),
        out_shape=(
            jax.ShapeDtypeStruct((batch, high, columns), BF),
            jax.ShapeDtypeStruct((batch, high, val), BF),
            jax.ShapeDtypeStruct((4, 2, rows, width), BF),
            jax.ShapeDtypeStruct((4, 2, rows, width), BF),
            jax.ShapeDtypeStruct((4, length, val), BF),
            *saved,
            jax.ShapeDtypeStruct((length, length), F32),
            jax.ShapeDtypeStruct((length, key // 2), F32),
            jax.ShapeDtypeStruct((length, key // 2), F32),
        ),
        in_specs=[anywhere()] * 4 + [vmem()] * 4 + [pl.BlockSpec(memory_space=pltpu.SMEM)] * 2,
        out_specs=(anywhere(), vmem(), anywhere(), anywhere(), vmem()) + tuple([anywhere()] * 10),
        scratch_shapes=[
            pltpu.VMEM((batch, high, columns), BF),
            pltpu.VMEM((4, 2, rows, width), BF),
            pltpu.VMEM((rows, width), BF),
            pltpu.VMEM((rows, width), BF),
            pltpu.VMEM((length, key // 2), F32),
            pltpu.VMEM((length, key // 2), F32),
            pltpu.VMEM((length, length), F32),
            pltpu.VMEM((4, length, val), F32),
        ]
        + [pltpu.VMEM(v.shape, v.dtype) for v in saved]
        + semaphores(6 * 2 * lines + 16)
        + [pltpu.SemaphoreType.DMA((21,))],
        compiler_params=pltpu.CompilerParams(collective_id=2, has_side_effects=True, vmem_limit_bytes=56 * 2**20),
        cost_estimate=pl.CostEstimate(flops=20 * 10**9, bytes_accessed=300000000, transcendentals=0),
        name="gather_first",
    )(*own, *other, x, gain[None], cotangent, *domains)
    stacked, out_t, normed, d_ffn, mixed = result[:5]
    return (
        stacked.reshape(-1, columns),
        out_t.reshape(-1, val),
        normed.reshape(8 * rows, width),
        d_ffn.reshape(8 * rows, width),
        mixed,
        result[5:12],
        result[12:],
    )


def partial_rows(part, rc, wires, rows, weights, s):
    half = part.shape[2]

    def body(i):
        cut = span(i, 512)
        total = dot(rows[...], weights[cut, :], 1, 1)
        part[s, 1, :, cut] = total[half:].astype(BF)
        part[s, 0, :, cut] = total[:half].astype(BF)

    blocks(weights.shape[0] // 512, body)
    send_cores(part, rc, wires, (s,))


def part_sums(part):
    return part.at[:, 0]


def forward_kernel(
    mixed,
    out_t,
    x,
    gain,
    own_up,
    own_down,
    other_up,
    other_down,
    d_ffn,
    whole,
    hidden,
    up,
    down,
    lifted,
    d_pre,
    part,
    rc,
    ra,
    rb,
    ea,
    eb,
    sa,
    sb,
    d_lifted,
    d_rows,
    send,
    recv,
    local,
    *,
    lines,
):
    b = lax.axis_index("batch")
    wires, moves = Wires(send, recv, lines), Moves(local)
    wires.enter(("head", "group", "x") + along(lines))
    order = first_order(lines)
    mine, others, weights = (own_up, own_down), (other_up, other_down), (up, down)
    half, wide = x.shape
    units = lifted.shape[2]

    def pointwise(r, total):
        row = x[r, :].astype(F32) + total
        hidden[r, :] = row
        shifted = row - jnp.mean(row, axis=1, keepdims=True)
        var_row = jnp.mean(shifted * shifted, axis=1, keepdims=True)
        whole[0, 0, r, :] = (shifted * lax.rsqrt(var_row + 1e-05) * gain[...]).astype(BF)

    def piece(i):
        for k in order:
            source = others[i] if k % 2 else mine[i]
            wires.start((i, k), source, weights[i].at[b], ("line", k))

    def relay(i):
        for k in order:
            wires.arrived((i, k))
            block = weights[i].at[b ^ (2 * k)]
            wires.start((i, "x", k), block, block, "x")

    def fetch(s):
        moves.start(d_ffn.at[s], d_rows.at[s % 2])

    def lift_back(s):
        moves.made[2 + s].wait()

        def body(i):
            r = span(i, half)
            d_lifted[s, r, :] = dot(d_rows[s % 2, r, :], down.reshape(wide, units)[...], 1, 0)

        blocks(2, body)
        if s < 2:
            fetch(s + 2)

    def lift(s):
        def body(i):
            r = span(i, half)
            act = dot(whole[s, i], up.reshape(wide, units)[...], 1, 0)
            square = act * act
            turn = jnp.tanh(GELU * act * (1 + 0.044715 * square))
            lifted[s, r, :] = (0.5 * act * (1 + turn)).astype(BF)
            slope = 0.5 * (1 + turn) + 0.5 * act * (1 - turn * turn) * GELU * (1 + 3 * 0.044715 * square)
            d_pre[s, r, :] = (d_lifted[s, r, :] * slope).astype(BF)

        blocks(2, body)

    for i in range(2):
        moves.start(mine[i], weights[i].at[b])
    fetch(0)
    fetch(1)
    piece(1)
    for i in (1, 0):
        wires.start((i, "x", 0), mine[i], weights[i].at[b], "x")
    for s in (3, 1, 2, 0):
        partial_rows(part, rc, wires, mixed.at[s], out_t, s)
    steps = exchange(part, whole, rc, part_sums(part), ra, rb, ea, eb, sa, sb, wires, pointwise)
    next(steps)
    relay(1)
    next(steps)
    piece(0)
    next(steps)
    next(steps)
    moves.made[0].wait()
    moves.made[1].wait()
    wires.arrived(*[(1, "x", k) for k in range(lines)])
    lift_back(0)
    next(steps)
    relay(0)
    lift_back(1)
    next(steps)
    lift_back(2)
    lift_back(3)
    wires.arrived(*[(0, "x", k) for k in range(lines)])
    wires.arrived("own")
    lift(0)
    wires.arrived("fa")
    wires.start("cfa", whole.at[3, 0, pl.ds(0, half // 2)], whole.at[3, 1, pl.ds(0, half // 2)], "head")
    wires.arrived("cza", "czb")
    lift(1)
    wires.arrived("fb")
    wires.start("cfb", whole.at[3, 0, pl.ds(half // 2, half // 2)], whole.at[3, 1, pl.ds(half // 2, half // 2)], "head")
    wires.arrived("cya", "cyb")
    lift(2)
    wires.arrived("cfa", "cfb")
    lift(3)
    wires.finish()


def backward_kernel(
    d_pre,
    up,
    ln_all,
    lifted,
    hidden,
    cotangent,
    gain,
    domains,
    domain_of,
    domain_weight,
    d_ffn,
    whole,
    d_hidden,
    d_gain,
    lines_out,
    part,
    rc,
    ra,
    rb,
    ea,
    eb,
    sa,
    sb,
    grads,
    rx,
    d_cols,
    send,
    recv,
    local,
    *,
    lines,
):
    wires, moves = Wires(send, recv, 2), Moves(local)
    wires.enter(TEAM + ("x",))
    wide, units = up.shape
    step = 256
    tokens = ln_all.shape[0]
    xbit = lax.axis_index("batch") % 2
    flat = grads.reshape(wide, 2 * units)
    d_flat = d_pre.reshape(tokens, units)
    l_flat = lifted.reshape(tokens, units)
    cuts = [pl.ds(0, units), pl.ds(units, units)]
    count = wide // step

    def fetch(i):
        moves.start(d_ffn.at[:, pl.ds(i * step, step)], d_cols.at[i % 2])

    fetch(0)
    fetch(1)
    d_gain[...] = jnp.zeros_like(d_gain)
    share = own_share(domains, domain_of, domain_weight)

    def pointwise(r, total):
        row = hidden[r, :]
        shifted = row - jnp.mean(row, axis=1, keepdims=True)
        var_row = jnp.mean(shifted * shifted, axis=1, keepdims=True)
        rstd = lax.rsqrt(var_row + 1e-05)
        unit = shifted * rstd
        terms = total * unit
        d_gain[...] += terms[:8] + terms[8:]
        d_unit = total * gain[...]
        mean_d = jnp.mean(d_unit, axis=1, keepdims=True)
        mean_du = jnp.mean(d_unit * unit, axis=1, keepdims=True)
        grad = cotangent[r, :].astype(F32) * share + rstd * (d_unit - mean_d - unit * mean_du)
        d_hidden[r, :] = grad
        whole[0, 0, r, :] = grad.astype(BF)

    def up_grads():
        def body(i):
            flat[span(i, step), cuts[0]] = dot(ln_all[:, span(i, step)], d_flat[...], 0, 0).astype(BF)

        blocks(count, body)
        across(wires, grads, rx, cuts[0], lines, "ffn")

    def down_grads():
        for i in range(count):
            moves.made[i].wait()
            flat[pl.ds(i * step, step), cuts[1]] = dot(d_cols[i % 2], l_flat[...], 0, 0).astype(BF)
            if i + 2 < count:
                fetch(i + 2)
        across(wires, grads, rx, cuts[1], lines, "ffn")

    def join(cut):
        for line in range(lines):
            wires.arrived(("ffn", "x", cut.start, line))

            def body(r):
                total = grads[2 * line + xbit, r, cut].astype(F32) + rx[line, r, cut].astype(F32)
                lines_out[line, r, cut] = total.astype(BF)

            tiles(rx.shape[1], body)

    for s in (3, 1, 2, 0):
        partial_rows(part, rc, wires, d_pre.at[s], up, s)
    steps = exchange(part, whole, rc, part_sums(part), ra, rb, ea, eb, sa, sb, wires, pointwise)
    next(steps)
    up_grads()
    next(steps)
    down_grads()
    next(steps)
    next(steps)
    join(cuts[0])
    next(steps)
    next(steps)
    join(cuts[1])
    for _ in steps:
        pass
    half = whole.shape[2] // 2
    for name, end, first in (("fa", "cfa", 0), ("fb", "cfb", half)):
        wires.arrived(name)
        block = pl.ds(first, half)
        wires.start(end, whole.at[3, 0, block], whole.at[3, 1, block], "head")
    wires.arrived("own", "cza", "cyb", "czb", "cya", "cfa", "cfb")
    wires.finish()


def first_order(lines):
    return [k for k in (2, 3, 1) if k < lines] + list(range(4, lines))


class Lines:
    def __init__(self, wires, lined, rz, slices, lines, tag, pick=lambda line: line):
        self.wires, self.lined, self.rz, self.slices, self.lines, self.tag = wires, lined, rz, slices, lines, tag
        self.pick = pick
        self.z = lax.axis_index("batch") // 2
        self.p = self.z % 2
        self.y = lax.axis_index("group")
        self.order = first_order(lines)

    def send(self, cut):
        for k in self.order:
            source = self.lined.at[self.pick(self.z ^ k), :, cut]
            self.wires.start((self.tag, "z", cut.start, k), source, self.rz.at[k, :, cut], ("line", k))

    def join(self, cut):
        lined, rz, slices, p, y = self.lined, self.rz, self.slices, self.p, self.y
        for k in self.order:
            self.wires.arrived((self.tag, "z", cut.start, k))

        def body(r):
            mine = lined[self.pick(self.z), r, cut].astype(F32)
            other = jnp.zeros_like(mine)
            for k in range(1, self.lines):
                term = rz[k, r, cut].astype(F32)
                if k % 2:
                    other = other + term
                else:
                    mine = mine + term
            slices[2 * p + y, r, cut] = mine.astype(BF)
            slices[2 * (1 - p) + y, r, cut] = other.astype(BF)

        tiles(lined.shape[1], body)
        for q in range(2):
            block = slices.at[2 * q + y, :, cut]
            self.wires.start((self.tag, "y", cut.start, q), block, block, "group")

    def store(self, cut, target, first, width, stage, turned=False):
        for q in range(2):
            self.wires.arrived((self.tag, "y", cut.start, q))
        for t in range(4):

            def fill(held):
                def body(r):
                    held[r, pl.ds(0, cut.size)] = self.slices[t, r, cut]

                tiles(target.shape[0], body)

            def fill_turned(held):
                for c in range(0, cut.size, 256):
                    piece = self.slices[t, :, pl.ds(cut.start + c, 256)].astype(F32)
                    held[pl.ds(c, 256), :] = piece.T.astype(BF)

            where = pl.ds(t * width + first, cut.size)
            if turned:
                stage.put(fill_turned, target.at[where, :])
            else:
                stage.put(fill, target.at[:, where], cut.size)


class Stage:
    def __init__(self, held, sems):
        self.held, self.sems, self.made = held, sems, []

    def put(self, fill, target, width=None):
        n, ring = len(self.made), self.held.shape[0]
        if n >= ring:
            self.made[n - ring].wait()
        held = self.held.at[n % ring]
        fill(held)
        source = held if width is None else held.at[:, pl.ds(0, width)]
        copy = pltpu.make_async_copy(source, target, self.sems.at[n])
        copy.start()
        self.made.append(copy)

    def finish(self):
        for copy in self.made[-self.held.shape[0] :]:
            copy.wait()


def across(wires, grads, rx, cut, lines, tag):
    other = 1 - lax.axis_index("batch") % 2
    for line in range(lines):
        wires.start((tag, "x", cut.start, line), grads.at[2 * line + other, :, cut], rx.at[line, :, cut], "x")


def across_join(wires, grads, rx, lined, cut, lines, tag, pick=lambda line: line):
    x = lax.axis_index("batch") % 2
    for line in range(lines):
        wires.arrived((tag, "x", cut.start, line))

        def body(r):
            total = grads[2 * line + x, r, cut].astype(F32) + rx[line, r, cut].astype(F32)
            lined[pick(line), r, cut] = total.astype(BF)

        tiles(rx.shape[1], body)


def middle_kernel(
    d_attn,
    w_out,
    mixed,
    gates,
    unit,
    rstd,
    values,
    q_rot,
    k_rot,
    weighted,
    decays,
    cosine,
    sine,
    lifted,
    down,
    hidden,
    ffn_lines,
    d_proj,
    output,
    d_up,
    d_down,
    d_out,
    part,
    rc,
    ry,
    rn,
    rz,
    slices,
    grads,
    rx,
    d_ret,
    d_scores,
    rz_out,
    slices_out,
    held,
    *rest,
    lines,
):
    buffers = rest[:7]
    turned, fetch_sems, stage_sems, turn_sems, send, recv = rest[7:]
    wires = Wires(send, recv, lines)
    stage = Stage(held, stage_sems)
    turner = Stage(turned, turn_sems)
    fetched = {}

    def fetch(s):
        for n, (source, buffer) in enumerate(zip((gates, unit, rstd, values, q_rot, k_rot, weighted), buffers)):
            copy = pltpu.make_async_copy(source.at[s], buffer.at[s % 2], fetch_sems.at[7 * s + n])
            copy.start()
            fetched[s, n] = copy

    fetch(0)
    fetch(1)
    wires.enter(("head", "group", "x") + along(lines))
    length = d_attn.shape[1]
    half = length // 2
    wide = w_out.shape[0]
    val = w_out.shape[1]
    units = lifted.shape[2]
    key = q_rot.shape[2]
    step = 256
    ffn = Lines(wires, ffn_lines, rz, slices, lines, "ffn")
    cuts = [pl.ds(c, units) for c in (0, units)]
    xbit = lax.axis_index("batch") % 2

    def pick(line):
        return 2 * line + xbit

    outs = Lines(wires, grads, rz_out, slices_out, lines, "out", pick)
    out_cut = pl.ds(0, val)

    def partial(s):
        def body(i):
            cut = span(i, 512)
            total = dot(lifted[s], down[cut, :], 1, 1)
            part[s, 1, :, cut] = total[half:].astype(BF)
            part[s, 0, :, cut] = total[:half].astype(BF)

        blocks(wide // 512, body)
        send_cores(part, rc, wires, (s,))

    def pointwise(r, total):
        output[r, :] = (hidden[r, :] + total).astype(BF)

    def retention(s):
        for n in range(7):
            fetched[s, n].wait()
        gates_s, unit_s, rstd_s, values_s, q_s, k_s, weighted_s = [buffer.at[s % 2] for buffer in buffers]

        def mix(i):
            r = span(i, half)
            d_mixed = dot(d_attn[s, r, :], w_out[...], 1, 0)
            gate = gates_s[r, :].astype(F32)
            sig = jax.nn.sigmoid(gate)
            norm = unit_s[r, :].astype(F32)
            d_gate = d_mixed * norm * (sig * (1 + gate * (1 - sig)))
            d_proj[s, r, pl.ds(2 * key + val, val)] = d_gate.astype(BF)
            d_norm = d_mixed * (gate * sig)
            mean_d = jnp.mean(d_norm, axis=1, keepdims=True)
            mean_dn = jnp.mean(d_norm * norm, axis=1, keepdims=True)
            d_ret[r, :] = (rstd_s[r, :][:, :1] * (d_norm - mean_d - norm * mean_dn)).astype(BF)

        blocks(2, mix)
        d_proj[s, :, pl.ds(2 * key, val)] = dot(weighted_s[...], d_ret[...], 0, 0).astype(BF)
        d_scores[...] = (dot(d_ret[...], values_s[...], 1, 1) * decays[...]).astype(BF)

        def turn(grad, first):
            a, b = grad[:, : key // 2], grad[:, key // 2 :]
            d_proj[s, :, pl.ds(first, key // 2)] = (a * cosine[...] + b * sine[...]).astype(BF)
            d_proj[s, :, pl.ds(first + key // 2, key // 2)] = (b * cosine[...] - a * sine[...]).astype(BF)

        turn(dot(d_scores[...], k_s[...], 1, 0), 0)
        turn(dot(d_scores[...], q_s[...], 0, 0), key)
        if s < 2:
            fetch(s + 2)

    def out_grads():
        flat = grads.reshape(wide, val)

        def body(i):
            total = jnp.zeros((step, val), F32)
            for s in range(4):
                total = total + dot(d_attn[s, :, span(i, step)], mixed[s], 0, 0)
            flat[span(i, step), :] = total.astype(BF)

        blocks(wide // step, body)
        across(wires, grads, rx, pl.ds(0, val), lines, "out")

    steps = reduce_rows(part, rc, ry, rn, wires, pointwise)
    ffn.send(cuts[0])
    ffn.send(cuts[1])
    partial(3)
    partial(2)
    next(steps)
    out_grads()
    partial(1)
    next(steps)
    partial(0)
    next(steps)
    retention(0)
    next(steps)
    retention(1)
    across_join(wires, grads, rx, grads, out_cut, lines, "out", pick)
    outs.send(out_cut)
    retention(2)
    ffn.join(cuts[0])
    ffn.join(cuts[1])
    retention(3)
    for _ in steps:
        pass
    ffn.store(cuts[0], d_up, 0, units, stage)
    ffn.store(cuts[1], d_down, 0, units, turner, True)
    outs.join(out_cut)
    outs.store(out_cut, d_out, 0, val, turner, True)
    stage.finish()
    turner.finish()
    wires.finish()


def last_kernel(
    d_proj,
    x,
    d_hidden,
    gain,
    ln_gains,
    normed_hbm,
    stacked_hbm,
    d_inputs,
    gains,
    d_query,
    d_key,
    d_value,
    d_gate,
    normed,
    stacked,
    grads,
    part,
    rc,
    ry,
    rn,
    rx,
    rz,
    slices,
    held,
    came,
    staged,
    local,
    stage_sems,
    send,
    recv,
    *,
    lines,
):
    wires, moves = Wires(send, recv, lines), Moves(local)
    wide, columns = stacked.shape
    tokens = normed.shape[0]
    step = 256
    val = d_value.shape[1] // 4
    key = d_query.shape[1] // 4
    for i in range(wide // step):
        cut = pl.ds(i * step, step)
        moves.start(normed_hbm.at[:, cut], normed.at[:, cut])
    moves.start(stacked_hbm, stacked)
    wires.enter(("head", "group", "x") + along(lines))
    xbit = lax.axis_index("batch") % 2
    stage = Stage(staged, stage_sems)

    def pick(line):
        return 2 * line + xbit

    main = Lines(wires, grads, rz, slices, lines, "main", pick)
    cuts = [pl.ds(c, 256) for c in (2 * key + val, 2 * key + val + 256, 2 * key, 2 * key + 256, 0, key)]
    flat = grads.reshape(wide, columns)
    held[0] = jnp.zeros_like(held[0])
    rows_all = d_proj.reshape(tokens, columns)

    def pointwise(r, total):
        row = x[r, :].astype(F32)
        scale = lax.rsqrt(jnp.mean(row * row, axis=1, keepdims=True) + 1e-06)
        unit = row * scale
        terms = total * unit
        held[0, :8] += terms[:8] + terms[8:]
        d_unit = total * gain[...]
        mean_du = jnp.mean(d_unit * unit, axis=1, keepdims=True)
        d_inputs[r, :] = (d_hidden[r, :] + scale * (d_unit - unit * mean_du)).astype(BF)

    def weight_grads(first, wait=False):
        cut = pl.ds(first, 512)

        def body(i):
            flat[span(i, step), cut] = dot(normed[:, span(i, step)], rows_all[:, cut], 0, 0).astype(BF)

        if wait:
            for i in range(wide // step):
                moves.made[i].wait()
                body(i)
        else:
            blocks(wide // step, body)
        for c in (first, first + 256):
            across(wires, grads, rx, pl.ds(c, 256), lines, "main")

    def partial(s):
        rows = d_proj.shape[1] // 2

        def body(i):
            cut = span(i, 512)
            total = dot(d_proj[s], stacked[cut, :], 1, 1)
            part[s, 1, :, cut] = total[rows:].astype(BF)
            part[s, 0, :, cut] = total[:rows].astype(BF)

        blocks(wide // 512, body)
        send_cores(part, rc, wires, (s,))

    def stage_x(at):
        across_join(wires, grads, rx, grads, cuts[at], lines, "main", pick)
        main.send(cuts[at])

    hops = ["head", "group", "x"]
    bit = 1
    while bit < lines:
        hops.append(("line", bit))
        bit *= 2

    def hop(at):
        if at:
            wires.arrived(("gain", at - 1))
            held[at] = held[at - 1] + came[at - 1]
        else:
            held[0, 8:] = ln_gains[...]
        if at < len(hops):
            wires.start(("gain", at), held.at[at], came.at[at], hops[at])
        else:
            gains[...] = held[at]

    targets = [(d_gate, val, 0), (d_gate, val, 256), (d_value, val, 0), (d_value, val, 256), (d_query, key, 0), (d_key, key, 0)]

    def store(at):
        target, width, first = targets[at]
        main.store(cuts[at], target, first, width, stage)

    steps = reduce_rows(part, rc, ry, rn, wires, pointwise)
    weight_grads(2 * key + val, True)
    moves.made[-1].wait()
    partial(3)
    partial(2)
    next(steps)
    weight_grads(2 * key)
    next(steps)
    stage_x(0)
    partial(1)
    weight_grads(0)
    next(steps)
    stage_x(1)
    partial(0)
    next(steps)
    stage_x(2)
    main.join(cuts[0])
    stage_x(3)
    main.join(cuts[1])
    stage_x(4)
    stage_x(5)
    main.join(cuts[2])
    for _ in steps:
        pass
    hop(0)
    main.join(cuts[3])
    hop(1)
    store(0)
    store(1)
    hop(2)
    store(2)
    main.join(cuts[4])
    hop(3)
    store(3)
    hop(4)
    main.join(cuts[5])
    store(4)
    store(5)
    for at in range(5, len(hops) + 1):
        hop(at)
    stage.finish()
    wires.finish()


def exchange_scratch(rows, width):
    half = rows // 2
    return [
        pltpu.VMEM((4, 2, rows, width), BF),
        pltpu.VMEM((4, rows, width), BF),
        pltpu.VMEM((2, half, width), BF),
        pltpu.VMEM((2, half, width), BF),
        pltpu.VMEM((half, width), BF),
        pltpu.VMEM((half, width), BF),
        pltpu.VMEM((half, width), BF),
        pltpu.VMEM((half, width), BF),
    ]


def lean_scratch(rows, width):
    return [
        pltpu.VMEM((4, 2, rows, width), BF),
        pltpu.VMEM((4, rows, width), BF),
        pltpu.VMEM((2, rows, width), BF),
        pltpu.VMEM((rows, width), BF),
    ]


def semaphores(count):
    return [pltpu.SemaphoreType.DMA((count,)), pltpu.SemaphoreType.DMA((count,))]


def anywhere():
    return pl.BlockSpec(memory_space=pl.ANY)


def vmem():
    return pl.BlockSpec(memory_space=pltpu.VMEM)


def forward_exchange(mixed, out_t, x, gain, own, other, d_ffn, batch):
    rows, width = x.shape
    lines = batch // 2
    high, units = own[0].shape
    length = 2 * rows
    whole, hidden, up, down, lifted, d_pre = pl.pallas_call(
        functools.partial(forward_kernel, lines=lines),
        out_shape=(
            jax.ShapeDtypeStruct((4, 2, rows, width), BF),
            jax.ShapeDtypeStruct((rows, width), F32),
            jax.ShapeDtypeStruct((batch, high, units), BF),
            jax.ShapeDtypeStruct((batch, high, units), BF),
            jax.ShapeDtypeStruct((4, length, units), BF),
            jax.ShapeDtypeStruct((4, length, units), BF),
        ),
        in_specs=[vmem()] * 8 + [anywhere()],
        out_specs=tuple([vmem()] * 6),
        scratch_shapes=exchange_scratch(rows, width)
        + [pltpu.VMEM((4, length, units), F32), pltpu.VMEM((2, length, width), BF)]
        + semaphores(24 + 4 * lines)
        + [pltpu.SemaphoreType.DMA((6,))],
        compiler_params=pltpu.CompilerParams(collective_id=0, has_side_effects=True, vmem_limit_bytes=58 * 2**20),
        cost_estimate=pl.CostEstimate(flops=12 * 10**9, bytes_accessed=300000000, transcendentals=0),
        name="forward_exchange",
    )(mixed, out_t, x, gain[None], *own, *other, d_ffn.reshape(4, length, width))
    return whole.reshape(8 * rows, width), hidden, up.reshape(width, -1), down.reshape(width, -1), lifted, d_pre


def backward_exchange(d_pre, up, ln_all, lifted, hidden, cotangent, gain, domains, d_ffn, batch):
    rows, width = hidden.shape
    lines = batch // 2
    block = (width // batch, 2 * up.shape[1])
    whole, d_hidden, d_gain, lined = pl.pallas_call(
        functools.partial(backward_kernel, lines=lines),
        out_shape=(
            jax.ShapeDtypeStruct((4, 2, rows, width), BF),
            jax.ShapeDtypeStruct((rows, width), F32),
            jax.ShapeDtypeStruct((8, width), F32),
            jax.ShapeDtypeStruct((lines,) + block, BF),
        ),
        in_specs=[vmem()] * 8 + [pl.BlockSpec(memory_space=pltpu.SMEM)] * 2 + [anywhere()],
        out_specs=(vmem(), vmem(), vmem(), vmem()),
        scratch_shapes=exchange_scratch(rows, width)
        + [
            pltpu.VMEM((batch,) + block, BF),
            pltpu.VMEM((lines,) + block, BF),
            pltpu.VMEM((2, 8 * rows, 256), BF),
        ]
        + semaphores(24 + 2 * lines)
        + [pltpu.SemaphoreType.DMA((width // 256,))],
        compiler_params=pltpu.CompilerParams(collective_id=1, has_side_effects=True, vmem_limit_bytes=63 * 2**20),
        cost_estimate=pl.CostEstimate(flops=14 * 10**9, bytes_accessed=300000000, transcendentals=0),
        name="backward_exchange",
    )(d_pre, up, ln_all, lifted, hidden, cotangent, gain[None], *domains, d_ffn)
    return whole.reshape(8 * rows, width), d_hidden, d_gain, lined


def middle_exchange(d_attn, w_out, mixed, saved, tables, lifted, down, hidden, ffn_lines, batch):
    rows, width = hidden.shape
    lines = batch // 2
    length = 2 * rows
    block = ffn_lines.shape[1:]
    val = w_out.shape[1]
    units = lifted.shape[2]
    gates, unit, rstd, values, q_rot, k_rot, weighted = saved
    columns = 2 * q_rot.shape[2] + 2 * val
    return pl.pallas_call(
        functools.partial(middle_kernel, lines=lines),
        out_shape=(
            jax.ShapeDtypeStruct((4, length, columns), BF),
            jax.ShapeDtypeStruct((rows, width), BF),
            jax.ShapeDtypeStruct((block[0], 4 * units), BF),
            jax.ShapeDtypeStruct((4 * units, block[0]), BF),
            jax.ShapeDtypeStruct((4 * val, block[0]), BF),
        ),
        in_specs=[vmem()] * 3 + [anywhere()] * 7 + [vmem()] * 7,
        out_specs=(vmem(), vmem(), anywhere(), anywhere(), anywhere()),
        scratch_shapes=lean_scratch(rows, width)
        + [
            pltpu.VMEM((lines,) + block, BF),
            pltpu.VMEM((4,) + block, BF),
            pltpu.VMEM((batch, block[0], val), BF),
            pltpu.VMEM((lines, block[0], val), BF),
            pltpu.VMEM((length, val), BF),
            pltpu.VMEM((length, length), BF),
            pltpu.VMEM((lines, block[0], val), BF),
            pltpu.VMEM((4, block[0], val), BF),
            pltpu.VMEM((2, block[0], units), BF),
        ]
        + [pltpu.VMEM((2,) + v.shape[1:], v.dtype) for v in saved]
        + [pltpu.VMEM((2, units, block[0]), BF)]
        + [pltpu.SemaphoreType.DMA((28,)), pltpu.SemaphoreType.DMA((4,)), pltpu.SemaphoreType.DMA((8,))]
        + semaphores(16 + 3 * (lines + 1) + lines),
        compiler_params=pltpu.CompilerParams(collective_id=4, has_side_effects=True, vmem_limit_bytes=63 * 2**20),
        cost_estimate=pl.CostEstimate(flops=20 * 10**9, bytes_accessed=200000000, transcendentals=0),
        name="middle_exchange",
    )(
        d_attn.reshape(4, length, width),
        w_out,
        mixed,
        gates,
        unit,
        rstd,
        values,
        q_rot,
        k_rot,
        weighted,
        *tables,
        lifted,
        down,
        hidden,
        ffn_lines,
    )


def last_exchange(d_proj, x, d_hidden, gain, ln_gains, normed, stacked, key, batch):
    rows, width = x.shape
    lines = batch // 2
    high = width // batch
    columns = stacked.shape[1]
    val = (columns - 2 * key) // 2
    steps = 2 + batch.bit_length() - 1
    return pl.pallas_call(
        functools.partial(last_kernel, lines=lines),
        out_shape=(
            jax.ShapeDtypeStruct((rows, width), BF),
            jax.ShapeDtypeStruct((16, width), F32),
            jax.ShapeDtypeStruct((high, 4 * key), BF),
            jax.ShapeDtypeStruct((high, 4 * key), BF),
            jax.ShapeDtypeStruct((high, 4 * val), BF),
            jax.ShapeDtypeStruct((high, 4 * val), BF),
        ),
        in_specs=[vmem()] * 5 + [anywhere()] * 2,
        out_specs=(vmem(), vmem()) + tuple([anywhere()] * 4),
        scratch_shapes=[
            pltpu.VMEM(normed.shape, BF),
            pltpu.VMEM(stacked.shape, BF),
            pltpu.VMEM((batch, high, columns), BF),
        ]
        + lean_scratch(rows, width)
        + [
            pltpu.VMEM((lines, high, columns), BF),
            pltpu.VMEM((lines, high, columns), BF),
            pltpu.VMEM((4, high, columns), BF),
            pltpu.VMEM((steps + 1, 16, width), F32),
            pltpu.VMEM((steps, 16, width), F32),
            pltpu.VMEM((2, high, val), BF),
            pltpu.SemaphoreType.DMA((width // 256 + 1,)),
            pltpu.SemaphoreType.DMA((4 * (columns // 256),)),
        ]
        + semaphores(16 + steps + (columns // 256) * (2 * lines + 1)),
        compiler_params=pltpu.CompilerParams(collective_id=3, has_side_effects=True, vmem_limit_bytes=63 * 2**20),
        cost_estimate=pl.CostEstimate(flops=26 * 10**9, bytes_accessed=300000000, transcendentals=0),
        name="last_exchange",
    )(d_proj, x, d_hidden, gain[None], ln_gains, normed, stacked)


class Place:
    def __init__(self):
        self.batch = lax.axis_size("batch")
        self.b = lax.axis_index("batch")
        self.y = lax.axis_index("group")
        self.c = lax.axis_index("head")
        self.lines = self.batch // 2
        self.z = self.b // 2
        self.x = self.b % 2
        self.p = self.z % 2
        self.slot = 2 * self.p + self.y

    def cut(self, array, axis):
        width = array.shape[axis] // 4
        own = lax.dynamic_slice_in_dim(array, self.slot * width, width, axis)
        other = lax.dynamic_slice_in_dim(array, (self.slot ^ 2) * width, width, axis)
        return own, other

def on_device(
    inputs,
    rms_gain,
    w_query,
    w_key,
    w_value,
    w_gate,
    w_out,
    ln_gain,
    w_up,
    w_down,
    cotangent,
    domain_of,
    domain_weight,
):
    here = Place()

    parts = [here.cut(w, 1) for w in (w_query, w_key, w_value, w_gate)]
    own = jnp.concatenate([own for own, _ in parts], axis=1)
    other = jnp.concatenate([other for _, other in parts], axis=1)
    out_own, out_other = [v.T for v in here.cut(w_out, 0)]
    domains = (domain_of[None], domain_of, domain_weight)
    stacked, out_t, normed_all, d_ffn_all, mixed, saved, tables = gather_first(
        (own, out_own), (other, out_other), inputs[0], rms_gain, cotangent[0], domains, KEY, here.batch
    )
    up_parts = here.cut(w_up, 1)
    down_parts = [v.T for v in here.cut(w_down, 0)]
    ln_all, hidden, up, down_t, lifted, d_pre = forward_exchange(
        mixed,
        out_t,
        inputs[0],
        ln_gain,
        (up_parts[0], down_parts[0]),
        (up_parts[1], down_parts[1]),
        d_ffn_all,
        here.batch,
    )
    d_attn_all, d_hidden, d_ln_gain, ffn_lines = backward_exchange(
        d_pre, up, ln_all, lifted, hidden, cotangent[0], ln_gain, domains, d_ffn_all, here.batch
    )
    d_proj, output, d_up, d_down, d_w_out = middle_exchange(
        d_attn_all,
        out_t,
        mixed,
        saved,
        tables,
        lifted,
        down_t,
        hidden,
        ffn_lines,
        here.batch,
    )
    d_inputs, gains, d_query, d_key, d_value, d_gate = last_exchange(
        d_proj, inputs[0], d_hidden, rms_gain, d_ln_gain, normed_all, stacked, KEY, here.batch
    )
    gain_rms = jnp.sum(gains[:8], axis=0)
    gain_ln = jnp.sum(gains[8:], axis=0)
    return (
        output[None],
        d_inputs[None],
        gain_rms,
        d_query.astype(F32),
        d_key.astype(F32),
        d_value.astype(F32),
        d_gate.astype(F32),
        d_w_out.astype(F32),
        gain_ln,
        d_up.astype(F32),
        d_down.astype(F32),
    )


def solution(mesh):
    rows = P(("batch", "group"), "head", None)
    wide = P("batch", "head")
    tall = P("head", "batch")
    return jax.shard_map(
        on_device,
        mesh=mesh,
        in_specs=(rows, P(), wide, wide, wide, wide, tall, P(), wide, tall, rows, P(), P()),
        out_specs=(rows, rows, P(), wide, wide, wide, wide, tall, P(), wide, tall),
        check_vma=False,
    )
```
